32 devices in a mesh: grp: 2 (over y), lon: 4 (over x, core), lat: 4 (over z).
Axes of the slice: x: 2, y: 2, z: 4, core: 2. Of those that a mesh axis runs over, the one named last changes fastest.
Arguments:
- tracers: float32 [4, 64, 128, 128], P('grp', 'lat', 'lon'), parts along dimension 0, may hold values from -6 to 6
- adjoint_in: float32 [4, 64, 128, 128], P('grp', 'lat', 'lon'), parts along dimension 0, may hold values from -6 to 6
- shifts: int32 [2, 64], replicated, may hold values from 0 to 127, as said below
- fractions: float32 [2, 64], replicated, may hold values from 0.05 to 0.95
- meridional: float32 [2, 64, 128], P(None, None, 'lon'), may hold values from -0.9 to 0.9
Outputs:
- advected: float32 [4, 64, 128, 128], P('grp', 'lat', 'lon'), parts along dimension 0
- adjoint_out: float32 [4, 64, 128, 128], P('grp', 'lat', 'lon'), parts along dimension 0
The draws below stay inside these ranges and needn't reach their ends.
There are 2 independent parts, one for each index of `grp`. The reference program is written for one: setup_inputs(seed, part) draws one part's arguments, and reference() takes and returns one part's arrays. A program takes and returns all parts, laid end to end along the dimension named above; an argument that names none is the same for every part. Nothing has to cross between parts.
Inputs may be any that keep to these rules, and one draw needn't show every extreme that they name: At row j, shifts lie below 1 + (127) d^2 / 63^2 with d = |2j - 63|.
All inputs are finite; a program needn't handle non-finite values.
Results may differ from the reference program's by a relative error of at most 0.0003.
Values sent between devices are 32-bit elements; how exact they have to be, the bound alone decides.
A program may use at most 128 MiB of HBM per device.

```python
import jax
import jax.numpy as jnp
from jax import lax

C = 128
LEV = 2
NX = 128
NY = 64


def draw_shifts(key, part):
    row_ids = jnp.arange(NY, dtype=jnp.int32)
    distance = jnp.abs(2 * row_ids + 1 - NY)
    ceiling = 1 + (NX - 1) * distance * distance // ((NY - 1) * (NY - 1))
    drawn = jax.random.randint(key, (LEV, NY), 0, ceiling[None, :], dtype=jnp.int32)
    drawn = drawn.at[0, 0].set(NX - 1)
    drawn = drawn.at[0, NY // 2].set(0)
    return drawn


def steps_of(own_key, extent, shards, least, largest):
    level = 1.0
    for axis_at, shards_of in shards:
        draws = jax.random.uniform(jax.random.fold_in(jax.random.fold_in(own_key, 6), axis_at), (shards_of,), jnp.float32, least / len(shards), largest / len(shards))
        level = level * jnp.repeat(jnp.exp(draws), extent[axis_at] // shards_of).reshape((-1,) + (1,) * (len(extent) - 1 - axis_at))
    return level


def noise(stream_key, dims, scale, reach, pieces=(), kind=jnp.bfloat16):
    values = scale * jax.random.normal(stream_key, dims, jnp.float32)
    if pieces:
        values = values * steps_of(stream_key, dims, pieces, -0.22, 0.18)
    return jnp.clip(values, -reach, reach).astype(kind)


def setup_inputs(seed: int = 0, part: int = 0) -> dict:
    seeds = jax.random.split(jax.random.key(seed), 6)
    part_keys = jax.random.split(jax.random.fold_in(seeds[5], part), 6)
    return {
        "tracers": noise(part_keys[0], (LEV, NY, NX, C), 1.0, 6.0, ((1, 4), (2, 4)), jnp.float32),
        "adjoint_in": noise(part_keys[1], (LEV, NY, NX, C), 1.0, 6.0, ((1, 4), (2, 4)), jnp.float32),
        "shifts": draw_shifts(jax.random.fold_in(seeds[5], 71), part),
        "fractions": jnp.clip(jax.random.uniform(seeds[3], (LEV, NY), jnp.float32, 0.05, 0.95), 0.05, 0.95),
        "meridional": jnp.clip(jax.random.uniform(seeds[4], (LEV, NY, NX), jnp.float32, -0.9, 0.9) * steps_of(seeds[4], (LEV, NY, NX), ((2, 4),), -0.4, 0.0), -0.9, 0.9),
    }


def take_slice(values_in, start_at, stop_at, dimension):
    return lax.slice_in_dim(values_in, start_at, stop_at, axis=dimension)

def edge_values(values_in, amount, dimension):
    inner_sum = take_slice(values_in, 1, amount + 1, dimension) + take_slice(values_in, 2, amount + 2, dimension)
    outer_sum = take_slice(values_in, 0, amount, dimension) + take_slice(values_in, 3, amount + 3, dimension)
    return (7.0 * inner_sum - outer_sum) / 12.0

def cell_profile(values_in, dimension):
    interior = values_in.shape[dimension] - 6
    edge_row = edge_values(values_in, interior + 3, dimension)
    left_edge = take_slice(edge_row, 0, interior + 2, dimension)
    right_edge = take_slice(edge_row, 1, interior + 3, dimension)
    centres = take_slice(values_in, 2, interior + 4, dimension)
    curvature = 6.0 * centres - 3.0 * (left_edge + right_edge)
    return (interior, left_edge, right_edge, right_edge - left_edge, curvature)

def zonal_step(values_in, courant, dimension):
    interior, left_edge, right_edge, difference, curvature = cell_profile(values_in, dimension)
    transport = courant * (right_edge - 0.5 * courant * (difference - (1.0 - courant * (2.0 / 3.0)) * curvature))
    return take_slice(values_in, 3, interior + 3, dimension) - take_slice(transport, 1, interior + 1, dimension) + take_slice(transport, 0, interior, dimension)

def meridional_step(values_in, face_courant, dimension):
    interior, left_edge, right_edge, difference, curvature = cell_profile(values_in, dimension)

    def below_part(source):
        return take_slice(source, 0, interior + 1, dimension)

    def above_part(source):
        return take_slice(source, 1, interior + 2, dimension)
    northward = face_courant * (below_part(right_edge) - 0.5 * face_courant * (below_part(difference) - (1.0 - face_courant * (2.0 / 3.0)) * below_part(curvature)))
    southward = face_courant * (above_part(left_edge) - 0.5 * face_courant * above_part(difference) - above_part(curvature) * (0.5 * face_courant + face_courant * face_courant / 3.0))
    transport = jnp.where(face_courant > 0.0, northward, southward)
    return take_slice(values_in, 3, interior + 3, dimension) - take_slice(transport, 1, interior + 1, dimension) + take_slice(transport, 0, interior, dimension)

def advect_level(values_in, shift_row, fraction_row, face_level):
    width_cells = values_in.shape[1]
    positions = jnp.mod(jnp.arange(width_cells, dtype=jnp.int32)[None, :] - shift_row[:, None].astype(jnp.int32), width_cells).astype(jnp.int32)
    shifted = jnp.take_along_axis(values_in, positions[:, :, None], axis=1)
    wrapped = jnp.concatenate([shifted[:, -3:], shifted, shifted[:, :3]], axis=1)
    zonal = zonal_step(wrapped, fraction_row[:, None, None], 1)
    padded = jnp.pad(zonal, ((3, 3), (0, 0), (0, 0)))
    return meridional_step(padded, face_level[:, :, None], 0)

def reference(tracers, adjoint_in, shifts, fractions, meridional):
    forward_levels = []
    backward_levels = []
    for level_index in range(LEV):
        zero_row = jnp.zeros((1, NX), meridional.dtype)
        face_level = jnp.concatenate([zero_row, meridional[level_index, 1:], zero_row], axis=0)

        def one_level(values_in):
            return advect_level(values_in, shifts[level_index], fractions[level_index], face_level)
        result, pullback = jax.vjp(one_level, tracers[level_index])
        forward_levels.append(result)
        backward_levels.append(pullback(adjoint_in[level_index])[0])
    return (jnp.stack(forward_levels), jnp.stack(backward_levels))
```

```python
import functools

import jax
import jax.numpy as jnp
from jax import lax
from jax.experimental import pallas as pl
from jax.experimental.pallas import tpu as pltpu
from jax.sharding import PartitionSpec as P

MESH = pl.DeviceIdType.MESH
SUB = 8
RIM = 3


def chunk_list(levels, rows, step):
    return [(lv, r0) for lv in range(levels) for r0 in range(0, rows, step)]


def reach(total_cells, total_rows, row):
    d = abs(2 * row + 1 - total_rows)
    return (total_cells - 1) * d * d // ((total_rows - 1) * (total_rows - 1))


def face_terms(v):
    size = jnp.abs(v)
    beta = v * (0.5 * size) * (1.0 - size * (2.0 / 3.0))
    return beta, 0.5 * v * v


def zonal_taps(c):
    b = 1.0 - c * (2.0 / 3.0)
    p = c * (1.0 - 0.5 * c - 1.5 * c * b)
    q = c * (0.5 * c - 1.5 * c * b)
    r = 3.0 * c * c * b
    d = p - q
    t = 1.0 / 12.0
    s = 7.0 / 12.0
    return (
        -t * q,
        s * q - t * d,
        r + t * p + s * d + s * q,
        1.0 - r - s * p + s * d - t * q,
        -s * p - t * d,
        t * p,
    )


def general(dims, *refs):
    levels, rows, cells, width, n_lon, n_lat, step = dims
    chunks = chunk_list(levels, rows, step)
    nq = len(chunks)
    tr, ad, shifts_in, fractions_in, mer_in, of, oa = refs[:7]
    gath = (refs[7 : 7 + nq], refs[7 + nq : 7 + 2 * nq])
    zb, ab, vb, taps, shifts, fractions, mer, loc, ssem, rsem, hs, hr = refs[7 + 2 * nq :]
    total_cells = cells * n_lon
    total_rows = rows * n_lat
    n_x = n_lon // 2

    me = lax.axis_index("lon")
    lat = lax.axis_index("lat")
    first = lat * rows
    core = lax.rem(me, 2)
    partner = me + 1 - 2 * core
    order = list(range(nq))

    own = []
    dup = []
    for q, (lv, r0) in enumerate(chunks):
        a = pltpu.make_async_copy(
            tr.at[lv, pl.ds(r0, step)], gath[0][q].at[:, pl.ds(0, cells)], loc.at[q]
        )
        a.start()
        own.append(a)
    adc = pltpu.make_async_copy(ad, ab.at[:, pl.ds(RIM, rows)], loc.at[2 * nq])
    adc.start()
    for q, (lv, r0) in enumerate(chunks):
        b = pltpu.make_async_copy(
            tr.at[lv, pl.ds(r0, step)],
            gath[0][q].at[:, pl.ds(total_cells, cells)],
            loc.at[nq + q],
        )
        b.start()
        dup.append(b)

    small = []
    for k, (source, target) in enumerate(
        ((shifts_in, shifts), (fractions_in, fractions), (mer_in, mer))
    ):
        d = pltpu.make_async_copy(source, target, loc.at[2 * nq + 1 + k])
        d.start()
        small.append(d)

    barrier = pltpu.get_barrier_semaphore()
    pl.semaphore_signal(barrier, inc=1, device_id={"lon": partner}, device_id_type=MESH)
    for dx in range(1, n_x):
        pl.semaphore_signal(
            barrier, inc=1, device_id={"lon": lax.rem(me + 2 * dx, n_lon)}, device_id_type=MESH
        )

    @pl.when(lat > 0)
    def _():
        pl.semaphore_signal(barrier, inc=1, device_id={"lat": lat - 1}, device_id_type=MESH)

    @pl.when(lat < n_lat - 1)
    def _():
        pl.semaphore_signal(barrier, inc=1, device_id={"lat": lat + 1}, device_id_type=MESH)

    inner = jnp.logical_and(lat > 0, lat < n_lat - 1)

    @pl.when(inner)
    def _():
        pl.semaphore_wait(barrier, n_x + 2)

    @pl.when(jnp.logical_not(inner))
    def _():
        pl.semaphore_wait(barrier, n_x + min(n_lat - 1, 1))

    def lat_copies(buf, k):
        down = pltpu.make_async_remote_copy(
            buf.at[:, pl.ds(RIM, RIM)],
            buf.at[:, pl.ds(RIM + rows, RIM)],
            hs.at[k, 0],
            hr.at[k, 0],
            device_id={"lat": lat - 1},
            device_id_type=MESH,
        )
        up = pltpu.make_async_remote_copy(
            buf.at[:, pl.ds(rows, RIM)],
            buf.at[:, pl.ds(0, RIM)],
            hs.at[k, 1],
            hr.at[k, 1],
            device_id={"lat": lat + 1},
            device_id_type=MESH,
        )
        return down, up

    def lat_start(buf, k):
        down, up = lat_copies(buf, k)

        @pl.when(lat > 0)
        def _():
            down.start()

        @pl.when(lat < n_lat - 1)
        def _():
            up.start()

    def lat_wait(buf, k):
        down, up = lat_copies(buf, k)

        @pl.when(lat > 0)
        def _():
            down.wait_send()
            up.wait_recv()

        @pl.when(lat < n_lat - 1)
        def _():
            up.wait_send()
            down.wait_recv()

    def x_copy(a, q, dx, span):
        lo, hi = span
        return pltpu.make_async_remote_copy(
            gath[a][q].at[:, pl.ds(lo, hi - lo)],
            gath[a][q].at[:, pl.ds((n_lon - 2 * dx) * cells + lo, hi - lo)],
            ssem.at[a, q, dx],
            rsem.at[a, q, dx],
            device_id={"lon": lax.rem(me + 2 * dx, n_lon)},
            device_id_type=MESH,
        )

    def core_copy(a, q, dx, span):
        lo, hi = span
        source = ((n_lon - 2 * dx) % n_lon) * cells + lo
        slot = lax.rem(2 * n_lon - 2 * dx + 2 * core - 1, n_lon)
        return pltpu.make_async_remote_copy(
            gath[a][q].at[:, pl.ds(source, hi - lo)],
            gath[a][q].at[:, pl.ds(pl.multiple_of(slot * cells + lo, SUB), hi - lo)],
            ssem.at[a, q, n_x + dx],
            rsem.at[a, q, n_x + dx],
            device_id={"lon": partner},
            device_id_type=MESH,
        )

    whole = (0, cells)

    def gather_start(a, q):
        for dx in range(1, n_x):
            x_copy(a, q, dx, whole).start()
        core_copy(a, q, 0, whole).start()

    def relay(a, q):
        for dx in range(1, n_x):
            x_copy(a, q, dx, whole).wait_recv()
            core_copy(a, q, dx, whole).start()

    def gather_finish(a, q):
        for dx in range(n_x):
            core_copy(a, q, dx, whole).wait_recv()

    def gather_drain(a, q):
        for dx in range(n_x):
            core_copy(a, q, dx, whole).wait_send()
        for dx in range(1, n_x):
            x_copy(a, q, dx, whole).wait_send()

    adc.wait()
    lat_start(ab, 0)
    for q in range(nq):
        own[q].wait()
        gather_start(0, q)

    @pl.when(lat == 0)
    def _():
        for buf in (ab, zb):
            buf[:, pl.ds(0, RIM)] = jnp.zeros((levels, RIM, cells, width), jnp.float32)

    @pl.when(lat == n_lat - 1)
    def _():
        for buf in (ab, zb):
            buf[:, pl.ds(RIM + rows, RIM)] = jnp.zeros((levels, RIM, cells, width), jnp.float32)

    for d in small:
        d.wait()
    faces = rows + 5
    lanes = lax.broadcasted_iota(jnp.int32, (cells, total_rows), 1)
    for lv in range(levels):

        @pl.loop(0, faces)
        def _(f):
            row = first + f - 2
            chosen = jnp.logical_and(lanes == row, lanes > 0)
            column = jnp.sum(jnp.where(chosen, mer[lv], 0.0), axis=1, keepdims=True)
            vb[lv, f] = jnp.broadcast_to(column, (cells, width))

        @pl.loop(0, rows)
        def _(r):
            for k, t in enumerate(zonal_taps(fractions[lv, first + r])):
                taps[(lv * rows + r) * 6 + k] = t

    lat_wait(ab, 0)
    for lv in range(levels):

        @pl.loop(0, cells // SUB)
        def _(c):
            at = pl.ds(pl.multiple_of(c * SUB, SUB), SUB)
            ev, q6b, dqb, eb = {}, {}, {}, {}
            carry = None
            y = {r: ab[lv, r + RIM, at, :] for r in range(-3, -1)}
            for f in range(-2, rows + 3):
                y[f] = ab[lv, f + RIM, at, :]
                v = vb[lv, f + 2, at, :]
                north = v > 0.0
                beta, gamma = face_terms(v)
                change = y[f] - y[f - 1]
                ev[f] = v * change
                b = beta * change
                g = -gamma * change
                bn, gn = jnp.where(north, b, 0.0), jnp.where(north, g, 0.0)
                if carry is not None:
                    q6b[f - 1] = bn + carry[0]
                    dqb[f - 1] = gn + carry[1]
                carry = (b - bn, g - gn)
                h = f - 1
                if h >= -1:
                    eb[h] = ev[h] - 3.0 * (q6b[h - 1] + q6b[h]) + (dqb[h - 1] - dqb[h])
                r = h - 2
                if r >= 0:
                    value = (
                        y[r]
                        + 6.0 * q6b[r]
                        + (7.0 / 12.0) * (eb[r] + eb[r + 1])
                        - (1.0 / 12.0) * (eb[r - 1] + eb[r + 2])
                    )
                    q = lv * (rows // step) + r // step
                    gath[1][q][r % step, at, :] = value
                    gath[1][q][
                        r % step, pl.ds(pl.multiple_of(total_cells + c * SUB, SUB), SUB), :
                    ] = value

        for q, (l2, _r) in enumerate(chunks):
            if l2 == lv:
                gather_start(1, q)

    def sweep(a, q, sink, sink_row, sign):
        lv, r0 = chunks[q]
        buf = gath[a][q]

        @pl.loop(0, step)
        def _(r):
            buf[r, pl.ds(total_cells + cells, SUB), :] = buf[r, pl.ds(cells, SUB), :]
            shift = shifts[lv, first + r0 + r]
            if sign < 0:
                start = lax.rem(2 * total_cells - shift - 3, total_cells)
            else:
                start = lax.rem(2 * total_cells + shift - 2, total_cells)
            base = (lv * rows + r0 + r) * 6
            w = [taps[base + k] for k in range(6)]
            if sign > 0:
                w = w[::-1]
            for c in range(cells // SUB):
                total = None
                for k in range(6):
                    term = w[k] * buf[r, pl.ds(start + c * SUB + k, SUB), :]
                    total = term if total is None else total + term
                sink[lv, sink_row + r0 + r, pl.ds(c * SUB, SUB), :] = total

    for b in dup:
        b.wait()
    for i, q in enumerate(order):
        relay(0, q)
        if i > 0:
            gather_finish(0, order[i - 1])
            sweep(0, order[i - 1], zb, RIM, -1)
    gather_finish(0, order[-1])
    sweep(0, order[-1], zb, RIM, -1)
    lat_start(zb, 1)

    relay(1, order[0])
    lat_wait(zb, 1)

    for lv in range(levels):

        @pl.loop(0, cells // SUB)
        def _(c):
            at = pl.ds(pl.multiple_of(c * SUB, SUB), SUB)
            z = {r: zb[lv, r + RIM, at, :] for r in range(-3, 0)}
            e, q6, dq, flux = {}, {}, {}, {}
            for f in range(-1, rows + 2):
                z[f + 1] = zb[lv, f + 1 + RIM, at, :]
                e[f] = (7.0 / 12.0) * (z[f - 1] + z[f]) - (1.0 / 12.0) * (z[f - 2] + z[f + 1])
                u = f - 1
                if u >= -1:
                    q6[u] = 6.0 * z[u] - 3.0 * (e[u] + e[f])
                    dq[u] = e[f] - e[u]
                if u >= 0:
                    v = vb[lv, u + 2, at, :]
                    north = v > 0.0
                    beta, gamma = face_terms(v)
                    flux[u] = (
                        v * e[u]
                        + beta * jnp.where(north, q6[u - 1], q6[u])
                        - gamma * jnp.where(north, dq[u - 1], dq[u])
                    )
                if u >= 1:
                    of[lv, u - 1, at, :] = z[u - 1] - flux[u] + flux[u - 1]

    def finish_adjoint(q):
        lv, r0 = chunks[q]
        gather_finish(1, q)
        sweep(1, q, oa, 0, 1)

    for i in range(1, nq):
        relay(1, order[i])
        finish_adjoint(order[i - 1])
    finish_adjoint(order[-1])

    for a in range(2):
        for q in range(nq):
            gather_drain(a, q)


HEAD, TAIL = 0, 1


def fits(rows, cells, n_lon, n_lat):
    if n_lon != 4 or n_lat != 4 or rows % 4 or cells % SUB:
        return False
    return reach(cells * n_lon, rows * n_lat, rows) + RIM <= cells + SUB


def detours(levels, rows, step):
    per = rows // step
    return ((1, 2, per + 2), (1, 2, per + 2))


def pack_plan(rows, cells, n_lon, n_lat, a, side):
    big = (side == TAIL) == (a == 0)
    slots = []
    at = SUB
    for k in range(rows):
        s = RIM - 1
        if big:
            s = min(reach(cells * n_lon, rows * n_lat, rows + k) + RIM, cells)
        if s >= SUB:
            begins = list(range(0, s - SUB + 1, SUB))
            if s % SUB:
                begins.append(s - SUB)
            shift = cells - s if side == TAIL else 0
            slots.append([(shift + b, at + b) for b in begins])
        elif side == TAIL:
            slots.append([(cells - SUB, at + s - SUB)])
        else:
            slots.append([(0, at)])
        at += s
    long = -(-(at - SUB) // SUB) * SUB
    return slots, long


def pack_room(rows, cells, n_lon, n_lat):
    return 2 * SUB + max(
        pack_plan(rows, cells, n_lon, n_lat, a, side)[1] for a in range(2) for side in (HEAD, TAIL)
    )


def paired(dims, *refs):
    levels, rows, cells, width, n_lon, n_lat, step, det = dims
    chunks = chunk_list(levels, rows, step)
    nq = len(chunks)
    per = rows // step
    tr, ad, shifts_in, fractions_in, mer_in, of, oa = refs[:7]
    gath = (refs[7 : 7 + nq], refs[7 + nq : 7 + 2 * nq])
    zb, ab, vb, taps, shifts, fractions, mer, held = refs[7 + 2 * nq : 15 + 2 * nq]
    sendp, recvp, sendx, recvx, loc, ssem, rsem, hs, hr, vs, vr, ps, pr = refs[15 + 2 * nq :]
    total_cells = cells * n_lon
    total_rows = rows * n_lat

    me = lax.axis_index("lon")
    lat = lax.axis_index("lat")
    first = lat * rows
    core = lax.rem(me, 2)
    partner = me + 1 - 2 * core
    beside = lax.rem(me + 2, n_lon)
    joint = lax.rem(me + n_lon + 2 * core - 1, n_lon)
    mate = lat + 1 - 2 * lax.rem(lat, 2)
    middle = jnp.logical_and(lat > 0, lat < n_lat - 1)
    polar = jnp.logical_not(middle)

    own = []
    dup = []
    for q, (lv, r0) in enumerate(chunks):
        a = pltpu.make_async_copy(
            tr.at[lv, pl.ds(r0, step)], gath[0][q].at[:, pl.ds(0, cells)], loc.at[q]
        )
        a.start()
        own.append(a)
    adc = pltpu.make_async_copy(ad, ab.at[:, pl.ds(RIM, rows)], loc.at[2 * nq])
    adc.start()
    small = []
    for k, (source, target) in enumerate(
        ((shifts_in, shifts), (fractions_in, fractions), (mer_in, mer))
    ):
        d = pltpu.make_async_copy(source, target, loc.at[2 * nq + 1 + k])
        d.start()
        small.append(d)
    for q, (lv, r0) in enumerate(chunks):
        b = pltpu.make_async_copy(
            tr.at[lv, pl.ds(r0, step)],
            gath[0][q].at[:, pl.ds(total_cells, cells)],
            loc.at[nq + q],
        )
        b.start()
        dup.append(b)

    barrier = pltpu.get_barrier_semaphore()

    def greet(**place):
        pl.semaphore_signal(barrier, inc=1, device_id=place, device_id_type=MESH)

    greet(lon=partner)
    greet(lon=beside)
    greet(lon=beside, lat=mate)

    @pl.when(lat > 0)
    def _():
        greet(lat=lat - 1)

    @pl.when(lat < n_lat - 1)
    def _():
        greet(lat=lat + 1)

    @pl.when(middle)
    def _():
        greet(lon=joint)
        pl.semaphore_wait(barrier, 6)

    @pl.when(polar)
    def _():
        pl.semaphore_wait(barrier, 4)

    def remote(source, target, send, recv, **place):
        return pltpu.make_async_remote_copy(
            source, target, send, recv, device_id=place, device_id_type=MESH
        )

    def lat_copies(buf, k):
        down = remote(
            buf.at[:, pl.ds(RIM, RIM)],
            buf.at[:, pl.ds(RIM + rows, RIM)],
            hs.at[k, 0],
            hr.at[k, 0],
            lat=lat - 1,
        )
        up = remote(
            buf.at[:, pl.ds(rows, RIM)], buf.at[:, pl.ds(0, RIM)], hs.at[k, 1], hr.at[k, 1], lat=lat + 1
        )
        return down, up

    def lat_start(buf, k):
        down, up = lat_copies(buf, k)

        @pl.when(lat > 0)
        def _():
            down.start()

        @pl.when(lat < n_lat - 1)
        def _():
            up.start()

    def lat_wait(buf, k):
        down, up = lat_copies(buf, k)

        @pl.when(lat > 0)
        def _():
            down.wait_send()
            up.wait_recv()

        @pl.when(lat < n_lat - 1)
        def _():
            up.wait_send()
            down.wait_recv()

    own_block = pl.ds(0, cells)
    far_block = pl.ds((n_lon - 2) * cells, cells)

    def x_copy(a, q):
        g = gath[a][q]
        return remote(
            g.at[:, own_block], g.at[:, far_block], ssem.at[a, q, 0], rsem.at[a, q, 0], lon=beside
        )

    def core_copy(a, q, dx):
        g = gath[a][q]
        source = ((n_lon - 2 * dx) % n_lon) * cells
        slot = lax.rem(2 * n_lon - 2 * dx + 2 * core - 1, n_lon)
        return remote(
            g.at[:, pl.ds(source, cells)],
            g.at[:, pl.ds(pl.multiple_of(slot * cells, SUB), cells)],
            ssem.at[a, q, 1 + dx],
            rsem.at[a, q, 1 + dx],
            lon=partner,
        )

    def out_copy(a, q):
        i = det[a].index(q)
        return remote(
            gath[a][q].at[:, own_block],
            held.at[a, i],
            vs.at[a, i, 0],
            vr.at[a, i, 0],
            lon=beside,
            lat=mate,
        )

    def on_copy(a, q):
        i = det[a].index(q)
        return remote(
            held.at[a, i], gath[a][q].at[:, far_block], vs.at[a, i, 1], vr.at[a, i, 1], lat=mate
        )

    def far_send(a, q):
        return out_copy(a, q) if q in det[a] else x_copy(a, q)

    def far_recv(a, q):
        return on_copy(a, q) if q in det[a] else x_copy(a, q)

    plans = [[pack_plan(rows, cells, n_lon, n_lat, a, side) for side in (HEAD, TAIL)] for a in range(2)]
    ring = (cells, (n_lon - 1) * cells)
    spill = [
        k for k in range(rows) if reach(total_cells, total_rows, rows + k) + RIM > cells
    ]
    last = (cells - SUB, 0)

    def place_of(lv, k, south):
        r = k if south else rows - 1 - k
        return lv * per + r // step, r % step

    def by_half(act):
        for south in (True, False):

            @pl.when(lat == (1 if south else n_lat - 2))
            def _():
                act(south)

    def pack_copy(a, lv, side):
        long = plans[a][side][1]
        return remote(
            sendp.at[a, lv, pl.ds(SUB, long)],
            recvp.at[a, lv, pl.ds(SUB, long)],
            ps.at[a, lv],
            pr.at[a, lv],
            lon=joint,
        )

    def few_copy(a):
        return remote(sendx.at[a], recvx.at[a], ps.at[a, levels], pr.at[a, levels], lon=beside)

    def pack_send(a, lv):
        for side in (HEAD, TAIL):

            @pl.when(core == side)
            def _():
                def fill(south):
                    order = range(rows) if side == HEAD else reversed(range(rows))
                    for k in order:
                        q, j = place_of(lv, k, south)
                        for source, target in plans[a][side][0][k]:
                            sendp[a, lv, pl.ds(target, SUB), :] = gath[a][q][j, pl.ds(source, SUB), :]

                by_half(fill)
                pack_copy(a, lv, side).start()

        if spill:

            def few(south):
                q, j = place_of(lv, spill[0], south)
                sendx[a, pl.ds(lv * SUB, SUB), :] = gath[a][q][j, pl.ds(last[a], SUB), :]

            by_half(few)
            if lv == levels - 1:
                few_copy(a).start()

    def pack_take(a, lv):
        for side in (HEAD, TAIL):

            @pl.when(core == 1 - side)
            def _():
                pack_copy(a, lv, side).wait_recv()

                def empty(south):
                    for k in range(rows):
                        q, j = place_of(lv, k, south)
                        for source, target in plans[a][side][0][k]:
                            gath[a][q][j, pl.ds(ring[side] + source, SUB), :] = recvp[
                                a, lv, pl.ds(target, SUB), :
                            ]

                by_half(empty)

        if spill:
            if lv == 0:
                few_copy(a).wait_recv()

            def few(south):
                q, j = place_of(lv, spill[0], south)
                gath[a][q][j, pl.ds(2 * cells + last[a], SUB), :] = recvx[a, pl.ds(lv * SUB, SUB), :]

            by_half(few)

    def pass_on(a, q):
        out_copy(a, q).wait_recv()
        on_copy(a, q).start()

    def send_level(a, lv):
        for q in range(lv * per, (lv + 1) * per):
            core_copy(a, q, 0).start()

            @pl.when(polar)
            def _():
                far_send(a, q).start()

        @pl.when(middle)
        def _():
            pack_send(a, lv)

    adc.wait()
    lat_start(ab, 0)
    for lv in range(levels):
        for q in range(lv * per, (lv + 1) * per):
            own[q].wait()
        send_level(0, lv)

    @pl.when(lat == 0)
    def _():
        for buf in (ab, zb):
            buf[:, pl.ds(0, RIM)] = jnp.zeros((levels, RIM, cells, width), jnp.float32)

    @pl.when(lat == n_lat - 1)
    def _():
        for buf in (ab, zb):
            buf[:, pl.ds(RIM + rows, RIM)] = jnp.zeros((levels, RIM, cells, width), jnp.float32)

    for d in small:
        d.wait()
    faces = rows + 5
    lanes = lax.broadcasted_iota(jnp.int32, (cells, total_rows), 1)
    for lv in range(levels):

        @pl.loop(0, faces)
        def _(f):
            row = first + f - 2
            chosen = jnp.logical_and(lanes == row, lanes > 0)
            column = jnp.sum(jnp.where(chosen, mer[lv], 0.0), axis=1, keepdims=True)
            vb[lv, f] = jnp.broadcast_to(column, (cells, width))

        @pl.loop(0, rows)
        def _(r):
            for k, t in enumerate(zonal_taps(fractions[lv, first + r])):
                taps[(lv * rows + r) * 6 + k] = t

    lat_wait(ab, 0)
    for lv in range(levels):

        @pl.loop(0, cells // SUB)
        def _(c):
            at = pl.ds(pl.multiple_of(c * SUB, SUB), SUB)
            ev, q6b, dqb, eb = {}, {}, {}, {}
            carry = None
            y = {r: ab[lv, r + RIM, at, :] for r in range(-3, -1)}
            for f in range(-2, rows + 3):
                y[f] = ab[lv, f + RIM, at, :]
                v = vb[lv, f + 2, at, :]
                north = v > 0.0
                beta, gamma = face_terms(v)
                change = y[f] - y[f - 1]
                ev[f] = v * change
                b = beta * change
                g = -gamma * change
                bn, gn = jnp.where(north, b, 0.0), jnp.where(north, g, 0.0)
                if carry is not None:
                    q6b[f - 1] = bn + carry[0]
                    dqb[f - 1] = gn + carry[1]
                carry = (b - bn, g - gn)
                h = f - 1
                if h >= -1:
                    eb[h] = ev[h] - 3.0 * (q6b[h - 1] + q6b[h]) + (dqb[h - 1] - dqb[h])
                r = h - 2
                if r >= 0:
                    value = (
                        y[r]
                        + 6.0 * q6b[r]
                        + (7.0 / 12.0) * (eb[r] + eb[r + 1])
                        - (1.0 / 12.0) * (eb[r - 1] + eb[r + 2])
                    )
                    q = lv * per + r // step
                    gath[1][q][r % step, at, :] = value
                    gath[1][q][
                        r % step, pl.ds(pl.multiple_of(total_cells + c * SUB, SUB), SUB), :
                    ] = value

        send_level(1, lv)

    def sweep(a, q, sink, sink_row, sign):
        lv, r0 = chunks[q]
        buf = gath[a][q]

        @pl.loop(0, step)
        def _(r):
            buf[r, pl.ds(total_cells + cells, SUB), :] = buf[r, pl.ds(cells, SUB), :]
            shift = shifts[lv, first + r0 + r]
            if sign < 0:
                start = lax.rem(2 * total_cells - shift - 3, total_cells)
            else:
                start = lax.rem(2 * total_cells + shift - 2, total_cells)
            base = (lv * rows + r0 + r) * 6
            w = [taps[base + k] for k in range(6)]
            if sign > 0:
                w = w[::-1]
            for c in range(cells // SUB):
                total = None
                for k in range(6):
                    term = w[k] * buf[r, pl.ds(start + c * SUB + k, SUB), :]
                    total = term if total is None else total + term
                sink[lv, sink_row + r0 + r, pl.ds(c * SUB, SUB), :] = total

    def finish(a, q):
        for dx in range(2):
            core_copy(a, q, dx).wait_recv()
        if a == 0:
            sweep(0, q, zb, RIM, -1)
        else:
            sweep(1, q, oa, 0, 1)

    def relay(a, q):
        far_recv(a, q).wait_recv()
        core_copy(a, q, 1).start()

    def polar_finish(a):
        order = [q for q in range(nq) if q not in det[a]] + list(det[a])
        for i, q in enumerate(order):
            relay(a, q)
            if i > 0:
                finish(a, order[i - 1])
        finish(a, order[-1])

    def middle_finish(a):
        for lv in range(levels):
            pack_take(a, lv)
            for q in range(lv * per, (lv + 1) * per):
                core_copy(a, q, 0).wait_recv()
                if a == 0:
                    sweep(0, q, zb, RIM, -1)
                else:
                    sweep(1, q, oa, 0, 1)

    for b in dup:
        b.wait()

    @pl.when(polar)
    def _():
        polar_finish(0)

    @pl.when(middle)
    def _():
        middle_finish(0)

    lat_start(zb, 1)

    @pl.when(middle)
    def _():
        for q in det[0]:
            pass_on(0, q)
        middle_finish(1)
        for q in det[1]:
            pass_on(1, q)

    lat_wait(zb, 1)

    for lv in range(levels):

        @pl.loop(0, cells // SUB)
        def _(c):
            at = pl.ds(pl.multiple_of(c * SUB, SUB), SUB)
            z = {r: zb[lv, r + RIM, at, :] for r in range(-3, 0)}
            e, q6, dq, flux = {}, {}, {}, {}
            for f in range(-1, rows + 2):
                z[f + 1] = zb[lv, f + 1 + RIM, at, :]
                e[f] = (7.0 / 12.0) * (z[f - 1] + z[f]) - (1.0 / 12.0) * (z[f - 2] + z[f + 1])
                u = f - 1
                if u >= -1:
                    q6[u] = 6.0 * z[u] - 3.0 * (e[u] + e[f])
                    dq[u] = e[f] - e[u]
                if u >= 0:
                    v = vb[lv, u + 2, at, :]
                    north = v > 0.0
                    beta, gamma = face_terms(v)
                    flux[u] = (
                        v * e[u]
                        + beta * jnp.where(north, q6[u - 1], q6[u])
                        - gamma * jnp.where(north, dq[u - 1], dq[u])
                    )
                if u >= 1:
                    of[lv, u - 1, at, :] = z[u - 1] - flux[u] + flux[u - 1]

    @pl.when(polar)
    def _():
        polar_finish(1)

    for a in range(2):
        for q in range(nq):
            core_copy(a, q, 0).wait_send()

            @pl.when(polar)
            def _():
                far_send(a, q).wait_send()
                core_copy(a, q, 1).wait_send()

        @pl.when(middle)
        def _():
            for q in det[a]:
                on_copy(a, q).wait_send()
            for lv in range(levels):
                for side in (HEAD, TAIL):

                    @pl.when(core == side)
                    def _():
                        pack_copy(a, lv, side).wait_send()

            if spill:
                few_copy(a).wait_send()


def store(f_in, a_in, f_out, a_out, sem):
    one = pltpu.make_async_copy(f_in, f_out, sem.at[0])
    two = pltpu.make_async_copy(a_in, a_out, sem.at[1])
    one.start()
    two.start()
    one.wait()
    two.wait()


def local(tracers, adjoint_in, shifts, fractions, meridional):
    levels, rows, cells, width = tracers.shape
    n_lon, n_lat = lax.axis_size("lon"), lax.axis_size("lat")
    n_x = n_lon // 2
    pair = fits(rows, cells, n_lon, n_lat)
    step = max(1, rows // (4 if pair else 2))
    nq = levels * (rows // step)
    dma = pltpu.SemaphoreType.DMA
    block = pltpu.VMEM((step, (n_lon + 1) * cells + SUB, width), jnp.float32)
    banded = pltpu.VMEM((levels, rows + 2 * RIM, cells, width), jnp.float32)
    scratch = [block] * (2 * nq) + [
        banded,
        banded,
        pltpu.VMEM((levels, rows + 5, cells, width), jnp.float32),
        pltpu.SMEM((levels * rows * 6,), jnp.float32),
        pltpu.SMEM(shifts.shape, jnp.int32),
        pltpu.SMEM(fractions.shape, jnp.float32),
        pltpu.VMEM((levels, cells, meridional.shape[1]), jnp.float32),
    ]
    if pair:
        det = detours(levels, rows, step)
        nd = max(len(d) for d in det)
        dims = (levels, rows, cells, width, n_lon, n_lat, step, det)
        long = pack_room(rows, cells, n_lon, n_lat)
        pack = pltpu.VMEM((2, levels, long, width), jnp.float32)
        few = pltpu.VMEM((2, levels * SUB, width), jnp.float32)
        body = paired
        scratch += [
            pltpu.VMEM((2, nd, step, cells, width), jnp.float32),
            pack,
            pack,
            few,
            few,
            dma((2 * nq + 4,)),
            dma((2, nq, 3)),
            dma((2, nq, 3)),
            dma((2, 2)),
            dma((2, 2)),
            dma((2, nd, 2)),
            dma((2, nd, 2)),
            dma((2, levels + 1)),
            dma((2, levels + 1)),
        ]
    else:
        dims = (levels, rows, cells, width, n_lon, n_lat, step)
        body = general
        scratch += [
            dma((2 * nq + 4,)),
            dma((2, nq, 2 * n_x)),
            dma((2, nq, 2 * n_x)),
            dma((2, 2)),
            dma((2, 2)),
        ]
    vmem = pl.BlockSpec(memory_space=pltpu.VMEM)
    far = pl.BlockSpec(memory_space=pltpu.HBM)
    kept = pltpu.VMEM(tracers.shape, jnp.float32)
    staged = pl.pallas_call(
        functools.partial(body, dims),
        out_shape=(kept, kept),
        in_specs=[far] * 5,
        out_specs=(vmem, vmem),
        scratch_shapes=scratch,
        compiler_params=pltpu.CompilerParams(
            collective_id=0, has_side_effects=True, vmem_limit_bytes=60 << 20
        ),
    )(tracers, adjoint_in, shifts, fractions, jnp.swapaxes(meridional, 1, 2))
    final = jax.ShapeDtypeStruct(tracers.shape, jnp.float32)
    return pl.pallas_call(
        store,
        out_shape=(final, final),
        in_specs=[vmem, vmem],
        out_specs=(far, far),
        scratch_shapes=[dma((2,))],
        compiler_params=pltpu.CompilerParams(vmem_limit_bytes=4 << 20),
    )(*staged)


def solution(mesh):
    block = P("grp", "lat", "lon", None)
    in_specs = (block, block, P(), P(), P(None, None, "lon"))
    return jax.shard_map(
        local, mesh=mesh, in_specs=in_specs, out_specs=(block, block), check_vma=False
    )
```

```python
import functools

import jax
import jax.numpy as jnp
from jax import lax
from jax.experimental import pallas as pl
from jax.experimental.pallas import tpu as pltpu
from jax.sharding import PartitionSpec as P

MESH = pl.DeviceIdType.MESH
SUB = 8
RIM = 3
LAG = 2
LATE = 4
HEAD, TAIL = 0, 1


def chunk_list(levels, rows, step):
    return [(lv, r0) for lv in range(levels) for r0 in range(0, rows, step)]


def reach(total_cells, total_rows, row):
    d = abs(2 * row + 1 - total_rows)
    return (total_cells - 1) * d * d // ((total_rows - 1) * (total_rows - 1))


def face_terms(v):
    size = jnp.abs(v)
    beta = v * (0.5 * size) * (1.0 - size * (2.0 / 3.0))
    return beta, 0.5 * v * v


def zonal_taps(c):
    b = 1.0 - c * (2.0 / 3.0)
    p = c * (1.0 - 0.5 * c - 1.5 * c * b)
    q = c * (0.5 * c - 1.5 * c * b)
    r = 3.0 * c * c * b
    d = p - q
    t = 1.0 / 12.0
    s = 7.0 / 12.0
    return (
        -t * q,
        s * q - t * d,
        r + t * p + s * d + s * q,
        1.0 - r - s * p + s * d - t * q,
        -s * p - t * d,
        t * p,
    )


def general(dims, *refs):
    levels, rows, cells, width, n_lon, n_lat, step = dims
    chunks = chunk_list(levels, rows, step)
    nq = len(chunks)
    tr, ad, shifts_in, fractions_in, mer_in, of, oa = refs[:7]
    gath = (refs[7 : 7 + nq], refs[7 + nq : 7 + 2 * nq])
    zb, ab, vb, taps, shifts, fractions, mer, loc, ssem, rsem, hs, hr = refs[7 + 2 * nq :]
    total_cells = cells * n_lon
    total_rows = rows * n_lat
    n_x = n_lon // 2

    me = lax.axis_index("lon")
    lat = lax.axis_index("lat")
    first = lat * rows
    core = lax.rem(me, 2)
    partner = me + 1 - 2 * core
    order = list(range(nq))

    own = []
    dup = []
    for q, (lv, r0) in enumerate(chunks):
        a = pltpu.make_async_copy(
            tr.at[lv, pl.ds(r0, step)], gath[0][q].at[:, pl.ds(0, cells)], loc.at[q]
        )
        a.start()
        own.append(a)
    adc = pltpu.make_async_copy(ad, ab.at[:, pl.ds(RIM, rows)], loc.at[2 * nq])
    adc.start()
    for q, (lv, r0) in enumerate(chunks):
        b = pltpu.make_async_copy(
            tr.at[lv, pl.ds(r0, step)],
            gath[0][q].at[:, pl.ds(total_cells, cells)],
            loc.at[nq + q],
        )
        b.start()
        dup.append(b)

    small = []
    for k, (source, target) in enumerate(
        ((shifts_in, shifts), (fractions_in, fractions), (mer_in, mer))
    ):
        d = pltpu.make_async_copy(source, target, loc.at[2 * nq + 1 + k])
        d.start()
        small.append(d)

    barrier = pltpu.get_barrier_semaphore()
    pl.semaphore_signal(barrier, inc=1, device_id={"lon": partner}, device_id_type=MESH)
    for dx in range(1, n_x):
        pl.semaphore_signal(
            barrier, inc=1, device_id={"lon": lax.rem(me + 2 * dx, n_lon)}, device_id_type=MESH
        )

    @pl.when(lat > 0)
    def _():
        pl.semaphore_signal(barrier, inc=1, device_id={"lat": lat - 1}, device_id_type=MESH)

    @pl.when(lat < n_lat - 1)
    def _():
        pl.semaphore_signal(barrier, inc=1, device_id={"lat": lat + 1}, device_id_type=MESH)

    inner = jnp.logical_and(lat > 0, lat < n_lat - 1)

    @pl.when(inner)
    def _():
        pl.semaphore_wait(barrier, n_x + 2)

    @pl.when(jnp.logical_not(inner))
    def _():
        pl.semaphore_wait(barrier, n_x + min(n_lat - 1, 1))

    def lat_copies(buf, k):
        down = pltpu.make_async_remote_copy(
            buf.at[:, pl.ds(RIM, RIM)],
            buf.at[:, pl.ds(RIM + rows, RIM)],
            hs.at[k, 0],
            hr.at[k, 0],
            device_id={"lat": lat - 1},
            device_id_type=MESH,
        )
        up = pltpu.make_async_remote_copy(
            buf.at[:, pl.ds(rows, RIM)],
            buf.at[:, pl.ds(0, RIM)],
            hs.at[k, 1],
            hr.at[k, 1],
            device_id={"lat": lat + 1},
            device_id_type=MESH,
        )
        return down, up

    def lat_start(buf, k):
        down, up = lat_copies(buf, k)

        @pl.when(lat > 0)
        def _():
            down.start()

        @pl.when(lat < n_lat - 1)
        def _():
            up.start()

    def lat_wait(buf, k):
        down, up = lat_copies(buf, k)

        @pl.when(lat > 0)
        def _():
            down.wait_send()
            up.wait_recv()

        @pl.when(lat < n_lat - 1)
        def _():
            up.wait_send()
            down.wait_recv()

    def x_copy(a, q, dx, span):
        lo, hi = span
        return pltpu.make_async_remote_copy(
            gath[a][q].at[:, pl.ds(lo, hi - lo)],
            gath[a][q].at[:, pl.ds((n_lon - 2 * dx) * cells + lo, hi - lo)],
            ssem.at[a, q, dx],
            rsem.at[a, q, dx],
            device_id={"lon": lax.rem(me + 2 * dx, n_lon)},
            device_id_type=MESH,
        )

    def core_copy(a, q, dx, span):
        lo, hi = span
        source = ((n_lon - 2 * dx) % n_lon) * cells + lo
        slot = lax.rem(2 * n_lon - 2 * dx + 2 * core - 1, n_lon)
        return pltpu.make_async_remote_copy(
            gath[a][q].at[:, pl.ds(source, hi - lo)],
            gath[a][q].at[:, pl.ds(pl.multiple_of(slot * cells + lo, SUB), hi - lo)],
            ssem.at[a, q, n_x + dx],
            rsem.at[a, q, n_x + dx],
            device_id={"lon": partner},
            device_id_type=MESH,
        )

    whole = (0, cells)

    def gather_start(a, q):
        for dx in range(1, n_x):
            x_copy(a, q, dx, whole).start()
        core_copy(a, q, 0, whole).start()

    def relay(a, q):
        for dx in range(1, n_x):
            x_copy(a, q, dx, whole).wait_recv()
            core_copy(a, q, dx, whole).start()

    def gather_finish(a, q):
        for dx in range(n_x):
            core_copy(a, q, dx, whole).wait_recv()

    def gather_drain(a, q):
        for dx in range(n_x):
            core_copy(a, q, dx, whole).wait_send()
        for dx in range(1, n_x):
            x_copy(a, q, dx, whole).wait_send()

    adc.wait()
    lat_start(ab, 0)
    for q in range(nq):
        own[q].wait()
        gather_start(0, q)

    @pl.when(lat == 0)
    def _():
        for buf in (ab, zb):
            buf[:, pl.ds(0, RIM)] = jnp.zeros((levels, RIM, cells, width), jnp.float32)

    @pl.when(lat == n_lat - 1)
    def _():
        for buf in (ab, zb):
            buf[:, pl.ds(RIM + rows, RIM)] = jnp.zeros((levels, RIM, cells, width), jnp.float32)

    for d in small:
        d.wait()
    faces = rows + 5
    lanes = lax.broadcasted_iota(jnp.int32, (cells, total_rows), 1)
    for lv in range(levels):

        @pl.loop(0, faces)
        def _(f):
            row = first + f - 2
            chosen = jnp.logical_and(lanes == row, lanes > 0)
            column = jnp.sum(jnp.where(chosen, mer[lv], 0.0), axis=1, keepdims=True)
            vb[lv, f] = jnp.broadcast_to(column, (cells, width))

        @pl.loop(0, rows)
        def _(r):
            for k, t in enumerate(zonal_taps(fractions[lv, first + r])):
                taps[(lv * rows + r) * 6 + k] = t

    lat_wait(ab, 0)
    for lv in range(levels):

        @pl.loop(0, cells // SUB)
        def _(c):
            at = pl.ds(pl.multiple_of(c * SUB, SUB), SUB)
            ev, q6b, dqb, eb = {}, {}, {}, {}
            carry = None
            y = {r: ab[lv, r + RIM, at, :] for r in range(-3, -1)}
            for f in range(-2, rows + 3):
                y[f] = ab[lv, f + RIM, at, :]
                v = vb[lv, f + 2, at, :]
                north = v > 0.0
                beta, gamma = face_terms(v)
                change = y[f] - y[f - 1]
                ev[f] = v * change
                b = beta * change
                g = -gamma * change
                bn, gn = jnp.where(north, b, 0.0), jnp.where(north, g, 0.0)
                if carry is not None:
                    q6b[f - 1] = bn + carry[0]
                    dqb[f - 1] = gn + carry[1]
                carry = (b - bn, g - gn)
                h = f - 1
                if h >= -1:
                    eb[h] = ev[h] - 3.0 * (q6b[h - 1] + q6b[h]) + (dqb[h - 1] - dqb[h])
                r = h - 2
                if r >= 0:
                    value = (
                        y[r]
                        + 6.0 * q6b[r]
                        + (7.0 / 12.0) * (eb[r] + eb[r + 1])
                        - (1.0 / 12.0) * (eb[r - 1] + eb[r + 2])
                    )
                    q = lv * (rows // step) + r // step
                    gath[1][q][r % step, at, :] = value
                    gath[1][q][
                        r % step, pl.ds(pl.multiple_of(total_cells + c * SUB, SUB), SUB), :
                    ] = value

        for q, (l2, _r) in enumerate(chunks):
            if l2 == lv:
                gather_start(1, q)

    def sweep(a, q, sink, sink_row, sign):
        lv, r0 = chunks[q]
        buf = gath[a][q]

        @pl.loop(0, step)
        def _(r):
            buf[r, pl.ds(total_cells + cells, SUB), :] = buf[r, pl.ds(cells, SUB), :]
            shift = shifts[lv, first + r0 + r]
            if sign < 0:
                start = lax.rem(2 * total_cells - shift - 3, total_cells)
            else:
                start = lax.rem(2 * total_cells + shift - 2, total_cells)
            base = (lv * rows + r0 + r) * 6
            w = [taps[base + k] for k in range(6)]
            if sign > 0:
                w = w[::-1]
            for c in range(cells // SUB):
                total = None
                for k in range(6):
                    term = w[k] * buf[r, pl.ds(start + c * SUB + k, SUB), :]
                    total = term if total is None else total + term
                sink[lv, sink_row + r0 + r, pl.ds(c * SUB, SUB), :] = total

    for b in dup:
        b.wait()
    for i, q in enumerate(order):
        relay(0, q)
        if i > 0:
            gather_finish(0, order[i - 1])
            sweep(0, order[i - 1], zb, RIM, -1)
    gather_finish(0, order[-1])
    sweep(0, order[-1], zb, RIM, -1)
    lat_start(zb, 1)

    relay(1, order[0])
    lat_wait(zb, 1)

    for lv in range(levels):

        @pl.loop(0, cells // SUB)
        def _(c):
            at = pl.ds(pl.multiple_of(c * SUB, SUB), SUB)
            z = {r: zb[lv, r + RIM, at, :] for r in range(-3, 0)}
            e, q6, dq, flux = {}, {}, {}, {}
            for f in range(-1, rows + 2):
                z[f + 1] = zb[lv, f + 1 + RIM, at, :]
                e[f] = (7.0 / 12.0) * (z[f - 1] + z[f]) - (1.0 / 12.0) * (z[f - 2] + z[f + 1])
                u = f - 1
                if u >= -1:
                    q6[u] = 6.0 * z[u] - 3.0 * (e[u] + e[f])
                    dq[u] = e[f] - e[u]
                if u >= 0:
                    v = vb[lv, u + 2, at, :]
                    north = v > 0.0
                    beta, gamma = face_terms(v)
                    flux[u] = (
                        v * e[u]
                        + beta * jnp.where(north, q6[u - 1], q6[u])
                        - gamma * jnp.where(north, dq[u - 1], dq[u])
                    )
                if u >= 1:
                    of[lv, u - 1, at, :] = z[u - 1] - flux[u] + flux[u - 1]

    def finish_adjoint(q):
        lv, r0 = chunks[q]
        gather_finish(1, q)
        sweep(1, q, oa, 0, 1)

    for i in range(1, nq):
        relay(1, order[i])
        finish_adjoint(order[i - 1])
    finish_adjoint(order[-1])

    for a in range(2):
        for q in range(nq):
            gather_drain(a, q)


def fits(rows, cells, n_lon, n_lat):
    if n_lon != 4 or n_lat != 4 or rows % 4 or cells % SUB:
        return False
    return reach(cells * n_lon, rows * n_lat, rows) + RIM <= cells + SUB


def detours(levels, rows, step):
    per = rows // step
    return ((), (1, 2, 3, per + 1, per + 2, per + 3))


def pack_plan(rows, cells, n_lon, n_lat, a, side):
    big = (side == TAIL) == (a == 0)
    slots = []
    at = SUB
    for k in range(rows):
        s = RIM - 1
        if big:
            s = min(reach(cells * n_lon, rows * n_lat, rows + k) + RIM, cells)
        if s >= SUB:
            begins = list(range(0, s - SUB + 1, SUB))
            if s % SUB:
                begins.append(s - SUB)
            shift = cells - s if side == TAIL else 0
            slots.append([(shift + b, at + b) for b in begins])
        elif side == TAIL:
            slots.append([(cells - SUB, at + s - SUB)])
        else:
            slots.append([(0, at)])
        at += s
    long = -(-(at - SUB) // SUB) * SUB
    return slots, long


def pack_room(rows, cells, n_lon, n_lat):
    return 2 * SUB + max(
        pack_plan(rows, cells, n_lon, n_lat, a, side)[1] for a in range(2) for side in (HEAD, TAIL)
    )


def paired(dims, *refs):
    levels, rows, cells, width, n_lon, n_lat, step, det = dims
    chunks = chunk_list(levels, rows, step)
    nq = len(chunks)
    per = rows // step
    tr, ad, shifts_in, fractions_in, mer_in, of, oa = refs[:7]
    gath = (refs[7 : 7 + nq], refs[7 + nq : 7 + 2 * nq])
    zb, ab, vb, taps, shifts, fractions, mer, held = refs[7 + 2 * nq : 15 + 2 * nq]
    sendp, recvp, sendx, recvx, loc, ssem, rsem, hs, hr, vs, vr, ps, pr = refs[15 + 2 * nq :]
    total_cells = cells * n_lon
    total_rows = rows * n_lat

    me = lax.axis_index("lon")
    lat = lax.axis_index("lat")
    first = lat * rows
    core = lax.rem(me, 2)
    partner = me + 1 - 2 * core
    beside = lax.rem(me + 2, n_lon)
    joint = lax.rem(me + n_lon + 2 * core - 1, n_lon)
    mate = lat + 1 - 2 * lax.rem(lat, 2)
    middle = jnp.logical_and(lat > 0, lat < n_lat - 1)
    polar = jnp.logical_not(middle)

    own = []
    dup = []
    for q, (lv, r0) in enumerate(chunks):
        a = pltpu.make_async_copy(
            tr.at[lv, pl.ds(r0, step)], gath[0][q].at[:, pl.ds(0, cells)], loc.at[q]
        )
        a.start()
        own.append(a)
    adc = pltpu.make_async_copy(ad, ab.at[:, pl.ds(RIM, rows)], loc.at[2 * nq])
    adc.start()
    small = []
    for k, (source, target) in enumerate(
        ((shifts_in, shifts), (fractions_in, fractions), (mer_in, mer))
    ):
        d = pltpu.make_async_copy(source, target, loc.at[2 * nq + 1 + k])
        d.start()
        small.append(d)
    for q, (lv, r0) in enumerate(chunks):
        b = pltpu.make_async_copy(
            tr.at[lv, pl.ds(r0, step)],
            gath[0][q].at[:, pl.ds(total_cells, cells)],
            loc.at[nq + q],
        )
        b.start()
        dup.append(b)

    barrier = pltpu.get_barrier_semaphore()

    def greet(**place):
        pl.semaphore_signal(barrier, inc=1, device_id=place, device_id_type=MESH)

    greet(lon=partner)
    greet(lon=beside)
    greet(lon=beside, lat=mate)

    @pl.when(lat > 0)
    def _():
        greet(lat=lat - 1)

    @pl.when(lat < n_lat - 1)
    def _():
        greet(lat=lat + 1)

    @pl.when(middle)
    def _():
        greet(lon=joint)
        pl.semaphore_wait(barrier, 6)

    @pl.when(polar)
    def _():
        pl.semaphore_wait(barrier, 4)

    def remote(source, target, send, recv, **place):
        return pltpu.make_async_remote_copy(
            source, target, send, recv, device_id=place, device_id_type=MESH
        )

    def lat_copies(buf, k):
        down = remote(
            buf.at[:, pl.ds(RIM, RIM)],
            buf.at[:, pl.ds(RIM + rows, RIM)],
            hs.at[k, 0],
            hr.at[k, 0],
            lat=lat - 1,
        )
        up = remote(
            buf.at[:, pl.ds(rows, RIM)], buf.at[:, pl.ds(0, RIM)], hs.at[k, 1], hr.at[k, 1], lat=lat + 1
        )
        return down, up

    def lat_start(buf, k):
        down, up = lat_copies(buf, k)

        @pl.when(lat > 0)
        def _():
            down.start()

        @pl.when(lat < n_lat - 1)
        def _():
            up.start()

    def lat_wait(buf, k):
        down, up = lat_copies(buf, k)

        @pl.when(lat > 0)
        def _():
            down.wait_send()
            up.wait_recv()

        @pl.when(lat < n_lat - 1)
        def _():
            up.wait_send()
            down.wait_recv()

    own_block = pl.ds(0, cells)
    far_block = pl.ds((n_lon - 2) * cells, cells)

    def x_copy(a, q):
        g = gath[a][q]
        return remote(
            g.at[:, own_block], g.at[:, far_block], ssem.at[a, q, 0], rsem.at[a, q, 0], lon=beside
        )

    def core_copy(a, q, dx):
        g = gath[a][q]
        source = ((n_lon - 2 * dx) % n_lon) * cells
        slot = lax.rem(2 * n_lon - 2 * dx + 2 * core - 1, n_lon)
        return remote(
            g.at[:, pl.ds(source, cells)],
            g.at[:, pl.ds(pl.multiple_of(slot * cells, SUB), cells)],
            ssem.at[a, q, 1 + dx],
            rsem.at[a, q, 1 + dx],
            lon=partner,
        )

    def out_copy(a, q):
        i = det[a].index(q)
        return remote(
            gath[a][q].at[:, own_block],
            held.at[a, i],
            vs.at[a, i, 0],
            vr.at[a, i, 0],
            lon=beside,
            lat=mate,
        )

    def on_copy(a, q):
        i = det[a].index(q)
        return remote(
            held.at[a, i], gath[a][q].at[:, far_block], vs.at[a, i, 1], vr.at[a, i, 1], lat=mate
        )

    def far_send(a, q):
        return out_copy(a, q) if q in det[a] else x_copy(a, q)

    def far_recv(a, q):
        return on_copy(a, q) if q in det[a] else x_copy(a, q)

    plans = [[pack_plan(rows, cells, n_lon, n_lat, a, side) for side in (HEAD, TAIL)] for a in range(2)]
    ring = (cells, (n_lon - 1) * cells)
    spill = [
        k for k in range(rows) if reach(total_cells, total_rows, rows + k) + RIM > cells
    ]
    last = (cells - SUB, 0)

    def place_of(lv, k, south):
        r = k if south else rows - 1 - k
        return lv * per + r // step, r % step

    def by_half(act):
        for south in (True, False):

            @pl.when(lat == (1 if south else n_lat - 2))
            def _():
                act(south)

    def pack_copy(a, lv, side):
        long = plans[a][side][1]
        return remote(
            sendp.at[a, lv, pl.ds(SUB, long)],
            recvp.at[a, lv, pl.ds(SUB, long)],
            ps.at[a, lv],
            pr.at[a, lv],
            lon=joint,
        )

    def few_copy(a):
        return remote(sendx.at[a], recvx.at[a], ps.at[a, levels], pr.at[a, levels], lon=beside)

    def pack_send(a, lv):
        for side in (HEAD, TAIL):

            @pl.when(core == side)
            def _():
                def fill(south):
                    order = range(rows) if side == HEAD else reversed(range(rows))
                    for k in order:
                        q, j = place_of(lv, k, south)
                        for source, target in plans[a][side][0][k]:
                            sendp[a, lv, pl.ds(target, SUB), :] = gath[a][q][j, pl.ds(source, SUB), :]

                by_half(fill)
                pack_copy(a, lv, side).start()

        if spill:

            def few(south):
                q, j = place_of(lv, spill[0], south)
                sendx[a, pl.ds(lv * SUB, SUB), :] = gath[a][q][j, pl.ds(last[a], SUB), :]

            by_half(few)
            if lv == levels - 1:
                few_copy(a).start()

    def pack_take(a, lv):
        for side in (HEAD, TAIL):

            @pl.when(core == 1 - side)
            def _():
                pack_copy(a, lv, side).wait_recv()

                def empty(south):
                    for k in range(rows):
                        q, j = place_of(lv, k, south)
                        for source, target in plans[a][side][0][k]:
                            gath[a][q][j, pl.ds(ring[side] + source, SUB), :] = recvp[
                                a, lv, pl.ds(target, SUB), :
                            ]

                by_half(empty)

        if spill:
            if lv == 0:
                few_copy(a).wait_recv()

            def few(south):
                q, j = place_of(lv, spill[0], south)
                gath[a][q][j, pl.ds(2 * cells + last[a], SUB), :] = recvx[a, pl.ds(lv * SUB, SUB), :]

            by_half(few)

    def pass_on(a, q):
        out_copy(a, q).wait_recv()
        on_copy(a, q).start()

    def send_level(a, lv):
        for q in range(lv * per, (lv + 1) * per):
            core_copy(a, q, 0).start()

            @pl.when(polar)
            def _():
                far_send(a, q).start()

        @pl.when(middle)
        def _():
            pack_send(a, lv)

    adc.wait()
    lat_start(ab, 0)
    for lv in range(levels):
        for q in range(lv * per, (lv + 1) * per):
            own[q].wait()
        send_level(0, lv)

    @pl.when(lat == 0)
    def _():
        for buf in (ab, zb):
            buf[:, pl.ds(0, RIM)] = jnp.zeros((levels, RIM, cells, width), jnp.float32)

    @pl.when(lat == n_lat - 1)
    def _():
        for buf in (ab, zb):
            buf[:, pl.ds(RIM + rows, RIM)] = jnp.zeros((levels, RIM, cells, width), jnp.float32)

    for d in small:
        d.wait()
    faces = rows + 5
    lanes = lax.broadcasted_iota(jnp.int32, (cells, total_rows), 1)
    for lv in range(levels):

        @pl.loop(0, faces, unroll=faces)
        def _(f):
            row = first + f - 2
            chosen = jnp.logical_and(lanes == row, lanes > 0)
            column = jnp.sum(jnp.where(chosen, mer[lv], 0.0), axis=1, keepdims=True)
            vb[lv, f] = jnp.broadcast_to(column, (cells, width))

        @pl.loop(0, rows)
        def _(r):
            for k, t in enumerate(zonal_taps(fractions[lv, first + r])):
                taps[(lv * rows + r) * 6 + k] = t

    lat_wait(ab, 0)
    for lv in range(levels):

        @pl.loop(0, cells // SUB)
        def _(c):
            at = pl.ds(pl.multiple_of(c * SUB, SUB), SUB)
            ev, q6b, dqb, eb = {}, {}, {}, {}
            carry = None
            y = {r: ab[lv, r + RIM, at, :] for r in range(-3, -1)}
            for f in range(-2, rows + 3):
                y[f] = ab[lv, f + RIM, at, :]
                v = vb[lv, f + 2, at, :]
                north = v > 0.0
                beta, gamma = face_terms(v)
                change = y[f] - y[f - 1]
                ev[f] = v * change
                b = beta * change
                g = -gamma * change
                bn, gn = jnp.where(north, b, 0.0), jnp.where(north, g, 0.0)
                if carry is not None:
                    q6b[f - 1] = bn + carry[0]
                    dqb[f - 1] = gn + carry[1]
                carry = (b - bn, g - gn)
                h = f - 1
                if h >= -1:
                    eb[h] = ev[h] - 3.0 * (q6b[h - 1] + q6b[h]) + (dqb[h - 1] - dqb[h])
                r = h - 2
                if r >= 0:
                    value = (
                        y[r]
                        + 6.0 * q6b[r]
                        + (7.0 / 12.0) * (eb[r] + eb[r + 1])
                        - (1.0 / 12.0) * (eb[r - 1] + eb[r + 2])
                    )
                    q = lv * per + r // step
                    gath[1][q][r % step, at, :] = value
                    gath[1][q][
                        r % step, pl.ds(pl.multiple_of(total_cells + c * SUB, SUB), SUB), :
                    ] = value

        send_level(1, lv)

    def sweep(a, q, sink, sink_row, sign):
        lv, r0 = chunks[q]
        buf = gath[a][q]

        @pl.loop(0, step)
        def _(r):
            buf[r, pl.ds(total_cells + cells, SUB), :] = buf[r, pl.ds(cells, SUB), :]
            shift = shifts[lv, first + r0 + r]
            if sign < 0:
                start = lax.rem(2 * total_cells - shift - 3, total_cells)
            else:
                start = lax.rem(2 * total_cells + shift - 2, total_cells)
            base = (lv * rows + r0 + r) * 6
            w = [taps[base + k] for k in range(6)]
            if sign > 0:
                w = w[::-1]
            for c in range(cells // SUB):
                total = None
                for k in range(6):
                    term = w[k] * buf[r, pl.ds(start + c * SUB + k, SUB), :]
                    total = term if total is None else total + term
                sink[lv, sink_row + r0 + r, pl.ds(c * SUB, SUB), :] = total

    def finish(a, q):
        for dx in range(2):
            core_copy(a, q, dx).wait_recv()
        if a == 0:
            sweep(0, q, zb, RIM, -1)
        else:
            sweep(1, q, oa, 0, 1)

    def relay(a, q):
        far_recv(a, q).wait_recv()
        core_copy(a, q, 1).start()

    def polar_steps(a):
        order = [q for q in range(nq) if q not in det[a]] + list(det[a])
        steps = []
        for i in range(nq + LAG):
            if i < nq:
                steps.append((relay, a, order[i]))
            if i >= LAG:
                steps.append((finish, a, order[i - LAG]))
        return steps

    def polar_run(steps):
        @pl.when(polar)
        def _():
            for act, a, q in steps:
                act(a, q)

    def middle_finish(a):
        for lv in range(levels):
            pack_take(a, lv)
            for q in range(lv * per, (lv + 1) * per):
                core_copy(a, q, 0).wait_recv()
                if a == 0:
                    sweep(0, q, zb, RIM, -1)
                else:
                    sweep(1, q, oa, 0, 1)

    for b in dup:
        b.wait()

    polar_run(polar_steps(0))

    @pl.when(middle)
    def _():
        middle_finish(0)

    lat_start(zb, 1)

    @pl.when(middle)
    def _():
        for a in range(2):
            for q in det[a]:
                pass_on(a, q)
        middle_finish(1)

    late = polar_steps(1)
    polar_run(late[:-LATE])

    lat_wait(zb, 1)

    for lv in range(levels):

        @pl.loop(0, cells // SUB)
        def _(c):
            at = pl.ds(pl.multiple_of(c * SUB, SUB), SUB)
            z = {r: zb[lv, r + RIM, at, :] for r in range(-3, 0)}
            e, q6, dq, flux = {}, {}, {}, {}
            for f in range(-1, rows + 2):
                z[f + 1] = zb[lv, f + 1 + RIM, at, :]
                e[f] = (7.0 / 12.0) * (z[f - 1] + z[f]) - (1.0 / 12.0) * (z[f - 2] + z[f + 1])
                u = f - 1
                if u >= -1:
                    q6[u] = 6.0 * z[u] - 3.0 * (e[u] + e[f])
                    dq[u] = e[f] - e[u]
                if u >= 0:
                    v = vb[lv, u + 2, at, :]
                    north = v > 0.0
                    beta, gamma = face_terms(v)
                    flux[u] = (
                        v * e[u]
                        + beta * jnp.where(north, q6[u - 1], q6[u])
                        - gamma * jnp.where(north, dq[u - 1], dq[u])
                    )
                if u >= 1:
                    of[lv, u - 1, at, :] = z[u - 1] - flux[u] + flux[u - 1]

    polar_run(late[-LATE:])

    for a in range(2):
        for q in range(nq):
            core_copy(a, q, 0).wait_send()

            @pl.when(polar)
            def _():
                far_send(a, q).wait_send()
                core_copy(a, q, 1).wait_send()

        @pl.when(middle)
        def _():
            for q in det[a]:
                on_copy(a, q).wait_send()
            for lv in range(levels):
                for side in (HEAD, TAIL):

                    @pl.when(core == side)
                    def _():
                        pack_copy(a, lv, side).wait_send()

            if spill:
                few_copy(a).wait_send()


def store(f_in, a_in, f_out, a_out, sem):
    one = pltpu.make_async_copy(f_in, f_out, sem.at[0])
    two = pltpu.make_async_copy(a_in, a_out, sem.at[1])
    one.start()
    two.start()
    one.wait()
    two.wait()


def local(tracers, adjoint_in, shifts, fractions, meridional):
    levels, rows, cells, width = tracers.shape
    n_lon, n_lat = lax.axis_size("lon"), lax.axis_size("lat")
    n_x = n_lon // 2
    pair = fits(rows, cells, n_lon, n_lat)
    step = max(1, rows // (4 if pair else 2))
    nq = levels * (rows // step)
    dma = pltpu.SemaphoreType.DMA
    block = pltpu.VMEM((step, (n_lon + 1) * cells + SUB, width), jnp.float32)
    banded = pltpu.VMEM((levels, rows + 2 * RIM, cells, width), jnp.float32)
    scratch = [block] * (2 * nq) + [
        banded,
        banded,
        pltpu.VMEM((levels, rows + 5, cells, width), jnp.float32),
        pltpu.SMEM((levels * rows * 6,), jnp.float32),
        pltpu.SMEM(shifts.shape, jnp.int32),
        pltpu.SMEM(fractions.shape, jnp.float32),
        pltpu.VMEM((levels, cells, meridional.shape[1]), jnp.float32),
    ]
    if pair:
        det = detours(levels, rows, step)
        nd = max(len(d) for d in det)
        dims = (levels, rows, cells, width, n_lon, n_lat, step, det)
        long = pack_room(rows, cells, n_lon, n_lat)
        pack = pltpu.VMEM((2, levels, long, width), jnp.float32)
        few = pltpu.VMEM((2, levels * SUB, width), jnp.float32)
        body = paired
        scratch += [
            pltpu.VMEM((2, nd, step, cells, width), jnp.float32),
            pack,
            pack,
            few,
            few,
            dma((2 * nq + 4,)),
            dma((2, nq, 3)),
            dma((2, nq, 3)),
            dma((2, 2)),
            dma((2, 2)),
            dma((2, nd, 2)),
            dma((2, nd, 2)),
            dma((2, levels + 1)),
            dma((2, levels + 1)),
        ]
    else:
        dims = (levels, rows, cells, width, n_lon, n_lat, step)
        body = general
        scratch += [
            dma((2 * nq + 4,)),
            dma((2, nq, 2 * n_x)),
            dma((2, nq, 2 * n_x)),
            dma((2, 2)),
            dma((2, 2)),
        ]
    vmem = pl.BlockSpec(memory_space=pltpu.VMEM)
    far = pl.BlockSpec(memory_space=pltpu.HBM)
    kept = pltpu.VMEM(tracers.shape, jnp.float32)
    staged = pl.pallas_call(
        functools.partial(body, dims),
        out_shape=(kept, kept),
        in_specs=[far] * 5,
        out_specs=(vmem, vmem),
        scratch_shapes=scratch,
        compiler_params=pltpu.CompilerParams(
            collective_id=0, has_side_effects=True, vmem_limit_bytes=60 << 20
        ),
    )(tracers, adjoint_in, shifts, fractions, jnp.swapaxes(meridional, 1, 2))
    final = jax.ShapeDtypeStruct(tracers.shape, jnp.float32)
    return pl.pallas_call(
        store,
        out_shape=(final, final),
        in_specs=[vmem, vmem],
        out_specs=(far, far),
        scratch_shapes=[dma((2,))],
        compiler_params=pltpu.CompilerParams(vmem_limit_bytes=4 << 20),
    )(*staged)


def solution(mesh):
    block = P("grp", "lat", "lon", None)
    in_specs = (block, block, P(), P(), P(None, None, "lon"))
    return jax.shard_map(
        local, mesh=mesh, in_specs=in_specs, out_specs=(block, block), check_vma=False
    )
```

```python
import functools

import jax
import jax.numpy as jnp
from jax import lax
from jax.experimental import pallas as pl
from jax.experimental.pallas import tpu as pltpu
from jax.sharding import PartitionSpec as P

MESH = pl.DeviceIdType.MESH
SUB = 8
RIM = 3
LAG = 2
LATE = 4
HALVES = 2
SLOW = 2.4
DETOUR = ((0, 0), (0, 1), (1, 0), (1, 1))
HEAD, TAIL = 0, 1


def chunk_list(levels, rows, step):
    return [(lv, r0) for lv in range(levels) for r0 in range(0, rows, step)]


def reach(total_cells, total_rows, row):
    d = abs(2 * row + 1 - total_rows)
    return (total_cells - 1) * d * d // ((total_rows - 1) * (total_rows - 1))


def face_terms(v):
    size = jnp.abs(v)
    beta = v * (0.5 * size) * (1.0 - size * (2.0 / 3.0))
    return beta, 0.5 * v * v


def zonal_taps(c):
    b = 1.0 - c * (2.0 / 3.0)
    p = c * (1.0 - 0.5 * c - 1.5 * c * b)
    q = c * (0.5 * c - 1.5 * c * b)
    r = 3.0 * c * c * b
    d = p - q
    t = 1.0 / 12.0
    s = 7.0 / 12.0
    return (
        -t * q,
        s * q - t * d,
        r + t * p + s * d + s * q,
        1.0 - r - s * p + s * d - t * q,
        -s * p - t * d,
        t * p,
    )


def general(dims, *refs):
    levels, rows, cells, width, n_lon, n_lat, step = dims
    chunks = chunk_list(levels, rows, step)
    nq = len(chunks)
    tr, ad, shifts_in, fractions_in, mer_in, of, oa = refs[:7]
    gath = (refs[7 : 7 + nq], refs[7 + nq : 7 + 2 * nq])
    zb, ab, vb, taps, shifts, fractions, mer, loc, ssem, rsem, hs, hr = refs[7 + 2 * nq :]
    total_cells = cells * n_lon
    total_rows = rows * n_lat
    n_x = n_lon // 2

    me = lax.axis_index("lon")
    lat = lax.axis_index("lat")
    first = lat * rows
    core = lax.rem(me, 2)
    partner = me + 1 - 2 * core
    order = list(range(nq))

    own = []
    dup = []
    for q, (lv, r0) in enumerate(chunks):
        a = pltpu.make_async_copy(
            tr.at[lv, pl.ds(r0, step)], gath[0][q].at[:, pl.ds(0, cells)], loc.at[q]
        )
        a.start()
        own.append(a)
    adc = pltpu.make_async_copy(ad, ab.at[:, pl.ds(RIM, rows)], loc.at[2 * nq])
    adc.start()
    for q, (lv, r0) in enumerate(chunks):
        b = pltpu.make_async_copy(
            tr.at[lv, pl.ds(r0, step)],
            gath[0][q].at[:, pl.ds(total_cells, cells)],
            loc.at[nq + q],
        )
        b.start()
        dup.append(b)

    small = []
    for k, (source, target) in enumerate(
        ((shifts_in, shifts), (fractions_in, fractions), (mer_in, mer))
    ):
        d = pltpu.make_async_copy(source, target, loc.at[2 * nq + 1 + k])
        d.start()
        small.append(d)

    barrier = pltpu.get_barrier_semaphore()
    pl.semaphore_signal(barrier, inc=1, device_id={"lon": partner}, device_id_type=MESH)
    for dx in range(1, n_x):
        pl.semaphore_signal(
            barrier, inc=1, device_id={"lon": lax.rem(me + 2 * dx, n_lon)}, device_id_type=MESH
        )

    @pl.when(lat > 0)
    def _():
        pl.semaphore_signal(barrier, inc=1, device_id={"lat": lat - 1}, device_id_type=MESH)

    @pl.when(lat < n_lat - 1)
    def _():
        pl.semaphore_signal(barrier, inc=1, device_id={"lat": lat + 1}, device_id_type=MESH)

    inner = jnp.logical_and(lat > 0, lat < n_lat - 1)

    @pl.when(inner)
    def _():
        pl.semaphore_wait(barrier, n_x + 2)

    @pl.when(jnp.logical_not(inner))
    def _():
        pl.semaphore_wait(barrier, n_x + min(n_lat - 1, 1))

    def lat_copies(buf, k):
        down = pltpu.make_async_remote_copy(
            buf.at[:, pl.ds(RIM, RIM)],
            buf.at[:, pl.ds(RIM + rows, RIM)],
            hs.at[k, 0],
            hr.at[k, 0],
            device_id={"lat": lat - 1},
            device_id_type=MESH,
        )
        up = pltpu.make_async_remote_copy(
            buf.at[:, pl.ds(rows, RIM)],
            buf.at[:, pl.ds(0, RIM)],
            hs.at[k, 1],
            hr.at[k, 1],
            device_id={"lat": lat + 1},
            device_id_type=MESH,
        )
        return down, up

    def lat_start(buf, k):
        down, up = lat_copies(buf, k)

        @pl.when(lat > 0)
        def _():
            down.start()

        @pl.when(lat < n_lat - 1)
        def _():
            up.start()

    def lat_wait(buf, k):
        down, up = lat_copies(buf, k)

        @pl.when(lat > 0)
        def _():
            down.wait_send()
            up.wait_recv()

        @pl.when(lat < n_lat - 1)
        def _():
            up.wait_send()
            down.wait_recv()

    def x_copy(a, q, dx, span):
        lo, hi = span
        return pltpu.make_async_remote_copy(
            gath[a][q].at[:, pl.ds(lo, hi - lo)],
            gath[a][q].at[:, pl.ds((n_lon - 2 * dx) * cells + lo, hi - lo)],
            ssem.at[a, q, dx],
            rsem.at[a, q, dx],
            device_id={"lon": lax.rem(me + 2 * dx, n_lon)},
            device_id_type=MESH,
        )

    def core_copy(a, q, dx, span):
        lo, hi = span
        source = ((n_lon - 2 * dx) % n_lon) * cells + lo
        slot = lax.rem(2 * n_lon - 2 * dx + 2 * core - 1, n_lon)
        return pltpu.make_async_remote_copy(
            gath[a][q].at[:, pl.ds(source, hi - lo)],
            gath[a][q].at[:, pl.ds(pl.multiple_of(slot * cells + lo, SUB), hi - lo)],
            ssem.at[a, q, n_x + dx],
            rsem.at[a, q, n_x + dx],
            device_id={"lon": partner},
            device_id_type=MESH,
        )

    whole = (0, cells)

    def gather_start(a, q):
        for dx in range(1, n_x):
            x_copy(a, q, dx, whole).start()
        core_copy(a, q, 0, whole).start()

    def relay(a, q):
        for dx in range(1, n_x):
            x_copy(a, q, dx, whole).wait_recv()
            core_copy(a, q, dx, whole).start()

    def gather_finish(a, q):
        for dx in range(n_x):
            core_copy(a, q, dx, whole).wait_recv()

    def gather_drain(a, q):
        for dx in range(n_x):
            core_copy(a, q, dx, whole).wait_send()
        for dx in range(1, n_x):
            x_copy(a, q, dx, whole).wait_send()

    adc.wait()
    lat_start(ab, 0)
    for q in range(nq):
        own[q].wait()
        gather_start(0, q)

    @pl.when(lat == 0)
    def _():
        for buf in (ab, zb):
            buf[:, pl.ds(0, RIM)] = jnp.zeros((levels, RIM, cells, width), jnp.float32)

    @pl.when(lat == n_lat - 1)
    def _():
        for buf in (ab, zb):
            buf[:, pl.ds(RIM + rows, RIM)] = jnp.zeros((levels, RIM, cells, width), jnp.float32)

    for d in small:
        d.wait()
    faces = rows + 5
    lanes = lax.broadcasted_iota(jnp.int32, (cells, total_rows), 1)
    for lv in range(levels):

        @pl.loop(0, faces)
        def _(f):
            row = first + f - 2
            chosen = jnp.logical_and(lanes == row, lanes > 0)
            column = jnp.sum(jnp.where(chosen, mer[lv], 0.0), axis=1, keepdims=True)
            vb[lv, f] = jnp.broadcast_to(column, (cells, width))

        @pl.loop(0, rows)
        def _(r):
            for k, t in enumerate(zonal_taps(fractions[lv, first + r])):
                taps[(lv * rows + r) * 6 + k] = t

    lat_wait(ab, 0)
    for lv in range(levels):

        @pl.loop(0, cells // SUB)
        def _(c):
            at = pl.ds(pl.multiple_of(c * SUB, SUB), SUB)
            ev, q6b, dqb, eb = {}, {}, {}, {}
            carry = None
            y = {r: ab[lv, r + RIM, at, :] for r in range(-3, -1)}
            for f in range(-2, rows + 3):
                y[f] = ab[lv, f + RIM, at, :]
                v = vb[lv, f + 2, at, :]
                north = v > 0.0
                beta, gamma = face_terms(v)
                change = y[f] - y[f - 1]
                ev[f] = v * change
                b = beta * change
                g = -gamma * change
                bn, gn = jnp.where(north, b, 0.0), jnp.where(north, g, 0.0)
                if carry is not None:
                    q6b[f - 1] = bn + carry[0]
                    dqb[f - 1] = gn + carry[1]
                carry = (b - bn, g - gn)
                h = f - 1
                if h >= -1:
                    eb[h] = ev[h] - 3.0 * (q6b[h - 1] + q6b[h]) + (dqb[h - 1] - dqb[h])
                r = h - 2
                if r >= 0:
                    value = (
                        y[r]
                        + 6.0 * q6b[r]
                        + (7.0 / 12.0) * (eb[r] + eb[r + 1])
                        - (1.0 / 12.0) * (eb[r - 1] + eb[r + 2])
                    )
                    q = lv * (rows // step) + r // step
                    gath[1][q][r % step, at, :] = value
                    gath[1][q][
                        r % step, pl.ds(pl.multiple_of(total_cells + c * SUB, SUB), SUB), :
                    ] = value

        for q, (l2, _r) in enumerate(chunks):
            if l2 == lv:
                gather_start(1, q)

    def sweep(a, q, sink, sink_row, sign):
        lv, r0 = chunks[q]
        buf = gath[a][q]

        @pl.loop(0, step)
        def _(r):
            buf[r, pl.ds(total_cells + cells, SUB), :] = buf[r, pl.ds(cells, SUB), :]
            shift = shifts[lv, first + r0 + r]
            if sign < 0:
                start = lax.rem(2 * total_cells - shift - 3, total_cells)
            else:
                start = lax.rem(2 * total_cells + shift - 2, total_cells)
            base = (lv * rows + r0 + r) * 6
            w = [taps[base + k] for k in range(6)]
            if sign > 0:
                w = w[::-1]
            for c in range(cells // SUB):
                total = None
                for k in range(6):
                    term = w[k] * buf[r, pl.ds(start + c * SUB + k, SUB), :]
                    total = term if total is None else total + term
                sink[lv, sink_row + r0 + r, pl.ds(c * SUB, SUB), :] = total

    for b in dup:
        b.wait()
    for i, q in enumerate(order):
        relay(0, q)
        if i > 0:
            gather_finish(0, order[i - 1])
            sweep(0, order[i - 1], zb, RIM, -1)
    gather_finish(0, order[-1])
    sweep(0, order[-1], zb, RIM, -1)
    lat_start(zb, 1)

    relay(1, order[0])
    lat_wait(zb, 1)

    for lv in range(levels):

        @pl.loop(0, cells // SUB)
        def _(c):
            at = pl.ds(pl.multiple_of(c * SUB, SUB), SUB)
            z = {r: zb[lv, r + RIM, at, :] for r in range(-3, 0)}
            e, q6, dq, flux = {}, {}, {}, {}
            for f in range(-1, rows + 2):
                z[f + 1] = zb[lv, f + 1 + RIM, at, :]
                e[f] = (7.0 / 12.0) * (z[f - 1] + z[f]) - (1.0 / 12.0) * (z[f - 2] + z[f + 1])
                u = f - 1
                if u >= -1:
                    q6[u] = 6.0 * z[u] - 3.0 * (e[u] + e[f])
                    dq[u] = e[f] - e[u]
                if u >= 0:
                    v = vb[lv, u + 2, at, :]
                    north = v > 0.0
                    beta, gamma = face_terms(v)
                    flux[u] = (
                        v * e[u]
                        + beta * jnp.where(north, q6[u - 1], q6[u])
                        - gamma * jnp.where(north, dq[u - 1], dq[u])
                    )
                if u >= 1:
                    of[lv, u - 1, at, :] = z[u - 1] - flux[u] + flux[u - 1]

    def finish_adjoint(q):
        lv, r0 = chunks[q]
        gather_finish(1, q)
        sweep(1, q, oa, 0, 1)

    for i in range(1, nq):
        relay(1, order[i])
        finish_adjoint(order[i - 1])
    finish_adjoint(order[-1])

    for a in range(2):
        for q in range(nq):
            gather_drain(a, q)


def reaches(rows, cells, n_lon, n_lat, lat):
    return [reach(cells * n_lon, rows * n_lat, lat * rows + k) + RIM for k in range(rows)]


def fits(levels, rows, cells, n_lon, n_lat):
    if levels != 2 or n_lon != 4 or n_lat != 4 or rows % 8 or cells % SUB:
        return False
    outer = reaches(rows, cells, n_lon, n_lat, 0)[-(rows // 4) :]
    inner = reaches(rows, cells, n_lon, n_lat, 1)
    return cells < min(outer) and max(outer) <= 2 * cells and max(inner) <= cells + SUB


def plan_of(cells, sizes, side):
    slots = []
    at = SUB
    for s in sizes:
        if s >= SUB:
            begins = list(range(0, s - SUB + 1, SUB))
            if s % SUB:
                begins.append(s - SUB)
            shift = cells - s if side == TAIL else 0
            slots.append([(shift + b, at + b) for b in begins])
        elif side == TAIL:
            slots.append([(cells - SUB, at + s - SUB)])
        else:
            slots.append([(0, at)])
        at += s
    return slots, -(-(at - SUB) // SUB) * SUB


def pack_plan(rows, cells, n_lon, n_lat, a, side):
    sizes = [RIM - 1] * rows
    if (side == TAIL) == (a == 0):
        sizes = [min(m, cells) for m in reaches(rows, cells, n_lon, n_lat, 1)]
    return plan_of(cells, sizes, side)


def trim_plan(rows, cells, n_lon, n_lat, a):
    step = rows // 4
    sizes = [m - cells for m in reaches(rows, cells, n_lon, n_lat, 0)[-step:]]
    near = TAIL if a == 0 else HEAD
    return near, plan_of(cells, sizes, near), plan_of(cells, [RIM - 1] * step, 1 - near)


def pack_room(rows, cells, n_lon, n_lat):
    return 2 * SUB + max(
        pack_plan(rows, cells, n_lon, n_lat, a, side)[1] for a in range(2) for side in (HEAD, TAIL)
    )


def trim_room(rows, cells, n_lon, n_lat):
    return 2 * SUB + max(
        plan[1] for a in range(2) for plan in trim_plan(rows, cells, n_lon, n_lat, a)[1:]
    )


def paired(dims, *refs):
    levels, rows, cells, width, n_lon, n_lat, step = dims
    chunks = chunk_list(levels, rows, step)
    nq = len(chunks)
    per = rows // step
    tr, ad, shifts_in, fractions_in, mer_in, of, oa = refs[:7]
    gath = (refs[7 : 7 + nq], refs[7 + nq : 7 + 2 * nq])
    zb, ab, vb, taps, shifts, fractions, mer, held = refs[7 + 2 * nq : 15 + 2 * nq]
    sendp, recvp, sendx, recvx, loc, ssem, rsem, hs, hr, vs, vr, ps, pr, sendt, recvt, ts, tr_, ready = refs[15 + 2 * nq :]
    total_cells = cells * n_lon
    total_rows = rows * n_lat

    me = lax.axis_index("lon")
    lat = lax.axis_index("lat")
    first = lat * rows
    core = lax.rem(me, 2)
    partner = me + 1 - 2 * core
    beside = lax.rem(me + 2, n_lon)
    joint = lax.rem(me + n_lon + 2 * core - 1, n_lon)
    mate = lat + 1 - 2 * lax.rem(lat, 2)
    middle = jnp.logical_and(lat > 0, lat < n_lat - 1)
    polar = jnp.logical_not(middle)

    barrier = pltpu.get_barrier_semaphore()

    def greet(**place):
        pl.semaphore_signal(barrier, inc=1, device_id=place, device_id_type=MESH)

    greet(lon=partner)
    greet(lon=beside)
    greet(lon=joint)

    @pl.when(lat > 0)
    def _():
        greet(lat=lat - 1)

    @pl.when(lat < n_lat - 1)
    def _():
        greet(lat=lat + 1)

    own = []
    dup = []
    for q, (lv, r0) in enumerate(chunks):
        a = pltpu.make_async_copy(
            tr.at[lv, pl.ds(r0, step)], gath[0][q].at[:, pl.ds(0, cells)], loc.at[q]
        )
        a.start()
        own.append(a)
    adc = pltpu.make_async_copy(ad, ab.at[:, pl.ds(RIM, rows)], loc.at[2 * nq])
    adc.start()
    small = []
    for k, (source, target) in enumerate(
        ((shifts_in, shifts), (fractions_in, fractions), (mer_in, mer))
    ):
        d = pltpu.make_async_copy(source, target, loc.at[2 * nq + 1 + k])
        d.start()
        small.append(d)
    for q, (lv, r0) in enumerate(chunks):
        b = pltpu.make_async_copy(
            tr.at[lv, pl.ds(r0, step)],
            gath[0][q].at[:, pl.ds(total_cells, cells)],
            loc.at[nq + q],
        )
        b.start()
        dup.append(b)

    @pl.when(middle)
    def _():
        pl.semaphore_wait(barrier, 5)
        pl.semaphore_signal(ready, inc=1, device_id={"lat": mate}, device_id_type=MESH)

    @pl.when(polar)
    def _():
        pl.semaphore_wait(barrier, 4)

    def remote(source, target, send, recv, **place):
        return pltpu.make_async_remote_copy(
            source, target, send, recv, device_id=place, device_id_type=MESH
        )

    def lat_copies(buf, k, lv):
        down = remote(
            buf.at[lv, pl.ds(RIM, RIM)],
            buf.at[lv, pl.ds(RIM + rows, RIM)],
            hs.at[k, lv, 0],
            hr.at[k, lv, 0],
            lat=lat - 1,
        )
        up = remote(
            buf.at[lv, pl.ds(rows, RIM)],
            buf.at[lv, pl.ds(0, RIM)],
            hs.at[k, lv, 1],
            hr.at[k, lv, 1],
            lat=lat + 1,
        )
        return down, up

    def lat_start(buf, k, lv):
        down, up = lat_copies(buf, k, lv)

        @pl.when(lat > 0)
        def _():
            down.start()

        @pl.when(lat < n_lat - 1)
        def _():
            up.start()

    def lat_wait(buf, k, lv):
        down, up = lat_copies(buf, k, lv)

        @pl.when(lat > 0)
        def _():
            down.wait_send()
            up.wait_recv()

        @pl.when(lat < n_lat - 1)
        def _():
            up.wait_send()
            down.wait_recv()

    own_block = pl.ds(0, cells)
    far_block = pl.ds((n_lon - 2) * cells, cells)

    def x_copy(a, q):
        g = gath[a][q]
        return remote(
            g.at[:, own_block], g.at[:, far_block], ssem.at[a, q, 0], rsem.at[a, q, 0], lon=beside
        )

    def core_copy(a, q, dx):
        g = gath[a][q]
        source = ((n_lon - 2 * dx) % n_lon) * cells
        slot = lax.rem(2 * n_lon - 2 * dx + 2 * core - 1, n_lon)
        return remote(
            g.at[:, pl.ds(source, cells)],
            g.at[:, pl.ds(pl.multiple_of(slot * cells, SUB), cells)],
            ssem.at[a, q, 1 + dx],
            rsem.at[a, q, 1 + dx],
            lon=partner,
        )

    piece = step // HALVES

    def chunk_at(lv, k, south):
        return lv * per + (k if south else per - 1 - k)

    def polar_half(act):
        for south in (True, False):

            @pl.when(lat == (0 if south else n_lat - 1))
            def _():
                act(south)

    def out_copy(i, h, south):
        q = chunk_at(*DETOUR[i], south)
        return remote(
            gath[1][q].at[pl.ds(h * piece, piece), own_block],
            held.at[i, pl.ds(h * piece, piece)],
            vs.at[i, h, 0],
            vr.at[i, h, 0],
            lon=beside,
            lat=mate,
        )

    def on_copy(i, h, south):
        q = chunk_at(*DETOUR[i], south)
        return remote(
            held.at[i, pl.ds(h * piece, piece)],
            gath[1][q].at[pl.ds(h * piece, piece), far_block],
            vs.at[i, h, 1],
            vr.at[i, h, 1],
            lat=mate,
        )

    def trim_copy(a, lv, w):
        long = trims[a][1 + w][1]
        return remote(
            sendt.at[a, lv, w, pl.ds(SUB, long)],
            recvt.at[a, lv, w, pl.ds(SUB, long)],
            ts.at[a, lv, w],
            tr_.at[a, lv, w],
            lon=joint if w else beside,
        )

    trims = [trim_plan(rows, cells, n_lon, n_lat, a) for a in range(2)]
    plans = [[pack_plan(rows, cells, n_lon, n_lat, a, side) for side in (HEAD, TAIL)] for a in range(2)]
    ring = (cells, (n_lon - 1) * cells)
    spill = [
        k for k in range(rows) if reach(total_cells, total_rows, rows + k) + RIM > cells
    ]
    last = (cells - SUB, 0)

    def place_of(lv, k, south):
        r = k if south else rows - 1 - k
        return lv * per + r // step, r % step

    def by_half(act):
        for south in (True, False):

            @pl.when(lat == (1 if south else n_lat - 2))
            def _():
                act(south)

    def pack_copy(a, lv, side):
        long = plans[a][side][1]
        return remote(
            sendp.at[a, lv, pl.ds(SUB, long)],
            recvp.at[a, lv, pl.ds(SUB, long)],
            ps.at[a, lv],
            pr.at[a, lv],
            lon=joint,
        )

    def few_copy(a):
        return remote(sendx.at[a], recvx.at[a], ps.at[a, levels], pr.at[a, levels], lon=beside)

    def pack_send(a, lv):
        for side in (HEAD, TAIL):

            @pl.when(core == side)
            def _():
                def fill(south):
                    order = range(rows) if side == HEAD else reversed(range(rows))
                    for k in order:
                        q, j = place_of(lv, k, south)
                        for source, target in plans[a][side][0][k]:
                            sendp[a, lv, pl.ds(target, SUB), :] = gath[a][q][j, pl.ds(source, SUB), :]

                by_half(fill)
                pack_copy(a, lv, side).start()

        if spill:

            def few(south):
                q, j = place_of(lv, spill[0], south)
                sendx[a, pl.ds(lv * SUB, SUB), :] = gath[a][q][j, pl.ds(last[a], SUB), :]

            by_half(few)
            if lv == levels - 1:
                few_copy(a).start()

    def pack_take(a, lv):
        for side in (HEAD, TAIL):

            @pl.when(core == 1 - side)
            def _():
                pack_copy(a, lv, side).wait_recv()

                def empty(south):
                    for k in range(rows):
                        q, j = place_of(lv, k, south)
                        for source, target in plans[a][side][0][k]:
                            gath[a][q][j, pl.ds(ring[side] + source, SUB), :] = recvp[
                                a, lv, pl.ds(target, SUB), :
                            ]

                by_half(empty)

        if spill:
            if lv == 0:
                few_copy(a).wait_recv()

            def few(south):
                q, j = place_of(lv, spill[0], south)
                gath[a][q][j, pl.ds(2 * cells + last[a], SUB), :] = recvx[a, pl.ds(lv * SUB, SUB), :]

            by_half(few)

    def trim_send(a, lv, south):
        near, *pair = trims[a]
        for w in range(2):
            side = 1 - near if w else near
            slots = pair[w][0]
            order = range(step) if side == HEAD else reversed(range(step))
            for k in order:
                q, j = place_of(lv, rows - step + k, south)
                for source, target in slots[k]:
                    sendt[a, lv, w, pl.ds(target, SUB), :] = gath[a][q][j, pl.ds(source, SUB), :]
            trim_copy(a, lv, w).start()

    def trim_take(a, lv, w, south):
        near, *pair = trims[a]
        base = ring[1 - near] if w else 2 * cells
        trim_copy(a, lv, w).wait_recv()
        for k in range(step):
            q, j = place_of(lv, rows - step + k, south)
            for source, target in pair[w][0][k]:
                gath[a][q][j, pl.ds(base + source, SUB), :] = recvt[a, lv, w, pl.ds(target, SUB), :]

    def kind(a, lv, k):
        if k == per - 1:
            return "trim"
        return "detour" if a == 1 and (lv, k) in DETOUR else "direct"

    def far_send(a, lv, k, south):
        q = chunk_at(lv, k, south)
        if kind(a, lv, k) == "detour":
            for h in range(HALVES):
                out_copy(DETOUR.index((lv, k)), h, south).start()
        elif kind(a, lv, k) == "direct":
            x_copy(a, q).start()
        else:

            @pl.when(core == 1 - a)
            def _():
                x_copy(a, q).start()

            @pl.when(core == a)
            def _():
                trim_send(a, lv, south)

    def relay(a, lv, k, south):
        q = chunk_at(lv, k, south)
        if kind(a, lv, k) == "detour":
            for h in range(HALVES):
                on_copy(DETOUR.index((lv, k)), h, south).wait_recv()
            core_copy(a, q, 1).start()
        elif kind(a, lv, k) == "direct":
            x_copy(a, q).wait_recv()
            core_copy(a, q, 1).start()
        else:

            @pl.when(core == 1 - a)
            def _():
                x_copy(a, q).wait_recv()
                core_copy(a, q, 1).start()
                trim_take(a, lv, 1, south)

            @pl.when(core == a)
            def _():
                trim_take(a, lv, 0, south)

    def far_done(a, lv, k, south):
        q = chunk_at(lv, k, south)
        if kind(a, lv, k) == "detour":
            for h in range(HALVES):
                out_copy(DETOUR.index((lv, k)), h, south).wait_send()
            core_copy(a, q, 1).wait_send()
        elif kind(a, lv, k) == "direct":
            x_copy(a, q).wait_send()
            core_copy(a, q, 1).wait_send()
        else:

            @pl.when(core == 1 - a)
            def _():
                x_copy(a, q).wait_send()
                core_copy(a, q, 1).wait_send()

            @pl.when(core == a)
            def _():
                for w in range(2):
                    trim_copy(a, lv, w).wait_send()

    def pass_on(south):
        for i in range(len(DETOUR)):
            for h in range(HALVES):
                out_copy(i, h, south).wait_recv()
                on_copy(i, h, south).start()

    def send_level(a, lv):
        polar_half(lambda south: [far_send(a, lv, k, south) for k in range(per)])

        @pl.when(middle)
        def _():
            pack_send(a, lv)

        for q in range(lv * per, (lv + 1) * per):
            core_copy(a, q, 0).start()

    adc.wait()
    lat_start(ab, 0, 0)
    for lv in range(levels):
        for q in range(lv * per, (lv + 1) * per):
            own[q].wait()
        send_level(0, lv)

    @pl.when(lat == 0)
    def _():
        for buf in (ab, zb):
            buf[:, pl.ds(0, RIM)] = jnp.zeros((levels, RIM, cells, width), jnp.float32)

    @pl.when(lat == n_lat - 1)
    def _():
        for buf in (ab, zb):
            buf[:, pl.ds(RIM + rows, RIM)] = jnp.zeros((levels, RIM, cells, width), jnp.float32)

    for d in small:
        d.wait()
    faces = rows + 5
    lanes = lax.broadcasted_iota(jnp.int32, (cells, total_rows), 1)
    for lv in range(levels):

        @pl.loop(0, faces, unroll=faces)
        def _(f):
            row = first + f - 2
            chosen = jnp.logical_and(lanes == row, lanes > 0)
            column = jnp.sum(jnp.where(chosen, mer[lv], 0.0), axis=1, keepdims=True)
            vb[lv, f] = jnp.broadcast_to(column, (cells, width))

        if lv + 1 < levels:
            lat_start(ab, 0, lv + 1)

        @pl.loop(0, rows)
        def _(r):
            for k, t in enumerate(zonal_taps(fractions[lv, first + r])):
                taps[(lv * rows + r) * 6 + k] = t

    for lv in range(levels):
        lat_wait(ab, 0, lv)

        @pl.loop(0, cells // SUB)
        def _(c):
            at = pl.ds(pl.multiple_of(c * SUB, SUB), SUB)
            ev, q6b, dqb, eb = {}, {}, {}, {}
            carry = None
            y = {r: ab[lv, r + RIM, at, :] for r in range(-3, -1)}
            for f in range(-2, rows + 3):
                y[f] = ab[lv, f + RIM, at, :]
                v = vb[lv, f + 2, at, :]
                north = v > 0.0
                beta, gamma = face_terms(v)
                change = y[f] - y[f - 1]
                ev[f] = v * change
                b = beta * change
                g = -gamma * change
                bn, gn = jnp.where(north, b, 0.0), jnp.where(north, g, 0.0)
                if carry is not None:
                    q6b[f - 1] = bn + carry[0]
                    dqb[f - 1] = gn + carry[1]
                carry = (b - bn, g - gn)
                h = f - 1
                if h >= -1:
                    eb[h] = ev[h] - 3.0 * (q6b[h - 1] + q6b[h]) + (dqb[h - 1] - dqb[h])
                r = h - 2
                if r >= 0:
                    value = (
                        y[r]
                        + 6.0 * q6b[r]
                        + (7.0 / 12.0) * (eb[r] + eb[r + 1])
                        - (1.0 / 12.0) * (eb[r - 1] + eb[r + 2])
                    )
                    q = lv * per + r // step
                    gath[1][q][r % step, at, :] = value
                    gath[1][q][
                        r % step, pl.ds(pl.multiple_of(total_cells + c * SUB, SUB), SUB), :
                    ] = value

        if lv == 0:

            @pl.when(polar)
            def _():
                pl.semaphore_wait(ready, 1)

        send_level(1, lv)

    def sweep(a, q, sink, sink_row, sign):
        lv, r0 = chunks[q]
        buf = gath[a][q]

        @pl.loop(0, step)
        def _(r):
            buf[r, pl.ds(total_cells + cells, SUB), :] = buf[r, pl.ds(cells, SUB), :]
            shift = shifts[lv, first + r0 + r]
            if sign < 0:
                start = lax.rem(2 * total_cells - shift - 3, total_cells)
            else:
                start = lax.rem(2 * total_cells + shift - 2, total_cells)
            base = (lv * rows + r0 + r) * 6
            w = [taps[base + k] for k in range(6)]
            if sign > 0:
                w = w[::-1]
            for c in range(cells // SUB):
                total = None
                for k in range(6):
                    term = w[k] * buf[r, pl.ds(start + c * SUB + k, SUB), :]
                    total = term if total is None else total + term
                sink[lv, sink_row + r0 + r, pl.ds(c * SUB, SUB), :] = total

    def finish(a, lv, k, south):
        q = chunk_at(lv, k, south)
        core_copy(a, q, 0).wait_recv()
        if kind(a, lv, k) == "trim":

            @pl.when(core == a)
            def _():
                core_copy(a, q, 1).wait_recv()

        else:
            core_copy(a, q, 1).wait_recv()
        if a == 0:
            sweep(0, q, zb, RIM, -1)
        else:
            sweep(1, q, oa, 0, 1)

    def polar_steps(a):
        spots = [(lv, k) for lv in range(levels) for k in range(per)]
        direct = [p for p in spots if kind(a, *p) != "detour"]
        due = {p: i + SLOW for i, p in enumerate(direct)}
        due.update({p: i for i, p in enumerate(DETOUR) if a == 1})
        order = sorted(spots, key=lambda p: due[p])
        steps = []
        for i in range(nq + LAG):
            if i < nq:
                steps.append((relay, a) + order[i])
            if i >= LAG:
                steps.append((finish, a) + order[i - LAG])
        return steps

    def polar_run(steps):
        polar_half(lambda south: [step_[0](*step_[1:], south) for step_ in steps])

    def middle_finish(a):
        for lv in range(levels):
            pack_take(a, lv)
            for q in range(lv * per, (lv + 1) * per):
                core_copy(a, q, 0).wait_recv()
                if a == 0:
                    sweep(0, q, zb, RIM, -1)
                else:
                    sweep(1, q, oa, 0, 1)

    for b in dup:
        b.wait()

    polar_run(polar_steps(0))

    @pl.when(middle)
    def _():
        middle_finish(0)

    for lv in range(levels):
        lat_start(zb, 1, lv)

    @pl.when(middle)
    def _():
        by_half(pass_on)
        middle_finish(1)

    late = polar_steps(1)
    polar_run(late[:-LATE])

    for lv in range(levels):
        lat_wait(zb, 1, lv)

        @pl.loop(0, cells // SUB)
        def _(c):
            at = pl.ds(pl.multiple_of(c * SUB, SUB), SUB)
            z = {r: zb[lv, r + RIM, at, :] for r in range(-3, 0)}
            e, q6, dq, flux = {}, {}, {}, {}
            for f in range(-1, rows + 2):
                z[f + 1] = zb[lv, f + 1 + RIM, at, :]
                e[f] = (7.0 / 12.0) * (z[f - 1] + z[f]) - (1.0 / 12.0) * (z[f - 2] + z[f + 1])
                u = f - 1
                if u >= -1:
                    q6[u] = 6.0 * z[u] - 3.0 * (e[u] + e[f])
                    dq[u] = e[f] - e[u]
                if u >= 0:
                    v = vb[lv, u + 2, at, :]
                    north = v > 0.0
                    beta, gamma = face_terms(v)
                    flux[u] = (
                        v * e[u]
                        + beta * jnp.where(north, q6[u - 1], q6[u])
                        - gamma * jnp.where(north, dq[u - 1], dq[u])
                    )
                if u >= 1:
                    of[lv, u - 1, at, :] = z[u - 1] - flux[u] + flux[u - 1]

    polar_run(late[-LATE:])

    for a in range(2):
        for q in range(nq):
            core_copy(a, q, 0).wait_send()
    polar_half(
        lambda south: [
            far_done(a, lv, k, south) for a in range(2) for lv in range(levels) for k in range(per)
        ]
    )

    @pl.when(middle)
    def _():
        def sent(south):
            for i in range(len(DETOUR)):
                for h in range(HALVES):
                    on_copy(i, h, south).wait_send()

        by_half(sent)
        for a in range(2):
            for lv in range(levels):
                for side in (HEAD, TAIL):

                    @pl.when(core == side)
                    def _():
                        pack_copy(a, lv, side).wait_send()

            if spill:
                few_copy(a).wait_send()


def store(f_in, a_in, f_out, a_out, sem):
    one = pltpu.make_async_copy(f_in, f_out, sem.at[0])
    two = pltpu.make_async_copy(a_in, a_out, sem.at[1])
    one.start()
    two.start()
    one.wait()
    two.wait()


def local(tracers, adjoint_in, shifts, fractions, meridional):
    levels, rows, cells, width = tracers.shape
    n_lon, n_lat = lax.axis_size("lon"), lax.axis_size("lat")
    n_x = n_lon // 2
    pair = fits(levels, rows, cells, n_lon, n_lat)
    step = max(1, rows // (4 if pair else 2))
    nq = levels * (rows // step)
    dma = pltpu.SemaphoreType.DMA
    block = pltpu.VMEM((step, (n_lon + 1) * cells + SUB, width), jnp.float32)
    banded = pltpu.VMEM((levels, rows + 2 * RIM, cells, width), jnp.float32)
    scratch = [block] * (2 * nq) + [
        banded,
        banded,
        pltpu.VMEM((levels, rows + 5, cells, width), jnp.float32),
        pltpu.SMEM((levels * rows * 6,), jnp.float32),
        pltpu.SMEM(shifts.shape, jnp.int32),
        pltpu.SMEM(fractions.shape, jnp.float32),
        pltpu.VMEM((levels, cells, meridional.shape[1]), jnp.float32),
    ]
    if pair:
        nd = len(DETOUR)
        dims = (levels, rows, cells, width, n_lon, n_lat, step)
        long = pack_room(rows, cells, n_lon, n_lat)
        pack = pltpu.VMEM((2, levels, long, width), jnp.float32)
        trim = pltpu.VMEM(
            (2, levels, 2, trim_room(rows, cells, n_lon, n_lat), width), jnp.float32
        )
        few = pltpu.VMEM((2, levels * SUB, width), jnp.float32)
        body = paired
        scratch += [
            pltpu.VMEM((nd, step, cells, width), jnp.float32),
            pack,
            pack,
            few,
            few,
            dma((2 * nq + 4,)),
            dma((2, nq, 3)),
            dma((2, nq, 3)),
            dma((2, levels, 2)),
            dma((2, levels, 2)),
            dma((nd, HALVES, 2)),
            dma((nd, HALVES, 2)),
            dma((2, levels + 1)),
            dma((2, levels + 1)),
            trim,
            trim,
            dma((2, levels, 2)),
            dma((2, levels, 2)),
            pltpu.SemaphoreType.REGULAR,
        ]
    else:
        dims = (levels, rows, cells, width, n_lon, n_lat, step)
        body = general
        scratch += [
            dma((2 * nq + 4,)),
            dma((2, nq, 2 * n_x)),
            dma((2, nq, 2 * n_x)),
            dma((2, 2)),
            dma((2, 2)),
        ]
    vmem = pl.BlockSpec(memory_space=pltpu.VMEM)
    far = pl.BlockSpec(memory_space=pltpu.HBM)
    kept = pltpu.VMEM(tracers.shape, jnp.float32)
    staged = pl.pallas_call(
        functools.partial(body, dims),
        out_shape=(kept, kept),
        in_specs=[far] * 5,
        out_specs=(vmem, vmem),
        scratch_shapes=scratch,
        compiler_params=pltpu.CompilerParams(
            collective_id=0, has_side_effects=True, vmem_limit_bytes=60 << 20
        ),
    )(tracers, adjoint_in, shifts, fractions, jnp.swapaxes(meridional, 1, 2))
    final = jax.ShapeDtypeStruct(tracers.shape, jnp.float32)
    return pl.pallas_call(
        store,
        out_shape=(final, final),
        in_specs=[vmem, vmem],
        out_specs=(far, far),
        scratch_shapes=[dma((2,))],
        compiler_params=pltpu.CompilerParams(vmem_limit_bytes=4 << 20),
    )(*staged)


def solution(mesh):
    block = P("grp", "lat", "lon", None)
    in_specs = (block, block, P(), P(), P(None, None, "lon"))
    return jax.shard_map(
        local, mesh=mesh, in_specs=in_specs, out_specs=(block, block), check_vma=False
    )
```

```python
import functools

import jax
import jax.numpy as jnp
from jax import lax
from jax.experimental import pallas as pl
from jax.experimental.pallas import tpu as pltpu
from jax.sharding import PartitionSpec as P

MESH = pl.DeviceIdType.MESH
SUB = 8
RIM = 3
LAG = 2
LATE = 4
HALVES = 2
SLOW = 2.4
DETOUR = ((0, 0), (0, 1), (1, 0), (1, 1))
HEAD, TAIL = 0, 1


def chunk_list(levels, rows, step):
    return [(lv, r0) for lv in range(levels) for r0 in range(0, rows, step)]


def reach(total_cells, total_rows, row):
    d = abs(2 * row + 1 - total_rows)
    return (total_cells - 1) * d * d // ((total_rows - 1) * (total_rows - 1))


def face_terms(v):
    size = jnp.abs(v)
    beta = v * (0.5 * size) * (1.0 - size * (2.0 / 3.0))
    return beta, 0.5 * v * v


def zonal_taps(c):
    b = 1.0 - c * (2.0 / 3.0)
    p = c * (1.0 - 0.5 * c - 1.5 * c * b)
    q = c * (0.5 * c - 1.5 * c * b)
    r = 3.0 * c * c * b
    d = p - q
    t = 1.0 / 12.0
    s = 7.0 / 12.0
    return (
        -t * q,
        s * q - t * d,
        r + t * p + s * d + s * q,
        1.0 - r - s * p + s * d - t * q,
        -s * p - t * d,
        t * p,
    )


def general(dims, *refs):
    levels, rows, cells, width, n_lon, n_lat, step = dims
    chunks = chunk_list(levels, rows, step)
    nq = len(chunks)
    tr, ad, shifts_in, fractions_in, mer_in, of, oa = refs[:7]
    gath = (refs[7 : 7 + nq], refs[7 + nq : 7 + 2 * nq])
    zb, ab, vb, taps, shifts, fractions, mer, loc, ssem, rsem, hs, hr = refs[7 + 2 * nq :]
    total_cells = cells * n_lon
    total_rows = rows * n_lat
    n_x = n_lon // 2

    me = lax.axis_index("lon")
    lat = lax.axis_index("lat")
    first = lat * rows
    core = lax.rem(me, 2)
    partner = me + 1 - 2 * core
    order = list(range(nq))

    own = []
    dup = []
    for q, (lv, r0) in enumerate(chunks):
        a = pltpu.make_async_copy(
            tr.at[lv, pl.ds(r0, step)], gath[0][q].at[:, pl.ds(0, cells)], loc.at[q]
        )
        a.start()
        own.append(a)
    adc = pltpu.make_async_copy(ad, ab.at[:, pl.ds(RIM, rows)], loc.at[2 * nq])
    adc.start()
    for q, (lv, r0) in enumerate(chunks):
        b = pltpu.make_async_copy(
            tr.at[lv, pl.ds(r0, step)],
            gath[0][q].at[:, pl.ds(total_cells, cells)],
            loc.at[nq + q],
        )
        b.start()
        dup.append(b)

    small = []
    for k, (source, target) in enumerate(
        ((shifts_in, shifts), (fractions_in, fractions), (mer_in, mer))
    ):
        d = pltpu.make_async_copy(source, target, loc.at[2 * nq + 1 + k])
        d.start()
        small.append(d)

    barrier = pltpu.get_barrier_semaphore()
    pl.semaphore_signal(barrier, inc=1, device_id={"lon": partner}, device_id_type=MESH)
    for dx in range(1, n_x):
        pl.semaphore_signal(
            barrier, inc=1, device_id={"lon": lax.rem(me + 2 * dx, n_lon)}, device_id_type=MESH
        )

    @pl.when(lat > 0)
    def _():
        pl.semaphore_signal(barrier, inc=1, device_id={"lat": lat - 1}, device_id_type=MESH)

    @pl.when(lat < n_lat - 1)
    def _():
        pl.semaphore_signal(barrier, inc=1, device_id={"lat": lat + 1}, device_id_type=MESH)

    inner = jnp.logical_and(lat > 0, lat < n_lat - 1)

    @pl.when(inner)
    def _():
        pl.semaphore_wait(barrier, n_x + 2)

    @pl.when(jnp.logical_not(inner))
    def _():
        pl.semaphore_wait(barrier, n_x + min(n_lat - 1, 1))

    def lat_copies(buf, k):
        down = pltpu.make_async_remote_copy(
            buf.at[:, pl.ds(RIM, RIM)],
            buf.at[:, pl.ds(RIM + rows, RIM)],
            hs.at[k, 0],
            hr.at[k, 0],
            device_id={"lat": lat - 1},
            device_id_type=MESH,
        )
        up = pltpu.make_async_remote_copy(
            buf.at[:, pl.ds(rows, RIM)],
            buf.at[:, pl.ds(0, RIM)],
            hs.at[k, 1],
            hr.at[k, 1],
            device_id={"lat": lat + 1},
            device_id_type=MESH,
        )
        return down, up

    def lat_start(buf, k):
        down, up = lat_copies(buf, k)

        @pl.when(lat > 0)
        def _():
            down.start()

        @pl.when(lat < n_lat - 1)
        def _():
            up.start()

    def lat_wait(buf, k):
        down, up = lat_copies(buf, k)

        @pl.when(lat > 0)
        def _():
            down.wait_send()
            up.wait_recv()

        @pl.when(lat < n_lat - 1)
        def _():
            up.wait_send()
            down.wait_recv()

    def x_copy(a, q, dx, span):
        lo, hi = span
        return pltpu.make_async_remote_copy(
            gath[a][q].at[:, pl.ds(lo, hi - lo)],
            gath[a][q].at[:, pl.ds((n_lon - 2 * dx) * cells + lo, hi - lo)],
            ssem.at[a, q, dx],
            rsem.at[a, q, dx],
            device_id={"lon": lax.rem(me + 2 * dx, n_lon)},
            device_id_type=MESH,
        )

    def core_copy(a, q, dx, span):
        lo, hi = span
        source = ((n_lon - 2 * dx) % n_lon) * cells + lo
        slot = lax.rem(2 * n_lon - 2 * dx + 2 * core - 1, n_lon)
        return pltpu.make_async_remote_copy(
            gath[a][q].at[:, pl.ds(source, hi - lo)],
            gath[a][q].at[:, pl.ds(pl.multiple_of(slot * cells + lo, SUB), hi - lo)],
            ssem.at[a, q, n_x + dx],
            rsem.at[a, q, n_x + dx],
            device_id={"lon": partner},
            device_id_type=MESH,
        )

    whole = (0, cells)

    def gather_start(a, q):
        for dx in range(1, n_x):
            x_copy(a, q, dx, whole).start()
        core_copy(a, q, 0, whole).start()

    def relay(a, q):
        for dx in range(1, n_x):
            x_copy(a, q, dx, whole).wait_recv()
            core_copy(a, q, dx, whole).start()

    def gather_finish(a, q):
        for dx in range(n_x):
            core_copy(a, q, dx, whole).wait_recv()

    def gather_drain(a, q):
        for dx in range(n_x):
            core_copy(a, q, dx, whole).wait_send()
        for dx in range(1, n_x):
            x_copy(a, q, dx, whole).wait_send()

    adc.wait()
    lat_start(ab, 0)
    for q in range(nq):
        own[q].wait()
        gather_start(0, q)

    @pl.when(lat == 0)
    def _():
        for buf in (ab, zb):
            buf[:, pl.ds(0, RIM)] = jnp.zeros((levels, RIM, cells, width), jnp.float32)

    @pl.when(lat == n_lat - 1)
    def _():
        for buf in (ab, zb):
            buf[:, pl.ds(RIM + rows, RIM)] = jnp.zeros((levels, RIM, cells, width), jnp.float32)

    for d in small:
        d.wait()
    faces = rows + 5
    lanes = lax.broadcasted_iota(jnp.int32, (cells, total_rows), 1)
    for lv in range(levels):

        @pl.loop(0, faces)
        def _(f):
            row = first + f - 2
            chosen = jnp.logical_and(lanes == row, lanes > 0)
            column = jnp.sum(jnp.where(chosen, mer[lv], 0.0), axis=1, keepdims=True)
            vb[lv, f] = jnp.broadcast_to(column, (cells, width))

        @pl.loop(0, rows)
        def _(r):
            for k, t in enumerate(zonal_taps(fractions[lv, first + r])):
                taps[(lv * rows + r) * 6 + k] = t

    lat_wait(ab, 0)
    for lv in range(levels):

        @pl.loop(0, cells // SUB)
        def _(c):
            at = pl.ds(pl.multiple_of(c * SUB, SUB), SUB)
            ev, q6b, dqb, eb = {}, {}, {}, {}
            carry = None
            y = {r: ab[lv, r + RIM, at, :] for r in range(-3, -1)}
            for f in range(-2, rows + 3):
                y[f] = ab[lv, f + RIM, at, :]
                v = vb[lv, f + 2, at, :]
                north = v > 0.0
                beta, gamma = face_terms(v)
                change = y[f] - y[f - 1]
                ev[f] = v * change
                b = beta * change
                g = -gamma * change
                bn, gn = jnp.where(north, b, 0.0), jnp.where(north, g, 0.0)
                if carry is not None:
                    q6b[f - 1] = bn + carry[0]
                    dqb[f - 1] = gn + carry[1]
                carry = (b - bn, g - gn)
                h = f - 1
                if h >= -1:
                    eb[h] = ev[h] - 3.0 * (q6b[h - 1] + q6b[h]) + (dqb[h - 1] - dqb[h])
                r = h - 2
                if r >= 0:
                    value = (
                        y[r]
                        + 6.0 * q6b[r]
                        + (7.0 / 12.0) * (eb[r] + eb[r + 1])
                        - (1.0 / 12.0) * (eb[r - 1] + eb[r + 2])
                    )
                    q = lv * (rows // step) + r // step
                    gath[1][q][r % step, at, :] = value
                    gath[1][q][
                        r % step, pl.ds(pl.multiple_of(total_cells + c * SUB, SUB), SUB), :
                    ] = value

        for q, (l2, _r) in enumerate(chunks):
            if l2 == lv:
                gather_start(1, q)

    def sweep(a, q, sink, sink_row, sign):
        lv, r0 = chunks[q]
        buf = gath[a][q]

        @pl.loop(0, step)
        def _(r):
            buf[r, pl.ds(total_cells + cells, SUB), :] = buf[r, pl.ds(cells, SUB), :]
            shift = shifts[lv, first + r0 + r]
            if sign < 0:
                start = lax.rem(2 * total_cells - shift - 3, total_cells)
            else:
                start = lax.rem(2 * total_cells + shift - 2, total_cells)
            base = (lv * rows + r0 + r) * 6
            w = [taps[base + k] for k in range(6)]
            if sign > 0:
                w = w[::-1]
            for c in range(cells // SUB):
                total = None
                for k in range(6):
                    term = w[k] * buf[r, pl.ds(start + c * SUB + k, SUB), :]
                    total = term if total is None else total + term
                sink[lv, sink_row + r0 + r, pl.ds(c * SUB, SUB), :] = total

    for b in dup:
        b.wait()
    for i, q in enumerate(order):
        relay(0, q)
        if i > 0:
            gather_finish(0, order[i - 1])
            sweep(0, order[i - 1], zb, RIM, -1)
    gather_finish(0, order[-1])
    sweep(0, order[-1], zb, RIM, -1)
    lat_start(zb, 1)

    relay(1, order[0])
    lat_wait(zb, 1)

    for lv in range(levels):

        @pl.loop(0, cells // SUB)
        def _(c):
            at = pl.ds(pl.multiple_of(c * SUB, SUB), SUB)
            z = {r: zb[lv, r + RIM, at, :] for r in range(-3, 0)}
            e, q6, dq, flux = {}, {}, {}, {}
            for f in range(-1, rows + 2):
                z[f + 1] = zb[lv, f + 1 + RIM, at, :]
                e[f] = (7.0 / 12.0) * (z[f - 1] + z[f]) - (1.0 / 12.0) * (z[f - 2] + z[f + 1])
                u = f - 1
                if u >= -1:
                    q6[u] = 6.0 * z[u] - 3.0 * (e[u] + e[f])
                    dq[u] = e[f] - e[u]
                if u >= 0:
                    v = vb[lv, u + 2, at, :]
                    north = v > 0.0
                    beta, gamma = face_terms(v)
                    flux[u] = (
                        v * e[u]
                        + beta * jnp.where(north, q6[u - 1], q6[u])
                        - gamma * jnp.where(north, dq[u - 1], dq[u])
                    )
                if u >= 1:
                    of[lv, u - 1, at, :] = z[u - 1] - flux[u] + flux[u - 1]

    def finish_adjoint(q):
        lv, r0 = chunks[q]
        gather_finish(1, q)
        sweep(1, q, oa, 0, 1)

    for i in range(1, nq):
        relay(1, order[i])
        finish_adjoint(order[i - 1])
    finish_adjoint(order[-1])

    for a in range(2):
        for q in range(nq):
            gather_drain(a, q)


def reaches(rows, cells, n_lon, n_lat, lat):
    return [reach(cells * n_lon, rows * n_lat, lat * rows + k) + RIM for k in range(rows)]


def fits(levels, rows, cells, n_lon, n_lat):
    if levels != 2 or n_lon != 4 or n_lat != 4 or rows % 8 or cells % SUB:
        return False
    outer = reaches(rows, cells, n_lon, n_lat, 0)[-(rows // 4) :]
    inner = reaches(rows, cells, n_lon, n_lat, 1)
    return cells < min(outer) and max(outer) <= 2 * cells and max(inner) <= cells + SUB


def plan_of(cells, sizes, side):
    slots = []
    at = SUB
    for s in sizes:
        if s >= SUB:
            begins = list(range(0, s - SUB + 1, SUB))
            if s % SUB:
                begins.append(s - SUB)
            shift = cells - s if side == TAIL else 0
            slots.append([(shift + b, at + b) for b in begins])
        elif side == TAIL:
            slots.append([(cells - SUB, at + s - SUB)])
        else:
            slots.append([(0, at)])
        at += s
    return slots, -(-(at - SUB) // SUB) * SUB


def pack_plan(rows, cells, n_lon, n_lat, a, side):
    sizes = [RIM - 1] * rows
    if (side == TAIL) == (a == 0):
        sizes = [min(m, cells) for m in reaches(rows, cells, n_lon, n_lat, 1)]
    return plan_of(cells, sizes, side)


def trim_plan(rows, cells, n_lon, n_lat, a):
    step = rows // 4
    sizes = [m - cells for m in reaches(rows, cells, n_lon, n_lat, 0)[-step:]]
    near = TAIL if a == 0 else HEAD
    return near, plan_of(cells, sizes, near), plan_of(cells, [RIM - 1] * step, 1 - near)


def pack_room(rows, cells, n_lon, n_lat):
    return 2 * SUB + max(
        pack_plan(rows, cells, n_lon, n_lat, a, side)[1] for a in range(2) for side in (HEAD, TAIL)
    )


def trim_room(rows, cells, n_lon, n_lat):
    return 2 * SUB + max(
        plan[1] for a in range(2) for plan in trim_plan(rows, cells, n_lon, n_lat, a)[1:]
    )


def paired(dims, *refs):
    levels, rows, cells, width, n_lon, n_lat, step = dims
    chunks = chunk_list(levels, rows, step)
    nq = len(chunks)
    per = rows // step
    tr, ad, shifts_in, fractions_in, mer_in, of, oa = refs[:7]
    gath = (refs[7 : 7 + nq], refs[7 + nq : 7 + 2 * nq])
    zb, ab, vb, taps, shifts, fractions, mer, held = refs[7 + 2 * nq : 15 + 2 * nq]
    sendp, recvp, sendx, recvx, sendt, recvt = refs[15 + 2 * nq : 21 + 2 * nq]
    loc, sx, sc, sd, st, sh, rf, rc0, rc1, rt, rh, ready = refs[21 + 2 * nq :]
    total_cells = cells * n_lon
    total_rows = rows * n_lat

    me = lax.axis_index("lon")
    lat = lax.axis_index("lat")
    first = lat * rows
    core = lax.rem(me, 2)
    partner = me + 1 - 2 * core
    beside = lax.rem(me + 2, n_lon)
    joint = lax.rem(me + n_lon + 2 * core - 1, n_lon)
    mate = lat + 1 - 2 * lax.rem(lat, 2)
    middle = jnp.logical_and(lat > 0, lat < n_lat - 1)
    polar = jnp.logical_not(middle)

    barrier = pltpu.get_barrier_semaphore()

    def greet(**place):
        pl.semaphore_signal(barrier, inc=1, device_id=place, device_id_type=MESH)

    greet(lon=partner)
    greet(lon=beside)
    greet(lon=joint)

    @pl.when(lat > 0)
    def _():
        greet(lat=lat - 1)

    @pl.when(lat < n_lat - 1)
    def _():
        greet(lat=lat + 1)

    def take(ref, sem):
        pltpu.make_async_copy(ref, ref, sem).wait()

    def lump(m):
        return tr.at[:, pl.ds(0, m * step // levels)]

    for q, (lv, r0) in enumerate(chunks):
        pltpu.make_async_copy(
            tr.at[lv, pl.ds(r0, step)], gath[0][q].at[:, pl.ds(0, cells)], loc.at[lv]
        ).start()
    pltpu.make_async_copy(ad, ab.at[:, pl.ds(RIM, rows)], loc.at[levels]).start()
    small = []
    for k, (source, target) in enumerate(
        ((shifts_in, shifts), (fractions_in, fractions), (mer_in, mer))
    ):
        d = pltpu.make_async_copy(source, target, loc.at[levels + 2 + k])
        d.start()
        small.append(d)
    for q, (lv, r0) in enumerate(chunks):
        pltpu.make_async_copy(
            tr.at[lv, pl.ds(r0, step)],
            gath[0][q].at[:, pl.ds(total_cells, cells)],
            loc.at[levels + 1],
        ).start()

    @pl.when(middle)
    def _():
        pl.semaphore_wait(barrier, 5)
        pl.semaphore_signal(ready, inc=1, device_id={"lat": mate}, device_id_type=MESH)

    @pl.when(polar)
    def _():
        pl.semaphore_wait(barrier, 4)

    def remote(source, target, send, recv, **place):
        return pltpu.make_async_remote_copy(
            source, target, send, recv, device_id=place, device_id_type=MESH
        )

    def lat_copies(buf, k, lv):
        down = remote(
            buf.at[lv, pl.ds(RIM, RIM)],
            buf.at[lv, pl.ds(RIM + rows, RIM)],
            sh.at[k, 0],
            rh.at[k, lv],
            lat=lat - 1,
        )
        up = remote(
            buf.at[lv, pl.ds(rows, RIM)],
            buf.at[lv, pl.ds(0, RIM)],
            sh.at[k, 1],
            rh.at[k, lv],
            lat=lat + 1,
        )
        return down, up

    def lat_start(buf, k, lv):
        down, up = lat_copies(buf, k, lv)

        @pl.when(lat > 0)
        def _():
            down.start()

        @pl.when(lat < n_lat - 1)
        def _():
            up.start()

    def lat_wait(k, lv):
        @pl.when(polar)
        def _():
            take(tr.at[lv, pl.ds(0, RIM)], rh.at[k, lv])

        @pl.when(middle)
        def _():
            take(tr.at[lv, pl.ds(0, 2 * RIM)], rh.at[k, lv])

    own_block = pl.ds(0, cells)
    far_block = pl.ds((n_lon - 2) * cells, cells)

    def x_copy(a, q):
        g = gath[a][q]
        return remote(
            g.at[:, own_block], g.at[:, far_block], sx.at[a], rf.at[a, q], lon=beside
        )

    def core_copy(a, q, dx):
        g = gath[a][q]
        source = ((n_lon - 2 * dx) % n_lon) * cells
        slot = lax.rem(2 * n_lon - 2 * dx + 2 * core - 1, n_lon)
        return remote(
            g.at[:, pl.ds(source, cells)],
            g.at[:, pl.ds(pl.multiple_of(slot * cells, SUB), cells)],
            sc.at[a, dx],
            rc1.at[a, q] if dx else rc0.at[a, q // per],
            lon=partner,
        )

    piece = step // HALVES

    def chunk_at(lv, k, south):
        return lv * per + (k if south else per - 1 - k)

    def polar_half(act):
        for south in (True, False):

            @pl.when(lat == (0 if south else n_lat - 1))
            def _():
                act(south)

    def out_copy(i, h, south):
        q = chunk_at(*DETOUR[i], south)
        return remote(
            gath[1][q].at[pl.ds(h * piece, piece), own_block],
            held.at[i, pl.ds(h * piece, piece)],
            sd.at[0],
            rf.at[(i * HALVES + h) // nq, (i * HALVES + h) % nq],
            lon=beside,
            lat=mate,
        )

    def on_copy(i, h, south):
        q = chunk_at(*DETOUR[i], south)
        return remote(
            held.at[i, pl.ds(h * piece, piece)],
            gath[1][q].at[pl.ds(h * piece, piece), far_block],
            sd.at[0],
            rf.at[1, q],
            lat=mate,
        )

    def trim_copy(a, lv, w):
        long = trims[a][1 + w][1]
        return remote(
            sendt.at[a, lv, w, pl.ds(SUB, long)],
            recvt.at[a, lv, w, pl.ds(SUB, long)],
            st.at[w],
            rt.at[a, lv],
            lon=joint if w else beside,
        )

    trims = [trim_plan(rows, cells, n_lon, n_lat, a) for a in range(2)]
    plans = [[pack_plan(rows, cells, n_lon, n_lat, a, side) for side in (HEAD, TAIL)] for a in range(2)]
    ring = (cells, (n_lon - 1) * cells)
    spill = [
        k for k in range(rows) if reach(total_cells, total_rows, rows + k) + RIM > cells
    ]
    last = (cells - SUB, 0)

    def place_of(lv, k, south):
        r = k if south else rows - 1 - k
        return lv * per + r // step, r % step

    def by_half(act):
        for south in (True, False):

            @pl.when(lat == (1 if south else n_lat - 2))
            def _():
                act(south)

    def pack_copy(a, lv, side):
        long = plans[a][side][1]
        return remote(
            sendp.at[a, lv, pl.ds(SUB, long)],
            recvp.at[a, lv, pl.ds(SUB, long)],
            sc.at[a, 1],
            rc1.at[a, lv],
            lon=joint,
        )

    def few_copy(a):
        return remote(sendx.at[a], recvx.at[a], sx.at[a], rc1.at[a, levels], lon=beside)

    def pack_send(a, lv):
        for side in (HEAD, TAIL):

            @pl.when(core == side)
            def _():
                def fill(south):
                    order = range(rows) if side == HEAD else reversed(range(rows))
                    for k in order:
                        q, j = place_of(lv, k, south)
                        for source, target in plans[a][side][0][k]:
                            sendp[a, lv, pl.ds(target, SUB), :] = gath[a][q][j, pl.ds(source, SUB), :]

                by_half(fill)
                pack_copy(a, lv, side).start()

        if spill:

            def few(south):
                q, j = place_of(lv, spill[0], south)
                sendx[a, pl.ds(lv * SUB, SUB), :] = gath[a][q][j, pl.ds(last[a], SUB), :]

            by_half(few)
            if lv == levels - 1:
                few_copy(a).start()

    def pack_take(a, lv):
        for side in (HEAD, TAIL):

            @pl.when(core == 1 - side)
            def _():
                pack_copy(a, lv, side).wait_recv()

                def empty(south):
                    for k in range(rows):
                        q, j = place_of(lv, k, south)
                        for source, target in plans[a][side][0][k]:
                            gath[a][q][j, pl.ds(ring[side] + source, SUB), :] = recvp[
                                a, lv, pl.ds(target, SUB), :
                            ]

                by_half(empty)

        if spill:
            if lv == 0:
                few_copy(a).wait_recv()

            def few(south):
                q, j = place_of(lv, spill[0], south)
                gath[a][q][j, pl.ds(2 * cells + last[a], SUB), :] = recvx[a, pl.ds(lv * SUB, SUB), :]

            by_half(few)

    def trim_send(a, lv, south):
        near, *pair = trims[a]
        for w in range(2):
            side = 1 - near if w else near
            slots = pair[w][0]
            order = range(step) if side == HEAD else reversed(range(step))
            for k in order:
                q, j = place_of(lv, rows - step + k, south)
                for source, target in slots[k]:
                    sendt[a, lv, w, pl.ds(target, SUB), :] = gath[a][q][j, pl.ds(source, SUB), :]
            trim_copy(a, lv, w).start()

    def trim_take(a, lv, w, south):
        near, *pair = trims[a]
        base = ring[1 - near] if w else 2 * cells
        trim_copy(a, lv, w).wait_recv()
        for k in range(step):
            q, j = place_of(lv, rows - step + k, south)
            for source, target in pair[w][0][k]:
                gath[a][q][j, pl.ds(base + source, SUB), :] = recvt[a, lv, w, pl.ds(target, SUB), :]

    def kind(a, lv, k):
        if k == per - 1:
            return "trim"
        return "detour" if a == 1 and (lv, k) in DETOUR else "direct"

    def far_send(a, lv, k, south):
        q = chunk_at(lv, k, south)
        if kind(a, lv, k) == "detour":
            for h in range(HALVES):
                out_copy(DETOUR.index((lv, k)), h, south).start()
        elif kind(a, lv, k) == "direct":
            x_copy(a, q).start()
        else:

            @pl.when(core == 1 - a)
            def _():
                x_copy(a, q).start()

            @pl.when(core == a)
            def _():
                trim_send(a, lv, south)

    def relay(a, lv, k, south):
        q = chunk_at(lv, k, south)
        if kind(a, lv, k) == "detour":
            take(gath[1][q].at[:, far_block], rf.at[1, q])
            core_copy(a, q, 1).start()
        elif kind(a, lv, k) == "direct":
            x_copy(a, q).wait_recv()
            core_copy(a, q, 1).start()
        else:

            @pl.when(core == 1 - a)
            def _():
                x_copy(a, q).wait_recv()
                core_copy(a, q, 1).start()
                trim_take(a, lv, 1, south)

            @pl.when(core == a)
            def _():
                trim_take(a, lv, 0, south)

    def pass_on(south):
        for i in range(len(DETOUR)):
            for h in range(HALVES):
                out_copy(i, h, south).wait_recv()
                on_copy(i, h, south).start()

    def send_level(a, lv):
        polar_half(lambda south: [far_send(a, lv, k, south) for k in range(per)])

        @pl.when(middle)
        def _():
            pack_send(a, lv)

        for q in range(lv * per, (lv + 1) * per):
            core_copy(a, q, 0).start()

    take(ad, loc.at[levels])
    lat_start(ab, 0, 0)
    for lv in range(levels):
        take(tr.at[lv], loc.at[lv])
        send_level(0, lv)

    @pl.when(lat == 0)
    def _():
        for buf in (ab, zb):
            buf[:, pl.ds(0, RIM)] = jnp.zeros((levels, RIM, cells, width), jnp.float32)

    @pl.when(lat == n_lat - 1)
    def _():
        for buf in (ab, zb):
            buf[:, pl.ds(RIM + rows, RIM)] = jnp.zeros((levels, RIM, cells, width), jnp.float32)

    for d in small:
        d.wait()
    faces = rows + 5
    lanes = lax.broadcasted_iota(jnp.int32, (cells, total_rows), 1)
    for lv in range(levels):

        @pl.loop(0, faces, unroll=faces)
        def _(f):
            row = first + f - 2
            chosen = jnp.logical_and(lanes == row, lanes > 0)
            column = jnp.sum(jnp.where(chosen, mer[lv], 0.0), axis=1, keepdims=True)
            vb[lv, f] = jnp.broadcast_to(column, (cells, width))

        if lv + 1 < levels:
            lat_start(ab, 0, lv + 1)

        @pl.loop(0, rows)
        def _(r):
            for k, t in enumerate(zonal_taps(fractions[lv, first + r])):
                taps[(lv * rows + r) * 6 + k] = t

    for lv in range(levels):
        lat_wait(0, lv)

        @pl.loop(0, cells // SUB)
        def _(c):
            at = pl.ds(pl.multiple_of(c * SUB, SUB), SUB)
            ev, q6b, dqb, eb = {}, {}, {}, {}
            carry = None
            y = {r: ab[lv, r + RIM, at, :] for r in range(-3, -1)}
            for f in range(-2, rows + 3):
                y[f] = ab[lv, f + RIM, at, :]
                v = vb[lv, f + 2, at, :]
                north = v > 0.0
                beta, gamma = face_terms(v)
                change = y[f] - y[f - 1]
                ev[f] = v * change
                b = beta * change
                g = -gamma * change
                bn, gn = jnp.where(north, b, 0.0), jnp.where(north, g, 0.0)
                if carry is not None:
                    q6b[f - 1] = bn + carry[0]
                    dqb[f - 1] = gn + carry[1]
                carry = (b - bn, g - gn)
                h = f - 1
                if h >= -1:
                    eb[h] = ev[h] - 3.0 * (q6b[h - 1] + q6b[h]) + (dqb[h - 1] - dqb[h])
                r = h - 2
                if r >= 0:
                    value = (
                        y[r]
                        + 6.0 * q6b[r]
                        + (7.0 / 12.0) * (eb[r] + eb[r + 1])
                        - (1.0 / 12.0) * (eb[r - 1] + eb[r + 2])
                    )
                    q = lv * per + r // step
                    gath[1][q][r % step, at, :] = value
                    gath[1][q][
                        r % step, pl.ds(pl.multiple_of(total_cells + c * SUB, SUB), SUB), :
                    ] = value

        if lv == 0:

            @pl.when(polar)
            def _():
                pl.semaphore_wait(ready, 1)

        send_level(1, lv)

    def sweep(a, q, sink, sink_row, sign):
        lv, r0 = chunks[q]
        buf = gath[a][q]

        @pl.loop(0, step)
        def _(r):
            buf[r, pl.ds(total_cells + cells, SUB), :] = buf[r, pl.ds(cells, SUB), :]
            shift = shifts[lv, first + r0 + r]
            if sign < 0:
                start = lax.rem(2 * total_cells - shift - 3, total_cells)
            else:
                start = lax.rem(2 * total_cells + shift - 2, total_cells)
            base = (lv * rows + r0 + r) * 6
            w = [taps[base + k] for k in range(6)]
            if sign > 0:
                w = w[::-1]
            for c in range(cells // SUB):
                total = None
                for k in range(6):
                    term = w[k] * buf[r, pl.ds(start + c * SUB + k, SUB), :]
                    total = term if total is None else total + term
                sink[lv, sink_row + r0 + r, pl.ds(c * SUB, SUB), :] = total

    def level_take(a, lv, k=0, south=True):
        take(tr.at[lv], rc0.at[a, lv])

    def finish(a, lv, k, south):
        q = chunk_at(lv, k, south)
        if kind(a, lv, k) == "trim":

            @pl.when(core == a)
            def _():
                core_copy(a, q, 1).wait_recv()

        else:
            core_copy(a, q, 1).wait_recv()
        if a == 0:
            sweep(0, q, zb, RIM, -1)
        else:
            sweep(1, q, oa, 0, 1)

    def polar_steps(a):
        spots = [(lv, k) for lv in range(levels) for k in range(per)]
        direct = [p for p in spots if kind(a, *p) != "detour"]
        due = {p: i + SLOW for i, p in enumerate(direct)}
        due.update({p: i for i, p in enumerate(DETOUR) if a == 1})
        order = sorted(spots, key=lambda p: due[p])
        steps = []
        ready_levels = []
        for i in range(nq + LAG):
            if i < nq:
                steps.append((relay, a) + order[i])
            if i >= LAG:
                lv, k = order[i - LAG]
                if lv not in ready_levels:
                    ready_levels.append(lv)
                    steps.append((level_take, a, lv, k))
                steps.append((finish, a, lv, k))
        return steps

    def polar_run(steps):
        polar_half(lambda south: [step_[0](*step_[1:], south) for step_ in steps])

    def middle_finish(a):
        for lv in range(levels):
            pack_take(a, lv)
            level_take(a, lv)
            for q in range(lv * per, (lv + 1) * per):
                if a == 0:
                    sweep(0, q, zb, RIM, -1)
                else:
                    sweep(1, q, oa, 0, 1)

    take(tr, loc.at[levels + 1])

    polar_run(polar_steps(0))

    @pl.when(middle)
    def _():
        middle_finish(0)

    for lv in range(levels):
        lat_start(zb, 1, lv)

    @pl.when(middle)
    def _():
        by_half(pass_on)
        middle_finish(1)

    late = polar_steps(1)
    polar_run(late[:-LATE])

    for lv in range(levels):
        lat_wait(1, lv)

        @pl.loop(0, cells // SUB)
        def _(c):
            at = pl.ds(pl.multiple_of(c * SUB, SUB), SUB)
            z = {r: zb[lv, r + RIM, at, :] for r in range(-3, 0)}
            e, q6, dq, flux = {}, {}, {}, {}
            for f in range(-1, rows + 2):
                z[f + 1] = zb[lv, f + 1 + RIM, at, :]
                e[f] = (7.0 / 12.0) * (z[f - 1] + z[f]) - (1.0 / 12.0) * (z[f - 2] + z[f + 1])
                u = f - 1
                if u >= -1:
                    q6[u] = 6.0 * z[u] - 3.0 * (e[u] + e[f])
                    dq[u] = e[f] - e[u]
                if u >= 0:
                    v = vb[lv, u + 2, at, :]
                    north = v > 0.0
                    beta, gamma = face_terms(v)
                    flux[u] = (
                        v * e[u]
                        + beta * jnp.where(north, q6[u - 1], q6[u])
                        - gamma * jnp.where(north, dq[u - 1], dq[u])
                    )
                if u >= 1:
                    of[lv, u - 1, at, :] = z[u - 1] - flux[u] + flux[u - 1]

    polar_run(late[-LATE:])

    take(lump(len(DETOUR)), sd.at[0])
    for k in range(2):

        @pl.when(lat > 0)
        def _():
            take(tr.at[:, pl.ds(0, RIM)], sh.at[k, 0])

        @pl.when(lat < n_lat - 1)
        def _():
            take(tr.at[:, pl.ds(0, RIM)], sh.at[k, 1])

    for a in range(2):
        take(tr, sc.at[a, 0])
        straight = nq - levels - (len(DETOUR) if a == 1 else 0)

        @pl.when(jnp.logical_and(polar, core == a))
        def _():
            take(lump(straight), sx.at[a])
            take(lump(nq - levels), sc.at[a, 1])
            for w in range(2):
                take(sendt.at[a, :, w, pl.ds(SUB, trims[a][1 + w][1])], st.at[w])

        @pl.when(jnp.logical_and(polar, core == 1 - a))
        def _():
            take(lump(straight + levels), sx.at[a])
            take(tr, sc.at[a, 1])

        for side in (HEAD, TAIL):

            @pl.when(jnp.logical_and(middle, core == side))
            def _():
                take(sendp.at[a, :, pl.ds(SUB, plans[a][side][1])], sc.at[a, 1])

        if spill:

            @pl.when(middle)
            def _():
                take(sendx.at[a], sx.at[a])


def store(f_in, a_in, f_out, a_out, sem):
    one = pltpu.make_async_copy(f_in, f_out, sem.at[0])
    two = pltpu.make_async_copy(a_in, a_out, sem.at[1])
    one.start()
    two.start()
    one.wait()
    two.wait()


def local(tracers, adjoint_in, shifts, fractions, meridional):
    levels, rows, cells, width = tracers.shape
    n_lon, n_lat = lax.axis_size("lon"), lax.axis_size("lat")
    n_x = n_lon // 2
    pair = fits(levels, rows, cells, n_lon, n_lat)
    step = max(1, rows // (4 if pair else 2))
    nq = levels * (rows // step)
    dma = pltpu.SemaphoreType.DMA
    block = pltpu.VMEM((step, (n_lon + 1) * cells + SUB, width), jnp.float32)
    banded = pltpu.VMEM((levels, rows + 2 * RIM, cells, width), jnp.float32)
    scratch = [block] * (2 * nq) + [
        banded,
        banded,
        pltpu.VMEM((levels, rows + 5, cells, width), jnp.float32),
        pltpu.SMEM((levels * rows * 6,), jnp.float32),
        pltpu.SMEM(shifts.shape, jnp.int32),
        pltpu.SMEM(fractions.shape, jnp.float32),
        pltpu.VMEM((levels, cells, meridional.shape[1]), jnp.float32),
    ]
    if pair:
        nd = len(DETOUR)
        dims = (levels, rows, cells, width, n_lon, n_lat, step)
        long = pack_room(rows, cells, n_lon, n_lat)
        pack = pltpu.VMEM((2, levels, long, width), jnp.float32)
        trim = pltpu.VMEM(
            (2, levels, 2, trim_room(rows, cells, n_lon, n_lat), width), jnp.float32
        )
        few = pltpu.VMEM((2, levels * SUB, width), jnp.float32)
        body = paired
        scratch += [
            pltpu.VMEM((nd, step, cells, width), jnp.float32),
            pack,
            pack,
            few,
            few,
            trim,
            trim,
            dma((levels + 5,)),
            dma((2,)),
            dma((2, 2)),
            dma((1,)),
            dma((2,)),
            dma((2, 2)),
            dma((2, nq)),
            dma((2, levels)),
            dma((2, nq)),
            dma((2, levels)),
            dma((2, levels)),
            pltpu.SemaphoreType.REGULAR,
        ]
    else:
        dims = (levels, rows, cells, width, n_lon, n_lat, step)
        body = general
        scratch += [
            dma((2 * nq + 4,)),
            dma((2, nq, 2 * n_x)),
            dma((2, nq, 2 * n_x)),
            dma((2, 2)),
            dma((2, 2)),
        ]
    vmem = pl.BlockSpec(memory_space=pltpu.VMEM)
    far = pl.BlockSpec(memory_space=pltpu.HBM)
    kept = pltpu.VMEM(tracers.shape, jnp.float32)
    staged = pl.pallas_call(
        functools.partial(body, dims),
        out_shape=(kept, kept),
        in_specs=[far] * 5,
        out_specs=(vmem, vmem),
        scratch_shapes=scratch,
        compiler_params=pltpu.CompilerParams(
            collective_id=0, has_side_effects=True, vmem_limit_bytes=60 << 20
        ),
    )(tracers, adjoint_in, shifts, fractions, jnp.swapaxes(meridional, 1, 2))
    final = jax.ShapeDtypeStruct(tracers.shape, jnp.float32)
    return pl.pallas_call(
        store,
        out_shape=(final, final),
        in_specs=[vmem, vmem],
        out_specs=(far, far),
        scratch_shapes=[dma((2,))],
        compiler_params=pltpu.CompilerParams(vmem_limit_bytes=4 << 20),
    )(*staged)


def solution(mesh):
    block = P("grp", "lat", "lon", None)
    in_specs = (block, block, P(), P(), P(None, None, "lon"))
    return jax.shard_map(
        local, mesh=mesh, in_specs=in_specs, out_specs=(block, block), check_vma=False
    )
```

```python
import functools

import jax
import jax.numpy as jnp
from jax import lax
from jax.experimental import pallas as pl
from jax.experimental.pallas import tpu as pltpu
from jax.sharding import PartitionSpec as P

MESH = pl.DeviceIdType.MESH
SUB = 8
RIM = 3
LAG = 2
LATE = 3
HALVES = 2
SLOW = 2.4
DETOUR = ((0, 0), (0, 1), (0, 2), (1, 0), (1, 1))
SINGLE = ((0, 2),)
HEAD, TAIL = 0, 1


def chunk_list(levels, rows, step):
    return [(lv, r0) for lv in range(levels) for r0 in range(0, rows, step)]


def reach(total_cells, total_rows, row):
    d = abs(2 * row + 1 - total_rows)
    return (total_cells - 1) * d * d // ((total_rows - 1) * (total_rows - 1))


def face_terms(v):
    size = jnp.abs(v)
    beta = v * (0.5 * size) * (1.0 - size * (2.0 / 3.0))
    return beta, 0.5 * v * v


def zonal_taps(c):
    b = 1.0 - c * (2.0 / 3.0)
    p = c * (1.0 - 0.5 * c - 1.5 * c * b)
    q = c * (0.5 * c - 1.5 * c * b)
    r = 3.0 * c * c * b
    d = p - q
    t = 1.0 / 12.0
    s = 7.0 / 12.0
    return (
        -t * q,
        s * q - t * d,
        r + t * p + s * d + s * q,
        1.0 - r - s * p + s * d - t * q,
        -s * p - t * d,
        t * p,
    )


def general(dims, *refs):
    levels, rows, cells, width, n_lon, n_lat, step = dims
    chunks = chunk_list(levels, rows, step)
    nq = len(chunks)
    tr, ad, shifts_in, fractions_in, mer_in, of, oa = refs[:7]
    gath = (refs[7 : 7 + nq], refs[7 + nq : 7 + 2 * nq])
    zb, ab, vb, taps, shifts, fractions, mer, loc, ssem, rsem, hs, hr = refs[7 + 2 * nq :]
    total_cells = cells * n_lon
    total_rows = rows * n_lat
    n_x = n_lon // 2

    me = lax.axis_index("lon")
    lat = lax.axis_index("lat")
    first = lat * rows
    core = lax.rem(me, 2)
    partner = me + 1 - 2 * core
    order = list(range(nq))

    own = []
    dup = []
    for q, (lv, r0) in enumerate(chunks):
        a = pltpu.make_async_copy(
            tr.at[lv, pl.ds(r0, step)], gath[0][q].at[:, pl.ds(0, cells)], loc.at[q]
        )
        a.start()
        own.append(a)
    adc = pltpu.make_async_copy(ad, ab.at[:, pl.ds(RIM, rows)], loc.at[2 * nq])
    adc.start()
    for q, (lv, r0) in enumerate(chunks):
        b = pltpu.make_async_copy(
            tr.at[lv, pl.ds(r0, step)],
            gath[0][q].at[:, pl.ds(total_cells, cells)],
            loc.at[nq + q],
        )
        b.start()
        dup.append(b)

    small = []
    for k, (source, target) in enumerate(
        ((shifts_in, shifts), (fractions_in, fractions), (mer_in, mer))
    ):
        d = pltpu.make_async_copy(source, target, loc.at[2 * nq + 1 + k])
        d.start()
        small.append(d)

    barrier = pltpu.get_barrier_semaphore()
    pl.semaphore_signal(barrier, inc=1, device_id={"lon": partner}, device_id_type=MESH)
    for dx in range(1, n_x):
        pl.semaphore_signal(
            barrier, inc=1, device_id={"lon": lax.rem(me + 2 * dx, n_lon)}, device_id_type=MESH
        )

    @pl.when(lat > 0)
    def _():
        pl.semaphore_signal(barrier, inc=1, device_id={"lat": lat - 1}, device_id_type=MESH)

    @pl.when(lat < n_lat - 1)
    def _():
        pl.semaphore_signal(barrier, inc=1, device_id={"lat": lat + 1}, device_id_type=MESH)

    inner = jnp.logical_and(lat > 0, lat < n_lat - 1)

    @pl.when(inner)
    def _():
        pl.semaphore_wait(barrier, n_x + 2)

    @pl.when(jnp.logical_not(inner))
    def _():
        pl.semaphore_wait(barrier, n_x + min(n_lat - 1, 1))

    def lat_copies(buf, k):
        down = pltpu.make_async_remote_copy(
            buf.at[:, pl.ds(RIM, RIM)],
            buf.at[:, pl.ds(RIM + rows, RIM)],
            hs.at[k, 0],
            hr.at[k, 0],
            device_id={"lat": lat - 1},
            device_id_type=MESH,
        )
        up = pltpu.make_async_remote_copy(
            buf.at[:, pl.ds(rows, RIM)],
            buf.at[:, pl.ds(0, RIM)],
            hs.at[k, 1],
            hr.at[k, 1],
            device_id={"lat": lat + 1},
            device_id_type=MESH,
        )
        return down, up

    def lat_start(buf, k):
        down, up = lat_copies(buf, k)

        @pl.when(lat > 0)
        def _():
            down.start()

        @pl.when(lat < n_lat - 1)
        def _():
            up.start()

    def lat_wait(buf, k):
        down, up = lat_copies(buf, k)

        @pl.when(lat > 0)
        def _():
            down.wait_send()
            up.wait_recv()

        @pl.when(lat < n_lat - 1)
        def _():
            up.wait_send()
            down.wait_recv()

    def x_copy(a, q, dx, span):
        lo, hi = span
        return pltpu.make_async_remote_copy(
            gath[a][q].at[:, pl.ds(lo, hi - lo)],
            gath[a][q].at[:, pl.ds((n_lon - 2 * dx) * cells + lo, hi - lo)],
            ssem.at[a, q, dx],
            rsem.at[a, q, dx],
            device_id={"lon": lax.rem(me + 2 * dx, n_lon)},
            device_id_type=MESH,
        )

    def core_copy(a, q, dx, span):
        lo, hi = span
        source = ((n_lon - 2 * dx) % n_lon) * cells + lo
        slot = lax.rem(2 * n_lon - 2 * dx + 2 * core - 1, n_lon)
        return pltpu.make_async_remote_copy(
            gath[a][q].at[:, pl.ds(source, hi - lo)],
            gath[a][q].at[:, pl.ds(pl.multiple_of(slot * cells + lo, SUB), hi - lo)],
            ssem.at[a, q, n_x + dx],
            rsem.at[a, q, n_x + dx],
            device_id={"lon": partner},
            device_id_type=MESH,
        )

    whole = (0, cells)

    def gather_start(a, q):
        for dx in range(1, n_x):
            x_copy(a, q, dx, whole).start()
        core_copy(a, q, 0, whole).start()

    def relay(a, q):
        for dx in range(1, n_x):
            x_copy(a, q, dx, whole).wait_recv()
            core_copy(a, q, dx, whole).start()

    def gather_finish(a, q):
        for dx in range(n_x):
            core_copy(a, q, dx, whole).wait_recv()

    def gather_drain(a, q):
        for dx in range(n_x):
            core_copy(a, q, dx, whole).wait_send()
        for dx in range(1, n_x):
            x_copy(a, q, dx, whole).wait_send()

    adc.wait()
    lat_start(ab, 0)
    for q in range(nq):
        own[q].wait()
        gather_start(0, q)

    @pl.when(lat == 0)
    def _():
        for buf in (ab, zb):
            buf[:, pl.ds(0, RIM)] = jnp.zeros((levels, RIM, cells, width), jnp.float32)

    @pl.when(lat == n_lat - 1)
    def _():
        for buf in (ab, zb):
            buf[:, pl.ds(RIM + rows, RIM)] = jnp.zeros((levels, RIM, cells, width), jnp.float32)

    for d in small:
        d.wait()
    faces = rows + 5
    lanes = lax.broadcasted_iota(jnp.int32, (cells, total_rows), 1)
    for lv in range(levels):

        @pl.loop(0, faces)
        def _(f):
            row = first + f - 2
            chosen = jnp.logical_and(lanes == row, lanes > 0)
            column = jnp.sum(jnp.where(chosen, mer[lv], 0.0), axis=1, keepdims=True)
            vb[lv, f] = jnp.broadcast_to(column, (cells, width))

        @pl.loop(0, rows)
        def _(r):
            for k, t in enumerate(zonal_taps(fractions[lv, first + r])):
                taps[(lv * rows + r) * 6 + k] = t

    lat_wait(ab, 0)
    for lv in range(levels):

        @pl.loop(0, cells // SUB)
        def _(c):
            at = pl.ds(pl.multiple_of(c * SUB, SUB), SUB)
            ev, q6b, dqb, eb = {}, {}, {}, {}
            carry = None
            y = {r: ab[lv, r + RIM, at, :] for r in range(-3, -1)}
            for f in range(-2, rows + 3):
                y[f] = ab[lv, f + RIM, at, :]
                v = vb[lv, f + 2, at, :]
                north = v > 0.0
                beta, gamma = face_terms(v)
                change = y[f] - y[f - 1]
                ev[f] = v * change
                b = beta * change
                g = -gamma * change
                bn, gn = jnp.where(north, b, 0.0), jnp.where(north, g, 0.0)
                if carry is not None:
                    q6b[f - 1] = bn + carry[0]
                    dqb[f - 1] = gn + carry[1]
                carry = (b - bn, g - gn)
                h = f - 1
                if h >= -1:
                    eb[h] = ev[h] - 3.0 * (q6b[h - 1] + q6b[h]) + (dqb[h - 1] - dqb[h])
                r = h - 2
                if r >= 0:
                    value = (
                        y[r]
                        + 6.0 * q6b[r]
                        + (7.0 / 12.0) * (eb[r] + eb[r + 1])
                        - (1.0 / 12.0) * (eb[r - 1] + eb[r + 2])
                    )
                    q = lv * (rows // step) + r // step
                    gath[1][q][r % step, at, :] = value
                    gath[1][q][
                        r % step, pl.ds(pl.multiple_of(total_cells + c * SUB, SUB), SUB), :
                    ] = value

        for q, (l2, _r) in enumerate(chunks):
            if l2 == lv:
                gather_start(1, q)

    def sweep(a, q, sink, sink_row, sign):
        lv, r0 = chunks[q]
        buf = gath[a][q]

        @pl.loop(0, step)
        def _(r):
            buf[r, pl.ds(total_cells + cells, SUB), :] = buf[r, pl.ds(cells, SUB), :]
            shift = shifts[lv, first + r0 + r]
            if sign < 0:
                start = lax.rem(2 * total_cells - shift - 3, total_cells)
            else:
                start = lax.rem(2 * total_cells + shift - 2, total_cells)
            base = (lv * rows + r0 + r) * 6
            w = [taps[base + k] for k in range(6)]
            if sign > 0:
                w = w[::-1]
            for c in range(cells // SUB):
                total = None
                for k in range(6):
                    term = w[k] * buf[r, pl.ds(start + c * SUB + k, SUB), :]
                    total = term if total is None else total + term
                sink[lv, sink_row + r0 + r, pl.ds(c * SUB, SUB), :] = total

    for b in dup:
        b.wait()
    for i, q in enumerate(order):
        relay(0, q)
        if i > 0:
            gather_finish(0, order[i - 1])
            sweep(0, order[i - 1], zb, RIM, -1)
    gather_finish(0, order[-1])
    sweep(0, order[-1], zb, RIM, -1)
    lat_start(zb, 1)

    relay(1, order[0])
    lat_wait(zb, 1)

    for lv in range(levels):

        @pl.loop(0, cells // SUB)
        def _(c):
            at = pl.ds(pl.multiple_of(c * SUB, SUB), SUB)
            z = {r: zb[lv, r + RIM, at, :] for r in range(-3, 0)}
            e, q6, dq, flux = {}, {}, {}, {}
            for f in range(-1, rows + 2):
                z[f + 1] = zb[lv, f + 1 + RIM, at, :]
                e[f] = (7.0 / 12.0) * (z[f - 1] + z[f]) - (1.0 / 12.0) * (z[f - 2] + z[f + 1])
                u = f - 1
                if u >= -1:
                    q6[u] = 6.0 * z[u] - 3.0 * (e[u] + e[f])
                    dq[u] = e[f] - e[u]
                if u >= 0:
                    v = vb[lv, u + 2, at, :]
                    north = v > 0.0
                    beta, gamma = face_terms(v)
                    flux[u] = (
                        v * e[u]
                        + beta * jnp.where(north, q6[u - 1], q6[u])
                        - gamma * jnp.where(north, dq[u - 1], dq[u])
                    )
                if u >= 1:
                    of[lv, u - 1, at, :] = z[u - 1] - flux[u] + flux[u - 1]

    def finish_adjoint(q):
        lv, r0 = chunks[q]
        gather_finish(1, q)
        sweep(1, q, oa, 0, 1)

    for i in range(1, nq):
        relay(1, order[i])
        finish_adjoint(order[i - 1])
    finish_adjoint(order[-1])

    for a in range(2):
        for q in range(nq):
            gather_drain(a, q)


def reaches(rows, cells, n_lon, n_lat, lat):
    return [reach(cells * n_lon, rows * n_lat, lat * rows + k) + RIM for k in range(rows)]


def fits(levels, rows, cells, n_lon, n_lat):
    if levels != 2 or n_lon != 4 or n_lat != 4 or rows % 8 or cells % SUB:
        return False
    outer = reaches(rows, cells, n_lon, n_lat, 0)[-(rows // 4) :]
    inner = reaches(rows, cells, n_lon, n_lat, 1)
    return cells < min(outer) and max(outer) <= 2 * cells and max(inner) <= cells + SUB


def plan_of(cells, sizes, side):
    slots = []
    at = SUB
    for s in sizes:
        if s >= SUB:
            begins = list(range(0, s - SUB + 1, SUB))
            if s % SUB:
                begins.append(s - SUB)
            shift = cells - s if side == TAIL else 0
            slots.append([(shift + b, at + b) for b in begins])
        elif side == TAIL:
            slots.append([(cells - SUB, at + s - SUB)])
        else:
            slots.append([(0, at)])
        at += s
    return slots, -(-(at - SUB) // SUB) * SUB


def pack_plan(rows, cells, n_lon, n_lat, a, side):
    sizes = [RIM - 1] * rows
    if (side == TAIL) == (a == 0):
        sizes = [min(m, cells) for m in reaches(rows, cells, n_lon, n_lat, 1)]
    return plan_of(cells, sizes, side)


def trim_plan(rows, cells, n_lon, n_lat, a):
    step = rows // 4
    sizes = [m - cells for m in reaches(rows, cells, n_lon, n_lat, 0)[-step:]]
    near = TAIL if a == 0 else HEAD
    return near, plan_of(cells, sizes, near), plan_of(cells, [RIM - 1] * step, 1 - near)


def pack_room(rows, cells, n_lon, n_lat):
    return 2 * SUB + max(
        pack_plan(rows, cells, n_lon, n_lat, a, side)[1] for a in range(2) for side in (HEAD, TAIL)
    )


def trim_room(rows, cells, n_lon, n_lat):
    return 2 * SUB + max(
        plan[1] for a in range(2) for plan in trim_plan(rows, cells, n_lon, n_lat, a)[1:]
    )


def paired(dims, *refs):
    levels, rows, cells, width, n_lon, n_lat, step = dims
    chunks = chunk_list(levels, rows, step)
    nq = len(chunks)
    per = rows // step
    tr, ad, shifts_in, fractions_in, mer_in, of, oa = refs[:7]
    gath = (refs[7 : 7 + nq], refs[7 + nq : 7 + 2 * nq])
    zb, ab, vb, taps, shifts, fractions, mer, held = refs[7 + 2 * nq : 15 + 2 * nq]
    sendp, recvp, sendx, recvx, sendt, recvt = refs[15 + 2 * nq : 21 + 2 * nq]
    loc, sx, sc, sd, st, sh, rf, rc0, rc1, rt, rh, ready = refs[21 + 2 * nq :]
    total_cells = cells * n_lon
    total_rows = rows * n_lat

    me = lax.axis_index("lon")
    lat = lax.axis_index("lat")
    first = lat * rows
    core = lax.rem(me, 2)
    partner = me + 1 - 2 * core
    beside = lax.rem(me + 2, n_lon)
    joint = lax.rem(me + n_lon + 2 * core - 1, n_lon)
    mate = lat + 1 - 2 * lax.rem(lat, 2)
    middle = jnp.logical_and(lat > 0, lat < n_lat - 1)
    polar = jnp.logical_not(middle)

    barrier = pltpu.get_barrier_semaphore()

    def greet(**place):
        pl.semaphore_signal(barrier, inc=1, device_id=place, device_id_type=MESH)

    greet(lon=partner)
    greet(lon=beside)
    greet(lon=joint)

    @pl.when(lat > 0)
    def _():
        greet(lat=lat - 1)

    @pl.when(lat < n_lat - 1)
    def _():
        greet(lat=lat + 1)

    def take(ref, sem):
        pltpu.make_async_copy(ref, ref, sem).wait()

    def lump(m):
        return tr.at[:, pl.ds(0, m * step // levels)]

    for q, (lv, r0) in enumerate(chunks):
        pltpu.make_async_copy(
            tr.at[lv, pl.ds(r0, step)], gath[0][q].at[:, pl.ds(0, cells)], loc.at[lv]
        ).start()
    pltpu.make_async_copy(ad, ab.at[:, pl.ds(RIM, rows)], loc.at[levels]).start()
    small = []
    for k, (source, target) in enumerate(
        ((shifts_in, shifts), (fractions_in, fractions), (mer_in, mer))
    ):
        d = pltpu.make_async_copy(source, target, loc.at[levels + 2 + k])
        d.start()
        small.append(d)
    for q, (lv, r0) in enumerate(chunks):
        pltpu.make_async_copy(
            tr.at[lv, pl.ds(r0, step)],
            gath[0][q].at[:, pl.ds(total_cells, cells)],
            loc.at[levels + 1],
        ).start()

    @pl.when(middle)
    def _():
        pl.semaphore_wait(barrier, 5)
        pl.semaphore_signal(ready, inc=1, device_id={"lat": mate}, device_id_type=MESH)

    @pl.when(polar)
    def _():
        pl.semaphore_wait(barrier, 4)

    def remote(source, target, send, recv, **place):
        return pltpu.make_async_remote_copy(
            source, target, send, recv, device_id=place, device_id_type=MESH
        )

    def lat_copies(buf, k, lv):
        down = remote(
            buf.at[lv, pl.ds(RIM, RIM)],
            buf.at[lv, pl.ds(RIM + rows, RIM)],
            sh.at[k, 0],
            rh.at[k, lv],
            lat=lat - 1,
        )
        up = remote(
            buf.at[lv, pl.ds(rows, RIM)],
            buf.at[lv, pl.ds(0, RIM)],
            sh.at[k, 1],
            rh.at[k, lv],
            lat=lat + 1,
        )
        return down, up

    def lat_start(buf, k, lv):
        down, up = lat_copies(buf, k, lv)

        @pl.when(lat > 0)
        def _():
            down.start()

        @pl.when(lat < n_lat - 1)
        def _():
            up.start()

    def lat_wait(k, lv):
        @pl.when(polar)
        def _():
            take(tr.at[lv, pl.ds(0, RIM)], rh.at[k, lv])

        @pl.when(middle)
        def _():
            take(tr.at[lv, pl.ds(0, 2 * RIM)], rh.at[k, lv])

    own_block = pl.ds(0, cells)
    far_block = pl.ds((n_lon - 2) * cells, cells)

    def x_copy(a, q):
        g = gath[a][q]
        return remote(
            g.at[:, own_block], g.at[:, far_block], sx.at[a], rf.at[a, q], lon=beside
        )

    def core_copy(a, q, dx):
        g = gath[a][q]
        source = ((n_lon - 2 * dx) % n_lon) * cells
        slot = lax.rem(2 * n_lon - 2 * dx + 2 * core - 1, n_lon)
        return remote(
            g.at[:, pl.ds(source, cells)],
            g.at[:, pl.ds(pl.multiple_of(slot * cells, SUB), cells)],
            sc.at[a, dx],
            rc1.at[a, q] if dx else rc0.at[a, q // per],
            lon=partner,
        )

    piece = step // HALVES

    def chunk_at(lv, k, south):
        return lv * per + (k if south else per - 1 - k)

    def polar_half(act):
        for south in (True, False):

            @pl.when(lat == (0 if south else n_lat - 1))
            def _():
                act(south)

    def out_copy(i, h, south):
        q = chunk_at(*DETOUR[i], south)
        return remote(
            gath[1][q].at[pl.ds(h * piece, piece), own_block],
            held.at[i, pl.ds(h * piece, piece)],
            sd.at[0],
            rf.at[(i * HALVES + h) // nq, (i * HALVES + h) % nq],
            lon=beside,
            lat=mate,
        )

    def on_copy(i, h, south):
        q = chunk_at(*DETOUR[i], south)
        return remote(
            held.at[i, pl.ds(h * piece, piece)],
            gath[1][q].at[pl.ds(h * piece, piece), far_block],
            sd.at[0],
            rf.at[1, q],
            lat=mate,
        )

    def trim_copy(a, lv, w):
        long = trims[a][1 + w][1]
        return remote(
            sendt.at[a, lv, w, pl.ds(SUB, long)],
            recvt.at[a, lv, w, pl.ds(SUB, long)],
            st.at[w],
            rt.at[a, lv],
            lon=joint if w else beside,
        )

    trims = [trim_plan(rows, cells, n_lon, n_lat, a) for a in range(2)]
    plans = [[pack_plan(rows, cells, n_lon, n_lat, a, side) for side in (HEAD, TAIL)] for a in range(2)]
    ring = (cells, (n_lon - 1) * cells)
    spill = [
        k for k in range(rows) if reach(total_cells, total_rows, rows + k) + RIM > cells
    ]
    last = (cells - SUB, 0)

    def place_of(lv, k, south):
        r = k if south else rows - 1 - k
        return lv * per + r // step, r % step

    def by_half(act):
        for south in (True, False):

            @pl.when(lat == (1 if south else n_lat - 2))
            def _():
                act(south)

    def pack_copy(a, lv, side):
        long = plans[a][side][1]
        return remote(
            sendp.at[a, lv, pl.ds(SUB, long)],
            recvp.at[a, lv, pl.ds(SUB, long)],
            sc.at[a, 1],
            rc1.at[a, lv],
            lon=joint,
        )

    def few_copy(a):
        return remote(sendx.at[a], recvx.at[a], sx.at[a], rc1.at[a, levels], lon=beside)

    def pack_send(a, lv):
        for side in (HEAD, TAIL):

            @pl.when(core == side)
            def _():
                def fill(south):
                    order = range(rows) if side == HEAD else reversed(range(rows))
                    for k in order:
                        q, j = place_of(lv, k, south)
                        for source, target in plans[a][side][0][k]:
                            sendp[a, lv, pl.ds(target, SUB), :] = gath[a][q][j, pl.ds(source, SUB), :]

                by_half(fill)
                pack_copy(a, lv, side).start()

        if spill:

            def few(south):
                q, j = place_of(lv, spill[0], south)
                sendx[a, pl.ds(lv * SUB, SUB), :] = gath[a][q][j, pl.ds(last[a], SUB), :]

            by_half(few)
            if lv == levels - 1:
                few_copy(a).start()

    def pack_take(a, lv):
        for side in (HEAD, TAIL):

            @pl.when(core == 1 - side)
            def _():
                pack_copy(a, lv, side).wait_recv()

                def empty(south):
                    for k in range(rows):
                        q, j = place_of(lv, k, south)
                        for source, target in plans[a][side][0][k]:
                            gath[a][q][j, pl.ds(ring[side] + source, SUB), :] = recvp[
                                a, lv, pl.ds(target, SUB), :
                            ]

                by_half(empty)

        if spill:
            if lv == 0:
                few_copy(a).wait_recv()

            def few(south):
                q, j = place_of(lv, spill[0], south)
                gath[a][q][j, pl.ds(2 * cells + last[a], SUB), :] = recvx[a, pl.ds(lv * SUB, SUB), :]

            by_half(few)

    def trim_send(a, lv, south):
        near, *pair = trims[a]
        for w in range(2):
            side = 1 - near if w else near
            slots = pair[w][0]
            order = range(step) if side == HEAD else reversed(range(step))
            for k in order:
                q, j = place_of(lv, rows - step + k, south)
                for source, target in slots[k]:
                    sendt[a, lv, w, pl.ds(target, SUB), :] = gath[a][q][j, pl.ds(source, SUB), :]
            trim_copy(a, lv, w).start()

    def trim_take(a, lv, w, south):
        near, *pair = trims[a]
        base = ring[1 - near] if w else 2 * cells
        trim_copy(a, lv, w).wait_recv()
        for k in range(step):
            q, j = place_of(lv, rows - step + k, south)
            for source, target in pair[w][0][k]:
                gath[a][q][j, pl.ds(base + source, SUB), :] = recvt[a, lv, w, pl.ds(target, SUB), :]

    def kind(a, lv, k):
        if k == per - 1:
            return "trim"
        return "detour" if a == 1 and (lv, k) in DETOUR else "direct"

    def far_send(a, lv, k, south):
        q = chunk_at(lv, k, south)
        if kind(a, lv, k) == "detour":

            def around():
                for h in range(HALVES):
                    out_copy(DETOUR.index((lv, k)), h, south).start()

            if (lv, k) not in SINGLE:
                around()
            else:
                pl.when(core == 1)(around)
                pl.when(core == 0)(x_copy(a, q).start)
        elif kind(a, lv, k) == "direct":
            x_copy(a, q).start()
        else:

            @pl.when(core == 1 - a)
            def _():
                x_copy(a, q).start()

            @pl.when(core == a)
            def _():
                trim_send(a, lv, south)

    def relay(a, lv, k, south):
        q = chunk_at(lv, k, south)
        if kind(a, lv, k) == "detour":
            take(gath[1][q].at[:, far_block], rf.at[1, q])
            core_copy(a, q, 1).start()
        elif kind(a, lv, k) == "direct":
            x_copy(a, q).wait_recv()
            core_copy(a, q, 1).start()
        else:

            @pl.when(core == 1 - a)
            def _():
                x_copy(a, q).wait_recv()
                core_copy(a, q, 1).start()
                trim_take(a, lv, 1, south)

            @pl.when(core == a)
            def _():
                trim_take(a, lv, 0, south)

    def pass_on(south):
        for i, spot in enumerate(DETOUR):

            def hand():
                for h in range(HALVES):
                    out_copy(i, h, south).wait_recv()
                    on_copy(i, h, south).start()

            if spot in SINGLE:
                pl.when(core == 1)(hand)
            else:
                hand()

    def send_level(a, lv):
        polar_half(lambda south: [far_send(a, lv, k, south) for k in range(per)])

        @pl.when(middle)
        def _():
            pack_send(a, lv)

        for q in range(lv * per, (lv + 1) * per):
            core_copy(a, q, 0).start()

    take(ad, loc.at[levels])
    lat_start(ab, 0, 0)
    for lv in range(levels):
        take(tr.at[lv], loc.at[lv])
        send_level(0, lv)

    @pl.when(lat == 0)
    def _():
        for buf in (ab, zb):
            buf[:, pl.ds(0, RIM)] = jnp.zeros((levels, RIM, cells, width), jnp.float32)

    @pl.when(lat == n_lat - 1)
    def _():
        for buf in (ab, zb):
            buf[:, pl.ds(RIM + rows, RIM)] = jnp.zeros((levels, RIM, cells, width), jnp.float32)

    for d in small:
        d.wait()
    faces = rows + 5
    lanes = lax.broadcasted_iota(jnp.int32, (cells, total_rows), 1)
    for lv in range(levels):

        @pl.loop(0, faces, unroll=faces)
        def _(f):
            row = first + f - 2
            chosen = jnp.logical_and(lanes == row, lanes > 0)
            column = jnp.sum(jnp.where(chosen, mer[lv], 0.0), axis=1, keepdims=True)
            vb[lv, f] = jnp.broadcast_to(column, (cells, width))

        if lv + 1 < levels:
            lat_start(ab, 0, lv + 1)

        @pl.loop(0, rows)
        def _(r):
            for k, t in enumerate(zonal_taps(fractions[lv, first + r])):
                taps[(lv * rows + r) * 6 + k] = t

    def sweep(a, q, sink, sink_row, sign):
        lv, r0 = chunks[q]
        buf = gath[a][q]

        @pl.loop(0, step)
        def _(r):
            buf[r, pl.ds(total_cells + cells, SUB), :] = buf[r, pl.ds(cells, SUB), :]
            shift = shifts[lv, first + r0 + r]
            if sign < 0:
                start = lax.rem(2 * total_cells - shift - 3, total_cells)
            else:
                start = lax.rem(2 * total_cells + shift - 2, total_cells)
            base = (lv * rows + r0 + r) * 6
            w = [taps[base + k] for k in range(6)]
            if sign > 0:
                w = w[::-1]
            for c in range(cells // SUB):
                total = None
                for k in range(6):
                    term = w[k] * buf[r, pl.ds(start + c * SUB + k, SUB), :]
                    total = term if total is None else total + term
                sink[lv, sink_row + r0 + r, pl.ds(c * SUB, SUB), :] = total

    def level_take(a, lv, k=0, south=True):
        take(tr.at[lv], rc0.at[a, lv])

    def finish(a, lv, k, south):
        q = chunk_at(lv, k, south)
        if kind(a, lv, k) == "trim":

            @pl.when(core == a)
            def _():
                core_copy(a, q, 1).wait_recv()

        else:
            core_copy(a, q, 1).wait_recv()
        if a == 0:
            sweep(0, q, zb, RIM, -1)
        else:
            sweep(1, q, oa, 0, 1)

    def polar_steps(a):
        spots = [(lv, k) for lv in range(levels) for k in range(per)]
        direct = [p for p in spots if kind(a, *p) != "detour"]
        due = {p: i + SLOW for i, p in enumerate(direct)}
        due.update({p: i for i, p in enumerate(DETOUR) if a == 1})
        order = sorted(spots, key=lambda p: due[p])
        steps = []
        ready_levels = []
        for i in range(nq + LAG):
            if i < nq:
                steps.append((relay, a) + order[i])
            if i >= LAG:
                lv, k = order[i - LAG]
                if lv not in ready_levels:
                    ready_levels.append(lv)
                    steps.append((level_take, a, lv, k))
                steps.append((finish, a, lv, k))
        return steps

    def polar_run(steps):
        polar_half(lambda south: [step_[0](*step_[1:], south) for step_ in steps])

    def middle_finish(a):
        for lv in range(levels):
            pack_take(a, lv)
            level_take(a, lv)
            for q in range(lv * per, (lv + 1) * per):
                if a == 0:
                    sweep(0, q, zb, RIM, -1)
                else:
                    sweep(1, q, oa, 0, 1)

    take(tr, loc.at[levels + 1])

    @pl.when(middle)
    def _():
        middle_finish(0)
        for lv in range(levels):
            lat_start(zb, 1, lv)

    for lv in range(levels):
        lat_wait(0, lv)

        @pl.loop(0, cells // SUB)
        def _(c):
            at = pl.ds(pl.multiple_of(c * SUB, SUB), SUB)
            ev, q6b, dqb, eb = {}, {}, {}, {}
            carry = None
            y = {r: ab[lv, r + RIM, at, :] for r in range(-3, -1)}
            for f in range(-2, rows + 3):
                y[f] = ab[lv, f + RIM, at, :]
                v = vb[lv, f + 2, at, :]
                north = v > 0.0
                beta, gamma = face_terms(v)
                change = y[f] - y[f - 1]
                ev[f] = v * change
                b = beta * change
                g = -gamma * change
                bn, gn = jnp.where(north, b, 0.0), jnp.where(north, g, 0.0)
                if carry is not None:
                    q6b[f - 1] = bn + carry[0]
                    dqb[f - 1] = gn + carry[1]
                carry = (b - bn, g - gn)
                h = f - 1
                if h >= -1:
                    eb[h] = ev[h] - 3.0 * (q6b[h - 1] + q6b[h]) + (dqb[h - 1] - dqb[h])
                r = h - 2
                if r >= 0:
                    value = (
                        y[r]
                        + 6.0 * q6b[r]
                        + (7.0 / 12.0) * (eb[r] + eb[r + 1])
                        - (1.0 / 12.0) * (eb[r - 1] + eb[r + 2])
                    )
                    q = lv * per + r // step
                    gath[1][q][r % step, at, :] = value
                    gath[1][q][
                        r % step, pl.ds(pl.multiple_of(total_cells + c * SUB, SUB), SUB), :
                    ] = value

        if lv == 0:

            @pl.when(polar)
            def _():
                pl.semaphore_wait(ready, 1)

        send_level(1, lv)


    polar_run(polar_steps(0))

    @pl.when(polar)
    def _():
        for lv in range(levels):
            lat_start(zb, 1, lv)

    @pl.when(middle)
    def _():
        by_half(pass_on)
        middle_finish(1)

    late = polar_steps(1)
    polar_run(late[:-LATE])

    for lv in range(levels):
        lat_wait(1, lv)

        @pl.loop(0, cells // SUB)
        def _(c):
            at = pl.ds(pl.multiple_of(c * SUB, SUB), SUB)
            z = {r: zb[lv, r + RIM, at, :] for r in range(-3, 0)}
            e, q6, dq, flux = {}, {}, {}, {}
            for f in range(-1, rows + 2):
                z[f + 1] = zb[lv, f + 1 + RIM, at, :]
                e[f] = (7.0 / 12.0) * (z[f - 1] + z[f]) - (1.0 / 12.0) * (z[f - 2] + z[f + 1])
                u = f - 1
                if u >= -1:
                    q6[u] = 6.0 * z[u] - 3.0 * (e[u] + e[f])
                    dq[u] = e[f] - e[u]
                if u >= 0:
                    v = vb[lv, u + 2, at, :]
                    north = v > 0.0
                    beta, gamma = face_terms(v)
                    flux[u] = (
                        v * e[u]
                        + beta * jnp.where(north, q6[u - 1], q6[u])
                        - gamma * jnp.where(north, dq[u - 1], dq[u])
                    )
                if u >= 1:
                    of[lv, u - 1, at, :] = z[u - 1] - flux[u] + flux[u - 1]

    polar_run(late[-LATE:])

    for side in (HEAD, TAIL):

        @pl.when(core == side)
        def _():
            take(lump(len(DETOUR) - (len(SINGLE) if side == 0 else 0)), sd.at[0])

    for k in range(2):

        @pl.when(lat > 0)
        def _():
            take(tr.at[:, pl.ds(0, RIM)], sh.at[k, 0])

        @pl.when(lat < n_lat - 1)
        def _():
            take(tr.at[:, pl.ds(0, RIM)], sh.at[k, 1])

    for a in range(2):
        take(tr, sc.at[a, 0])
        around = (len(DETOUR) - len(SINGLE), len(DETOUR)) if a == 1 else (0, 0)
        straight = [nq - levels - m for m in around]

        @pl.when(jnp.logical_and(polar, core == a))
        def _():
            take(lump(straight[a]), sx.at[a])
            take(lump(nq - levels), sc.at[a, 1])
            for w in range(2):
                take(sendt.at[a, :, w, pl.ds(SUB, trims[a][1 + w][1])], st.at[w])

        @pl.when(jnp.logical_and(polar, core == 1 - a))
        def _():
            take(lump(straight[1 - a] + levels), sx.at[a])
            take(tr, sc.at[a, 1])

        for side in (HEAD, TAIL):

            @pl.when(jnp.logical_and(middle, core == side))
            def _():
                take(sendp.at[a, :, pl.ds(SUB, plans[a][side][1])], sc.at[a, 1])

        if spill:

            @pl.when(middle)
            def _():
                take(sendx.at[a], sx.at[a])


def store(f_in, a_in, f_out, a_out, sem):
    one = pltpu.make_async_copy(f_in, f_out, sem.at[0])
    two = pltpu.make_async_copy(a_in, a_out, sem.at[1])
    one.start()
    two.start()
    one.wait()
    two.wait()


def local(tracers, adjoint_in, shifts, fractions, meridional):
    levels, rows, cells, width = tracers.shape
    n_lon, n_lat = lax.axis_size("lon"), lax.axis_size("lat")
    n_x = n_lon // 2
    pair = fits(levels, rows, cells, n_lon, n_lat)
    step = max(1, rows // (4 if pair else 2))
    nq = levels * (rows // step)
    dma = pltpu.SemaphoreType.DMA
    block = pltpu.VMEM((step, (n_lon + 1) * cells + SUB, width), jnp.float32)
    banded = pltpu.VMEM((levels, rows + 2 * RIM, cells, width), jnp.float32)
    scratch = [block] * (2 * nq) + [
        banded,
        banded,
        pltpu.VMEM((levels, rows + 5, cells, width), jnp.float32),
        pltpu.SMEM((levels * rows * 6,), jnp.float32),
        pltpu.SMEM(shifts.shape, jnp.int32),
        pltpu.SMEM(fractions.shape, jnp.float32),
        pltpu.VMEM((levels, cells, meridional.shape[1]), jnp.float32),
    ]
    if pair:
        nd = len(DETOUR)
        dims = (levels, rows, cells, width, n_lon, n_lat, step)
        long = pack_room(rows, cells, n_lon, n_lat)
        pack = pltpu.VMEM((2, levels, long, width), jnp.float32)
        trim = pltpu.VMEM(
            (2, levels, 2, trim_room(rows, cells, n_lon, n_lat), width), jnp.float32
        )
        few = pltpu.VMEM((2, levels * SUB, width), jnp.float32)
        body = paired
        scratch += [
            pltpu.VMEM((nd, step, cells, width), jnp.float32),
            pack,
            pack,
            few,
            few,
            trim,
            trim,
            dma((levels + 5,)),
            dma((2,)),
            dma((2, 2)),
            dma((1,)),
            dma((2,)),
            dma((2, 2)),
            dma((2, nq)),
            dma((2, levels)),
            dma((2, nq)),
            dma((2, levels)),
            dma((2, levels)),
            pltpu.SemaphoreType.REGULAR,
        ]
    else:
        dims = (levels, rows, cells, width, n_lon, n_lat, step)
        body = general
        scratch += [
            dma((2 * nq + 4,)),
            dma((2, nq, 2 * n_x)),
            dma((2, nq, 2 * n_x)),
            dma((2, 2)),
            dma((2, 2)),
        ]
    vmem = pl.BlockSpec(memory_space=pltpu.VMEM)
    far = pl.BlockSpec(memory_space=pltpu.HBM)
    kept = pltpu.VMEM(tracers.shape, jnp.float32)
    staged = pl.pallas_call(
        functools.partial(body, dims),
        out_shape=(kept, kept),
        in_specs=[far] * 5,
        out_specs=(vmem, vmem),
        scratch_shapes=scratch,
        compiler_params=pltpu.CompilerParams(
            collective_id=0, has_side_effects=True, vmem_limit_bytes=60 << 20
        ),
    )(tracers, adjoint_in, shifts, fractions, jnp.swapaxes(meridional, 1, 2))
    final = jax.ShapeDtypeStruct(tracers.shape, jnp.float32)
    return pl.pallas_call(
        store,
        out_shape=(final, final),
        in_specs=[vmem, vmem],
        out_specs=(far, far),
        scratch_shapes=[dma((2,))],
        compiler_params=pltpu.CompilerParams(vmem_limit_bytes=4 << 20),
    )(*staged)


def solution(mesh):
    block = P("grp", "lat", "lon", None)
    in_specs = (block, block, P(), P(), P(None, None, "lon"))
    return jax.shard_map(
        local, mesh=mesh, in_specs=in_specs, out_specs=(block, block), check_vma=False
    )
```

```python
import functools

import jax
import jax.numpy as jnp
from jax import lax
from jax.experimental import pallas as pl
from jax.experimental.pallas import tpu as pltpu
from jax.sharding import PartitionSpec as P

MESH = pl.DeviceIdType.MESH
SUB = 8
RIM = 3
LAG = 2
LATE = 3
HALVES = 2
SLOW = 2.4
DETOUR = ((0, 0), (0, 1), (0, 2), (1, 0), (1, 1))
SINGLE = ((0, 2),)
HEAD, TAIL = 0, 1


def chunk_list(levels, rows, step):
    return [(lv, r0) for lv in range(levels) for r0 in range(0, rows, step)]


def reach(total_cells, total_rows, row):
    d = abs(2 * row + 1 - total_rows)
    return (total_cells - 1) * d * d // ((total_rows - 1) * (total_rows - 1))


def face_terms(v):
    size = jnp.abs(v)
    beta = v * (0.5 * size) * (1.0 - size * (2.0 / 3.0))
    return beta, 0.5 * v * v


def zonal_taps(c):
    b = 1.0 - c * (2.0 / 3.0)
    p = c * (1.0 - 0.5 * c - 1.5 * c * b)
    q = c * (0.5 * c - 1.5 * c * b)
    r = 3.0 * c * c * b
    d = p - q
    t = 1.0 / 12.0
    s = 7.0 / 12.0
    return (
        -t * q,
        s * q - t * d,
        r + t * p + s * d + s * q,
        1.0 - r - s * p + s * d - t * q,
        -s * p - t * d,
        t * p,
    )


def general(dims, *refs):
    levels, rows, cells, width, n_lon, n_lat, step = dims
    chunks = chunk_list(levels, rows, step)
    nq = len(chunks)
    tr, ad, shifts_in, fractions_in, mer_in, of, oa = refs[:7]
    gath = (refs[7 : 7 + nq], refs[7 + nq : 7 + 2 * nq])
    zb, ab, vb, taps, shifts, fractions, mer, loc, ssem, rsem, hs, hr = refs[7 + 2 * nq :]
    total_cells = cells * n_lon
    total_rows = rows * n_lat
    n_x = n_lon // 2

    me = lax.axis_index("lon")
    lat = lax.axis_index("lat")
    first = lat * rows
    core = lax.rem(me, 2)
    partner = me + 1 - 2 * core
    order = list(range(nq))

    own = []
    dup = []
    for q, (lv, r0) in enumerate(chunks):
        a = pltpu.make_async_copy(
            tr.at[lv, pl.ds(r0, step)], gath[0][q].at[:, pl.ds(0, cells)], loc.at[q]
        )
        a.start()
        own.append(a)
    adc = pltpu.make_async_copy(ad, ab.at[:, pl.ds(RIM, rows)], loc.at[2 * nq])
    adc.start()
    for q, (lv, r0) in enumerate(chunks):
        b = pltpu.make_async_copy(
            tr.at[lv, pl.ds(r0, step)],
            gath[0][q].at[:, pl.ds(total_cells, cells)],
            loc.at[nq + q],
        )
        b.start()
        dup.append(b)

    small = []
    for k, (source, target) in enumerate(
        ((shifts_in, shifts), (fractions_in, fractions), (mer_in, mer))
    ):
        d = pltpu.make_async_copy(source, target, loc.at[2 * nq + 1 + k])
        d.start()
        small.append(d)

    barrier = pltpu.get_barrier_semaphore()
    pl.semaphore_signal(barrier, inc=1, device_id={"lon": partner}, device_id_type=MESH)
    for dx in range(1, n_x):
        pl.semaphore_signal(
            barrier, inc=1, device_id={"lon": lax.rem(me + 2 * dx, n_lon)}, device_id_type=MESH
        )

    @pl.when(lat > 0)
    def _():
        pl.semaphore_signal(barrier, inc=1, device_id={"lat": lat - 1}, device_id_type=MESH)

    @pl.when(lat < n_lat - 1)
    def _():
        pl.semaphore_signal(barrier, inc=1, device_id={"lat": lat + 1}, device_id_type=MESH)

    inner = jnp.logical_and(lat > 0, lat < n_lat - 1)

    @pl.when(inner)
    def _():
        pl.semaphore_wait(barrier, n_x + 2)

    @pl.when(jnp.logical_not(inner))
    def _():
        pl.semaphore_wait(barrier, n_x + min(n_lat - 1, 1))

    def lat_copies(buf, k):
        down = pltpu.make_async_remote_copy(
            buf.at[:, pl.ds(RIM, RIM)],
            buf.at[:, pl.ds(RIM + rows, RIM)],
            hs.at[k, 0],
            hr.at[k, 0],
            device_id={"lat": lat - 1},
            device_id_type=MESH,
        )
        up = pltpu.make_async_remote_copy(
            buf.at[:, pl.ds(rows, RIM)],
            buf.at[:, pl.ds(0, RIM)],
            hs.at[k, 1],
            hr.at[k, 1],
            device_id={"lat": lat + 1},
            device_id_type=MESH,
        )
        return down, up

    def lat_start(buf, k):
        down, up = lat_copies(buf, k)

        @pl.when(lat > 0)
        def _():
            down.start()

        @pl.when(lat < n_lat - 1)
        def _():
            up.start()

    def lat_wait(buf, k):
        down, up = lat_copies(buf, k)

        @pl.when(lat > 0)
        def _():
            down.wait_send()
            up.wait_recv()

        @pl.when(lat < n_lat - 1)
        def _():
            up.wait_send()
            down.wait_recv()

    def x_copy(a, q, dx, span):
        lo, hi = span
        return pltpu.make_async_remote_copy(
            gath[a][q].at[:, pl.ds(lo, hi - lo)],
            gath[a][q].at[:, pl.ds((n_lon - 2 * dx) * cells + lo, hi - lo)],
            ssem.at[a, q, dx],
            rsem.at[a, q, dx],
            device_id={"lon": lax.rem(me + 2 * dx, n_lon)},
            device_id_type=MESH,
        )

    def core_copy(a, q, dx, span):
        lo, hi = span
        source = ((n_lon - 2 * dx) % n_lon) * cells + lo
        slot = lax.rem(2 * n_lon - 2 * dx + 2 * core - 1, n_lon)
        return pltpu.make_async_remote_copy(
            gath[a][q].at[:, pl.ds(source, hi - lo)],
            gath[a][q].at[:, pl.ds(pl.multiple_of(slot * cells + lo, SUB), hi - lo)],
            ssem.at[a, q, n_x + dx],
            rsem.at[a, q, n_x + dx],
            device_id={"lon": partner},
            device_id_type=MESH,
        )

    whole = (0, cells)

    def gather_start(a, q):
        for dx in range(1, n_x):
            x_copy(a, q, dx, whole).start()
        core_copy(a, q, 0, whole).start()

    def relay(a, q):
        for dx in range(1, n_x):
            x_copy(a, q, dx, whole).wait_recv()
            core_copy(a, q, dx, whole).start()

    def gather_finish(a, q):
        for dx in range(n_x):
            core_copy(a, q, dx, whole).wait_recv()

    def gather_drain(a, q):
        for dx in range(n_x):
            core_copy(a, q, dx, whole).wait_send()
        for dx in range(1, n_x):
            x_copy(a, q, dx, whole).wait_send()

    adc.wait()
    lat_start(ab, 0)
    for q in range(nq):
        own[q].wait()
        gather_start(0, q)

    @pl.when(lat == 0)
    def _():
        for buf in (ab, zb):
            buf[:, pl.ds(0, RIM)] = jnp.zeros((levels, RIM, cells, width), jnp.float32)

    @pl.when(lat == n_lat - 1)
    def _():
        for buf in (ab, zb):
            buf[:, pl.ds(RIM + rows, RIM)] = jnp.zeros((levels, RIM, cells, width), jnp.float32)

    for d in small:
        d.wait()
    faces = rows + 5
    lanes = lax.broadcasted_iota(jnp.int32, (cells, total_rows), 1)
    for lv in range(levels):

        @pl.loop(0, faces)
        def _(f):
            row = first + f - 2
            chosen = jnp.logical_and(lanes == row, lanes > 0)
            column = jnp.sum(jnp.where(chosen, mer[lv], 0.0), axis=1, keepdims=True)
            vb[lv, f] = jnp.broadcast_to(column, (cells, width))

        @pl.loop(0, rows)
        def _(r):
            for k, t in enumerate(zonal_taps(fractions[lv, first + r])):
                taps[(lv * rows + r) * 6 + k] = t

    lat_wait(ab, 0)
    for lv in range(levels):

        @pl.loop(0, cells // SUB)
        def _(c):
            at = pl.ds(pl.multiple_of(c * SUB, SUB), SUB)
            ev, q6b, dqb, eb = {}, {}, {}, {}
            carry = None
            y = {r: ab[lv, r + RIM, at, :] for r in range(-3, -1)}
            for f in range(-2, rows + 3):
                y[f] = ab[lv, f + RIM, at, :]
                v = vb[lv, f + 2, at, :]
                north = v > 0.0
                beta, gamma = face_terms(v)
                change = y[f] - y[f - 1]
                ev[f] = v * change
                b = beta * change
                g = -gamma * change
                bn, gn = jnp.where(north, b, 0.0), jnp.where(north, g, 0.0)
                if carry is not None:
                    q6b[f - 1] = bn + carry[0]
                    dqb[f - 1] = gn + carry[1]
                carry = (b - bn, g - gn)
                h = f - 1
                if h >= -1:
                    eb[h] = ev[h] - 3.0 * (q6b[h - 1] + q6b[h]) + (dqb[h - 1] - dqb[h])
                r = h - 2
                if r >= 0:
                    value = (
                        y[r]
                        + 6.0 * q6b[r]
                        + (7.0 / 12.0) * (eb[r] + eb[r + 1])
                        - (1.0 / 12.0) * (eb[r - 1] + eb[r + 2])
                    )
                    q = lv * (rows // step) + r // step
                    gath[1][q][r % step, at, :] = value
                    gath[1][q][
                        r % step, pl.ds(pl.multiple_of(total_cells + c * SUB, SUB), SUB), :
                    ] = value

        for q, (l2, _r) in enumerate(chunks):
            if l2 == lv:
                gather_start(1, q)

    def sweep(a, q, sink, sink_row, sign):
        lv, r0 = chunks[q]
        buf = gath[a][q]

        @pl.loop(0, step)
        def _(r):
            buf[r, pl.ds(total_cells + cells, SUB), :] = buf[r, pl.ds(cells, SUB), :]
            shift = shifts[lv, first + r0 + r]
            if sign < 0:
                start = lax.rem(2 * total_cells - shift - 3, total_cells)
            else:
                start = lax.rem(2 * total_cells + shift - 2, total_cells)
            base = (lv * rows + r0 + r) * 6
            w = [taps[base + k] for k in range(6)]
            if sign > 0:
                w = w[::-1]
            for c in range(cells // SUB):
                total = None
                for k in range(6):
                    term = w[k] * buf[r, pl.ds(start + c * SUB + k, SUB), :]
                    total = term if total is None else total + term
                sink[lv, sink_row + r0 + r, pl.ds(c * SUB, SUB), :] = total

    for b in dup:
        b.wait()
    for i, q in enumerate(order):
        relay(0, q)
        if i > 0:
            gather_finish(0, order[i - 1])
            sweep(0, order[i - 1], zb, RIM, -1)
    gather_finish(0, order[-1])
    sweep(0, order[-1], zb, RIM, -1)
    lat_start(zb, 1)

    relay(1, order[0])
    lat_wait(zb, 1)

    for lv in range(levels):

        @pl.loop(0, cells // SUB)
        def _(c):
            at = pl.ds(pl.multiple_of(c * SUB, SUB), SUB)
            z = {r: zb[lv, r + RIM, at, :] for r in range(-3, 0)}
            e, q6, dq, flux = {}, {}, {}, {}
            for f in range(-1, rows + 2):
                z[f + 1] = zb[lv, f + 1 + RIM, at, :]
                e[f] = (7.0 / 12.0) * (z[f - 1] + z[f]) - (1.0 / 12.0) * (z[f - 2] + z[f + 1])
                u = f - 1
                if u >= -1:
                    q6[u] = 6.0 * z[u] - 3.0 * (e[u] + e[f])
                    dq[u] = e[f] - e[u]
                if u >= 0:
                    v = vb[lv, u + 2, at, :]
                    north = v > 0.0
                    beta, gamma = face_terms(v)
                    flux[u] = (
                        v * e[u]
                        + beta * jnp.where(north, q6[u - 1], q6[u])
                        - gamma * jnp.where(north, dq[u - 1], dq[u])
                    )
                if u >= 1:
                    of[lv, u - 1, at, :] = z[u - 1] - flux[u] + flux[u - 1]

    def finish_adjoint(q):
        lv, r0 = chunks[q]
        gather_finish(1, q)
        sweep(1, q, oa, 0, 1)

    for i in range(1, nq):
        relay(1, order[i])
        finish_adjoint(order[i - 1])
    finish_adjoint(order[-1])

    for a in range(2):
        for q in range(nq):
            gather_drain(a, q)


def reaches(rows, cells, n_lon, n_lat, lat):
    return [reach(cells * n_lon, rows * n_lat, lat * rows + k) + RIM for k in range(rows)]


def fits(levels, rows, cells, n_lon, n_lat):
    if levels != 2 or n_lon != 4 or n_lat != 4 or rows % 8 or cells % SUB:
        return False
    outer = reaches(rows, cells, n_lon, n_lat, 0)[-(rows // 4) :]
    inner = reaches(rows, cells, n_lon, n_lat, 1)
    return cells < min(outer) and max(outer) <= 2 * cells and max(inner) <= cells + SUB


def plan_of(cells, sizes, side):
    slots = []
    at = SUB
    for s in sizes:
        if s >= SUB:
            begins = list(range(0, s - SUB + 1, SUB))
            if s % SUB:
                begins.append(s - SUB)
            shift = cells - s if side == TAIL else 0
            slots.append([(shift + b, at + b) for b in begins])
        elif side == TAIL:
            slots.append([(cells - SUB, at + s - SUB)])
        else:
            slots.append([(0, at)])
        at += s
    return slots, -(-(at - SUB) // SUB) * SUB


def pack_plan(rows, cells, n_lon, n_lat, a, side):
    sizes = [RIM - 1] * rows
    if (side == TAIL) == (a == 0):
        sizes = [min(m, cells) for m in reaches(rows, cells, n_lon, n_lat, 1)]
    return plan_of(cells, sizes, side)


def trim_plan(rows, cells, n_lon, n_lat, a):
    step = rows // 4
    sizes = [m - cells for m in reaches(rows, cells, n_lon, n_lat, 0)[-step:]]
    near = TAIL if a == 0 else HEAD
    return near, plan_of(cells, sizes, near), plan_of(cells, [RIM - 1] * step, 1 - near)


def pack_room(rows, cells, n_lon, n_lat):
    return 2 * SUB + max(
        pack_plan(rows, cells, n_lon, n_lat, a, side)[1] for a in range(2) for side in (HEAD, TAIL)
    )


def trim_room(rows, cells, n_lon, n_lat):
    return 2 * SUB + max(
        plan[1] for a in range(2) for plan in trim_plan(rows, cells, n_lon, n_lat, a)[1:]
    )


def paired(dims, *refs):
    levels, rows, cells, width, n_lon, n_lat, step = dims
    chunks = chunk_list(levels, rows, step)
    nq = len(chunks)
    per = rows // step
    tr, ad, shifts_in, fractions_in, mer_in, of, oa = refs[:7]
    gath = (refs[7 : 7 + nq], refs[7 + nq : 7 + 2 * nq])
    zb, ab, vb, taps, shifts, fractions, mer, held = refs[7 + 2 * nq : 15 + 2 * nq]
    sendp, recvp, sendx, recvx, sendt, recvt = refs[15 + 2 * nq : 21 + 2 * nq]
    loc, sx, sc, sd, st, sh, rf, rc0, rc1, rh, ready = refs[21 + 2 * nq :]
    total_cells = cells * n_lon
    total_rows = rows * n_lat

    me = lax.axis_index("lon")
    lat = lax.axis_index("lat")
    first = lat * rows
    core = lax.rem(me, 2)
    partner = me + 1 - 2 * core
    beside = lax.rem(me + 2, n_lon)
    joint = lax.rem(me + n_lon + 2 * core - 1, n_lon)
    mate = lat + 1 - 2 * lax.rem(lat, 2)
    middle = jnp.logical_and(lat > 0, lat < n_lat - 1)
    polar = jnp.logical_not(middle)

    barrier = pltpu.get_barrier_semaphore()

    def greet(**place):
        pl.semaphore_signal(barrier, inc=1, device_id=place, device_id_type=MESH)

    greet(lon=partner)
    greet(lon=beside)
    greet(lon=joint)

    @pl.when(lat > 0)
    def _():
        greet(lat=lat - 1)

    @pl.when(lat < n_lat - 1)
    def _():
        greet(lat=lat + 1)

    def take(ref, sem):
        pltpu.make_async_copy(ref, ref, sem).wait()

    def lump(m):
        return tr.at[:, pl.ds(0, m * step // levels)]

    for q, (lv, r0) in enumerate(chunks):
        pltpu.make_async_copy(
            tr.at[lv, pl.ds(r0, step)], gath[0][q].at[:, pl.ds(0, cells)], loc.at[lv]
        ).start()
    pltpu.make_async_copy(ad, ab.at[:, pl.ds(RIM, rows)], loc.at[levels]).start()
    small = []
    for k, (source, target) in enumerate(
        ((shifts_in, shifts), (fractions_in, fractions), (mer_in, mer))
    ):
        d = pltpu.make_async_copy(source, target, loc.at[levels + 2 + k])
        d.start()
        small.append(d)
    for q, (lv, r0) in enumerate(chunks):
        pltpu.make_async_copy(
            tr.at[lv, pl.ds(r0, step)],
            gath[0][q].at[:, pl.ds(total_cells, cells)],
            loc.at[levels + 1],
        ).start()

    @pl.when(middle)
    def _():
        pl.semaphore_wait(barrier, 5)
        pl.semaphore_signal(ready, inc=1, device_id={"lat": mate}, device_id_type=MESH)

    @pl.when(polar)
    def _():
        pl.semaphore_wait(barrier, 4)

    def remote(source, target, send, recv, **place):
        return pltpu.make_async_remote_copy(
            source, target, send, recv, device_id=place, device_id_type=MESH
        )

    def lat_copies(buf, k, lv):
        down = remote(
            buf.at[lv, pl.ds(RIM, RIM)],
            buf.at[lv, pl.ds(RIM + rows, RIM)],
            sh.at[k, 0],
            rh.at[k, lv],
            lat=lat - 1,
        )
        up = remote(
            buf.at[lv, pl.ds(rows, RIM)],
            buf.at[lv, pl.ds(0, RIM)],
            sh.at[k, 1],
            rh.at[k, lv],
            lat=lat + 1,
        )
        return down, up

    def lat_start(buf, k, lv):
        down, up = lat_copies(buf, k, lv)

        @pl.when(lat > 0)
        def _():
            down.start()

        @pl.when(lat < n_lat - 1)
        def _():
            up.start()

    def lat_wait(k, lv):
        @pl.when(polar)
        def _():
            take(tr.at[lv, pl.ds(0, RIM)], rh.at[k, lv])

        @pl.when(middle)
        def _():
            take(tr.at[lv, pl.ds(0, 2 * RIM)], rh.at[k, lv])

    own_block = pl.ds(0, cells)
    far_block = pl.ds((n_lon - 2) * cells, cells)

    def x_copy(a, q):
        g = gath[a][q]
        return remote(
            g.at[:, own_block], g.at[:, far_block], sx.at[a], rf.at[a, q], lon=beside
        )

    def core_copy(a, q, dx):
        g = gath[a][q]
        source = ((n_lon - 2 * dx) % n_lon) * cells
        slot = lax.rem(2 * n_lon - 2 * dx + 2 * core - 1, n_lon)
        return remote(
            g.at[:, pl.ds(source, cells)],
            g.at[:, pl.ds(pl.multiple_of(slot * cells, SUB), cells)],
            sc.at[a, dx],
            rc1.at[a, q] if dx else rc0.at[a, q // per],
            lon=partner,
        )

    piece = step // HALVES

    def chunk_at(lv, k, south):
        return lv * per + (k if south else per - 1 - k)

    def polar_half(act):
        for south in (True, False):

            @pl.when(lat == (0 if south else n_lat - 1))
            def _():
                act(south)

    def out_copy(i, h, south):
        q = chunk_at(*DETOUR[i], south)
        return remote(
            gath[1][q].at[pl.ds(h * piece, piece), own_block],
            held.at[i, pl.ds(h * piece, piece)],
            sd.at[0],
            rf.at[(i * HALVES + h) // nq, (i * HALVES + h) % nq],
            lon=beside,
            lat=mate,
        )

    def on_copy(i, h, south):
        q = chunk_at(*DETOUR[i], south)
        return remote(
            held.at[i, pl.ds(h * piece, piece)],
            gath[1][q].at[pl.ds(h * piece, piece), far_block],
            sd.at[0],
            rf.at[1, q],
            lat=mate,
        )

    def trim_copy(a, lv, w, south):
        q = chunk_at(lv, per - 1, south)
        long = trims[a][1 + w][1]
        return remote(
            sendt.at[a, lv, w, pl.ds(SUB, long)],
            recvt.at[a, lv, w, pl.ds(SUB, long)],
            st.at[w],
            rc1.at[a, q] if w else rf.at[a, q],
            lon=joint if w else beside,
        )

    trims = [trim_plan(rows, cells, n_lon, n_lat, a) for a in range(2)]
    plans = [[pack_plan(rows, cells, n_lon, n_lat, a, side) for side in (HEAD, TAIL)] for a in range(2)]
    ring = (cells, (n_lon - 1) * cells)
    spill = [
        k for k in range(rows) if reach(total_cells, total_rows, rows + k) + RIM > cells
    ]
    last = (cells - SUB, 0)

    def place_of(lv, k, south):
        r = k if south else rows - 1 - k
        return lv * per + r // step, r % step

    def by_half(act):
        for south in (True, False):

            @pl.when(lat == (1 if south else n_lat - 2))
            def _():
                act(south)

    def pack_copy(a, lv, side):
        long = plans[a][side][1]
        return remote(
            sendp.at[a, lv, pl.ds(SUB, long)],
            recvp.at[a, lv, pl.ds(SUB, long)],
            sc.at[a, 1],
            rc1.at[a, lv],
            lon=joint,
        )

    def few_copy(a):
        return remote(sendx.at[a], recvx.at[a], sx.at[a], rc1.at[a, levels], lon=beside)

    def pack_send(a, lv):
        for side in (HEAD, TAIL):

            @pl.when(core == side)
            def _():
                def fill(south):
                    order = range(rows) if side == HEAD else reversed(range(rows))
                    for k in order:
                        q, j = place_of(lv, k, south)
                        for source, target in plans[a][side][0][k]:
                            sendp[a, lv, pl.ds(target, SUB), :] = gath[a][q][j, pl.ds(source, SUB), :]

                by_half(fill)
                pack_copy(a, lv, side).start()

        if spill:

            def few(south):
                q, j = place_of(lv, spill[0], south)
                sendx[a, pl.ds(lv * SUB, SUB), :] = gath[a][q][j, pl.ds(last[a], SUB), :]

            by_half(few)
            if lv == levels - 1:
                few_copy(a).start()

    def pack_take(a, lv):
        for side in (HEAD, TAIL):

            @pl.when(core == 1 - side)
            def _():
                pack_copy(a, lv, side).wait_recv()

                def empty(south):
                    for k in range(rows):
                        q, j = place_of(lv, k, south)
                        for source, target in plans[a][side][0][k]:
                            gath[a][q][j, pl.ds(ring[side] + source, SUB), :] = recvp[
                                a, lv, pl.ds(target, SUB), :
                            ]

                by_half(empty)

        if spill:
            if lv == 0:
                few_copy(a).wait_recv()

            def few(south):
                q, j = place_of(lv, spill[0], south)
                gath[a][q][j, pl.ds(2 * cells + last[a], SUB), :] = recvx[a, pl.ds(lv * SUB, SUB), :]

            by_half(few)

    def trim_send(a, lv, south):
        near, *pair = trims[a]
        for w in range(2):
            side = 1 - near if w else near
            slots = pair[w][0]
            order = range(step) if side == HEAD else reversed(range(step))
            for k in order:
                q, j = place_of(lv, rows - step + k, south)
                for source, target in slots[k]:
                    sendt[a, lv, w, pl.ds(target, SUB), :] = gath[a][q][j, pl.ds(source, SUB), :]
            trim_copy(a, lv, w, south).start()

    def trim_take(a, lv, w, south):
        near, *pair = trims[a]
        base = ring[1 - near] if w else 2 * cells
        trim_copy(a, lv, w, south).wait_recv()
        for k in range(step):
            q, j = place_of(lv, rows - step + k, south)
            for source, target in pair[w][0][k]:
                gath[a][q][j, pl.ds(base + source, SUB), :] = recvt[a, lv, w, pl.ds(target, SUB), :]

    def kind(a, lv, k):
        if k == per - 1:
            return "trim"
        return "detour" if a == 1 and (lv, k) in DETOUR else "direct"

    def far_send(a, lv, k, south):
        q = chunk_at(lv, k, south)
        if kind(a, lv, k) == "detour":

            def around():
                for h in range(HALVES):
                    out_copy(DETOUR.index((lv, k)), h, south).start()

            if (lv, k) not in SINGLE:
                around()
            else:
                pl.when(core == 1)(around)
                pl.when(core == 0)(x_copy(a, q).start)
        elif kind(a, lv, k) == "direct":
            x_copy(a, q).start()
        else:

            @pl.when(core == 1 - a)
            def _():
                x_copy(a, q).start()

            @pl.when(core == a)
            def _():
                trim_send(a, lv, south)

    def relay(a, lv, k, south):
        q = chunk_at(lv, k, south)
        if kind(a, lv, k) == "detour":
            take(gath[1][q].at[:, far_block], rf.at[1, q])
            core_copy(a, q, 1).start()
        elif kind(a, lv, k) == "direct":
            x_copy(a, q).wait_recv()
            core_copy(a, q, 1).start()
        else:

            @pl.when(core == 1 - a)
            def _():
                x_copy(a, q).wait_recv()
                core_copy(a, q, 1).start()
                trim_take(a, lv, 1, south)

            @pl.when(core == a)
            def _():
                trim_take(a, lv, 0, south)

    def pass_on(south):
        for i, spot in enumerate(DETOUR):

            def hand():
                for h in range(HALVES):
                    out_copy(i, h, south).wait_recv()
                    on_copy(i, h, south).start()

            if spot in SINGLE:
                pl.when(core == 1)(hand)
            else:
                hand()

    def send_level(a, lv):
        polar_half(lambda south: [far_send(a, lv, k, south) for k in range(per)])

        @pl.when(middle)
        def _():
            pack_send(a, lv)

        for q in range(lv * per, (lv + 1) * per):
            core_copy(a, q, 0).start()

    for lv in range(levels):
        take(tr.at[lv], loc.at[lv])
        send_level(0, lv)
        if lv == 0:
            take(ad, loc.at[levels])
            lat_start(ab, 0, 0)

    @pl.when(lat == 0)
    def _():
        for buf in (ab, zb):
            buf[:, pl.ds(0, RIM)] = jnp.zeros((levels, RIM, cells, width), jnp.float32)

    @pl.when(lat == n_lat - 1)
    def _():
        for buf in (ab, zb):
            buf[:, pl.ds(RIM + rows, RIM)] = jnp.zeros((levels, RIM, cells, width), jnp.float32)

    for d in small:
        d.wait()
    faces = rows + 5
    lanes = lax.broadcasted_iota(jnp.int32, (cells, total_rows), 1)
    for lv in range(levels):

        @pl.loop(0, faces, unroll=faces)
        def _(f):
            row = first + f - 2
            chosen = jnp.logical_and(lanes == row, lanes > 0)
            column = jnp.sum(jnp.where(chosen, mer[lv], 0.0), axis=1, keepdims=True)
            vb[lv, f] = jnp.broadcast_to(column, (cells, width))

        if lv + 1 < levels:
            lat_start(ab, 0, lv + 1)

        @pl.loop(0, rows)
        def _(r):
            for k, t in enumerate(zonal_taps(fractions[lv, first + r])):
                taps[(lv * rows + r) * 6 + k] = t

    def sweep(a, q, sink, sink_row, sign):
        lv, r0 = chunks[q]
        buf = gath[a][q]

        @pl.loop(0, step)
        def _(r):
            buf[r, pl.ds(total_cells + cells, SUB), :] = buf[r, pl.ds(cells, SUB), :]
            shift = shifts[lv, first + r0 + r]
            if sign < 0:
                start = lax.rem(2 * total_cells - shift - 3, total_cells)
            else:
                start = lax.rem(2 * total_cells + shift - 2, total_cells)
            base = (lv * rows + r0 + r) * 6
            w = [taps[base + k] for k in range(6)]
            if sign > 0:
                w = w[::-1]
            for c in range(cells // SUB):
                total = None
                for k in range(6):
                    term = w[k] * buf[r, pl.ds(start + c * SUB + k, SUB), :]
                    total = term if total is None else total + term
                sink[lv, sink_row + r0 + r, pl.ds(c * SUB, SUB), :] = total

    def level_take(a, lv, k=0, south=True):
        take(tr.at[lv], rc0.at[a, lv])

    def finish(a, lv, k, south):
        q = chunk_at(lv, k, south)
        if kind(a, lv, k) == "trim":

            @pl.when(core == a)
            def _():
                core_copy(a, q, 1).wait_recv()

        else:
            core_copy(a, q, 1).wait_recv()
        if a == 0:
            sweep(0, q, zb, RIM, -1)
        else:
            sweep(1, q, oa, 0, 1)

    def polar_steps(a):
        spots = [(lv, k) for lv in range(levels) for k in range(per)]
        direct = [p for p in spots if kind(a, *p) != "detour"]
        due = {p: i + SLOW for i, p in enumerate(direct)}
        due.update({p: i for i, p in enumerate(DETOUR) if a == 1})
        order = sorted(spots, key=lambda p: due[p])
        steps = []
        ready_levels = []
        for i in range(nq + LAG):
            if i < nq:
                steps.append((relay, a) + order[i])
            if i >= LAG:
                lv, k = order[i - LAG]
                if lv not in ready_levels:
                    ready_levels.append(lv)
                    steps.append((level_take, a, lv, k))
                steps.append((finish, a, lv, k))
        return steps

    def polar_run(steps):
        polar_half(lambda south: [step_[0](*step_[1:], south) for step_ in steps])

    def middle_finish(a):
        for lv in range(levels):
            pack_take(a, lv)
            level_take(a, lv)
            for q in range(lv * per, (lv + 1) * per):
                if a == 0:
                    sweep(0, q, zb, RIM, -1)
                else:
                    sweep(1, q, oa, 0, 1)

    take(tr, loc.at[levels + 1])

    @pl.when(middle)
    def _():
        middle_finish(0)
        for lv in range(levels):
            lat_start(zb, 1, lv)

    for lv in range(levels):
        lat_wait(0, lv)

        @pl.loop(0, cells // SUB)
        def _(c):
            at = pl.ds(pl.multiple_of(c * SUB, SUB), SUB)
            ev, q6b, dqb, eb = {}, {}, {}, {}
            carry = None
            y = {r: ab[lv, r + RIM, at, :] for r in range(-3, -1)}
            for f in range(-2, rows + 3):
                y[f] = ab[lv, f + RIM, at, :]
                v = vb[lv, f + 2, at, :]
                north = v > 0.0
                beta, gamma = face_terms(v)
                change = y[f] - y[f - 1]
                ev[f] = v * change
                b = beta * change
                g = -gamma * change
                bn, gn = jnp.where(north, b, 0.0), jnp.where(north, g, 0.0)
                if carry is not None:
                    q6b[f - 1] = bn + carry[0]
                    dqb[f - 1] = gn + carry[1]
                carry = (b - bn, g - gn)
                h = f - 1
                if h >= -1:
                    eb[h] = ev[h] - 3.0 * (q6b[h - 1] + q6b[h]) + (dqb[h - 1] - dqb[h])
                r = h - 2
                if r >= 0:
                    value = (
                        y[r]
                        + 6.0 * q6b[r]
                        + (7.0 / 12.0) * (eb[r] + eb[r + 1])
                        - (1.0 / 12.0) * (eb[r - 1] + eb[r + 2])
                    )
                    q = lv * per + r // step
                    gath[1][q][r % step, at, :] = value
                    gath[1][q][
                        r % step, pl.ds(pl.multiple_of(total_cells + c * SUB, SUB), SUB), :
                    ] = value

        if lv == 0:

            @pl.when(polar)
            def _():
                pl.semaphore_wait(ready, 1)

        send_level(1, lv)


    polar_run(polar_steps(0))

    @pl.when(polar)
    def _():
        for lv in range(levels):
            lat_start(zb, 1, lv)

    @pl.when(middle)
    def _():
        by_half(pass_on)
        middle_finish(1)

    late = polar_steps(1)
    polar_run(late[:-LATE])

    for lv in range(levels):
        lat_wait(1, lv)

        @pl.loop(0, cells // SUB)
        def _(c):
            at = pl.ds(pl.multiple_of(c * SUB, SUB), SUB)
            z = {r: zb[lv, r + RIM, at, :] for r in range(-3, 0)}
            e, q6, dq, flux = {}, {}, {}, {}
            for f in range(-1, rows + 2):
                z[f + 1] = zb[lv, f + 1 + RIM, at, :]
                e[f] = (7.0 / 12.0) * (z[f - 1] + z[f]) - (1.0 / 12.0) * (z[f - 2] + z[f + 1])
                u = f - 1
                if u >= -1:
                    q6[u] = 6.0 * z[u] - 3.0 * (e[u] + e[f])
                    dq[u] = e[f] - e[u]
                if u >= 0:
                    v = vb[lv, u + 2, at, :]
                    north = v > 0.0
                    beta, gamma = face_terms(v)
                    flux[u] = (
                        v * e[u]
                        + beta * jnp.where(north, q6[u - 1], q6[u])
                        - gamma * jnp.where(north, dq[u - 1], dq[u])
                    )
                if u >= 1:
                    of[lv, u - 1, at, :] = z[u - 1] - flux[u] + flux[u - 1]

    polar_run(late[-LATE:])

    for side in (HEAD, TAIL):

        @pl.when(core == side)
        def _():
            take(lump(len(DETOUR) - (len(SINGLE) if side == 0 else 0)), sd.at[0])

    for k in range(2):

        @pl.when(lat > 0)
        def _():
            take(tr.at[:, pl.ds(0, RIM)], sh.at[k, 0])

        @pl.when(lat < n_lat - 1)
        def _():
            take(tr.at[:, pl.ds(0, RIM)], sh.at[k, 1])

    for a in range(2):
        take(tr, sc.at[a, 0])
        around = (len(DETOUR) - len(SINGLE), len(DETOUR)) if a == 1 else (0, 0)
        straight = [nq - levels - m for m in around]

        @pl.when(jnp.logical_and(polar, core == a))
        def _():
            take(lump(straight[a]), sx.at[a])
            take(lump(nq - levels), sc.at[a, 1])
            for w in range(2):
                take(sendt.at[a, :, w, pl.ds(SUB, trims[a][1 + w][1])], st.at[w])

        @pl.when(jnp.logical_and(polar, core == 1 - a))
        def _():
            take(lump(straight[1 - a] + levels), sx.at[a])
            take(tr, sc.at[a, 1])

        for side in (HEAD, TAIL):

            @pl.when(jnp.logical_and(middle, core == side))
            def _():
                take(sendp.at[a, :, pl.ds(SUB, plans[a][side][1])], sc.at[a, 1])

        if spill:

            @pl.when(middle)
            def _():
                take(sendx.at[a], sx.at[a])


def store(f_in, a_in, f_out, a_out, sem):
    part = max(1, f_in.shape[1] // 4)
    pairs = ((f_in, f_out), (a_in, a_out))
    for k, (source, target) in enumerate(pairs):
        for lv in range(f_in.shape[0]):
            for r0 in range(0, f_in.shape[1], part):
                at = (lv, pl.ds(r0, part))
                pltpu.make_async_copy(source.at[at], target.at[at], sem.at[k]).start()
    for k, (source, target) in enumerate(pairs):
        pltpu.make_async_copy(source, target, sem.at[k]).wait()


def local(tracers, adjoint_in, shifts, fractions, meridional):
    levels, rows, cells, width = tracers.shape
    n_lon, n_lat = lax.axis_size("lon"), lax.axis_size("lat")
    n_x = n_lon // 2
    pair = fits(levels, rows, cells, n_lon, n_lat)
    step = max(1, rows // (4 if pair else 2))
    nq = levels * (rows // step)
    dma = pltpu.SemaphoreType.DMA
    block = pltpu.VMEM((step, (n_lon + 1) * cells + SUB, width), jnp.float32)
    banded = pltpu.VMEM((levels, rows + 2 * RIM, cells, width), jnp.float32)
    scratch = [block] * (2 * nq) + [
        banded,
        banded,
        pltpu.VMEM((levels, rows + 5, cells, width), jnp.float32),
        pltpu.SMEM((levels * rows * 6,), jnp.float32),
        pltpu.SMEM(shifts.shape, jnp.int32),
        pltpu.SMEM(fractions.shape, jnp.float32),
        pltpu.VMEM((levels, cells, meridional.shape[1]), jnp.float32),
    ]
    if pair:
        nd = len(DETOUR)
        dims = (levels, rows, cells, width, n_lon, n_lat, step)
        long = pack_room(rows, cells, n_lon, n_lat)
        pack = pltpu.VMEM((2, levels, long, width), jnp.float32)
        trim = pltpu.VMEM(
            (2, levels, 2, trim_room(rows, cells, n_lon, n_lat), width), jnp.float32
        )
        few = pltpu.VMEM((2, levels * SUB, width), jnp.float32)
        body = paired
        scratch += [
            pltpu.VMEM((nd, step, cells, width), jnp.float32),
            pack,
            pack,
            few,
            few,
            trim,
            trim,
            dma((levels + 5,)),
            dma((2,)),
            dma((2, 2)),
            dma((1,)),
            dma((2,)),
            dma((2, 2)),
            dma((2, nq)),
            dma((2, levels)),
            dma((2, nq)),
            dma((2, levels)),
            pltpu.SemaphoreType.REGULAR,
        ]
    else:
        dims = (levels, rows, cells, width, n_lon, n_lat, step)
        body = general
        scratch += [
            dma((2 * nq + 4,)),
            dma((2, nq, 2 * n_x)),
            dma((2, nq, 2 * n_x)),
            dma((2, 2)),
            dma((2, 2)),
        ]
    vmem = pl.BlockSpec(memory_space=pltpu.VMEM)
    far = pl.BlockSpec(memory_space=pltpu.HBM)
    kept = pltpu.VMEM(tracers.shape, jnp.float32)
    staged = pl.pallas_call(
        functools.partial(body, dims),
        out_shape=(kept, kept),
        in_specs=[far] * 5,
        out_specs=(vmem, vmem),
        scratch_shapes=scratch,
        compiler_params=pltpu.CompilerParams(
            collective_id=0, has_side_effects=True, vmem_limit_bytes=60 << 20
        ),
    )(tracers, adjoint_in, shifts, fractions, jnp.swapaxes(meridional, 1, 2))
    final = jax.ShapeDtypeStruct(tracers.shape, jnp.float32)
    return pl.pallas_call(
        store,
        out_shape=(final, final),
        in_specs=[vmem, vmem],
        out_specs=(far, far),
        scratch_shapes=[dma((2,))],
        compiler_params=pltpu.CompilerParams(vmem_limit_bytes=4 << 20),
    )(*staged)


def solution(mesh):
    block = P("grp", "lat", "lon", None)
    in_specs = (block, block, P(), P(), P(None, None, "lon"))
    return jax.shard_map(
        local, mesh=mesh, in_specs=in_specs, out_specs=(block, block), check_vma=False
    )
```
